32 devices in a mesh: gz: 16 (over z, y, core), ba: 2 (over x).
Axes of the slice: x: 2, y: 2, z: 4, core: 2. Of those that a mesh axis runs over, the one named last changes fastest.
Arguments:
- coeffs: float32 [2, 3, 4, 32, 128, 128], P(None, None, 'ba', 'gz'), may hold values from -6 to 6
- material: int32 [32, 128, 128], P('gz'), may hold values from 0 to 3
- inv_diag: float32 [4, 3], replicated, may hold values from 0.1 to 1
- inv_off: float32 [4, 3], replicated, may hold values from -0.1 to 0.1
Outputs:
- theta: float32 [2, 3, 4, 32, 128, 128], P(None, None, 'ba', 'gz')
- gram: float32 [2, 4, 4], P(None, None, 'ba')
The draws below stay inside these ranges and needn't reach their ends.
Inputs may be any that keep to these rules, and one draw needn't show every extreme that they name: material indices.
All inputs are finite; a program needn't handle non-finite values.
Results may differ from the reference program's by a relative error of at most 0.00011.
Values sent between devices are 32-bit elements; how exact they have to be, the bound alone decides.
A program may use at most 64 MiB of HBM per device.

```python
import math
import jax
import jax.numpy as jnp
from jax import lax

NX = 128
NY = 128
CZ = 2
MATERIALS = 4
NZ = 32
BANDS = 4
N_GZ = 16


def with_ends(values, stream_key, low, largest):
    index_at = [jax.random.randint(jax.random.fold_in(stream_key, axis), (), 0, length) for axis, length in enumerate(values.shape)]
    widest = values.shape.index(max(values.shape))
    next_to = index_at[:widest] + [(index_at[widest] + 1) % values.shape[widest]] + index_at[widest + 1:]
    return values.at[tuple(index_at)].set(low).at[tuple(next_to)].set(largest)


def block_levels(rng, extent, cuts, low, largest):
    def one(axis_at, blocks):
        heights = jax.random.uniform(jax.random.fold_in(jax.random.fold_in(rng, 6), axis_at), (blocks,), jnp.float32, low / len(cuts), largest / len(cuts))
        return jnp.repeat(jnp.exp(heights), extent[axis_at] // blocks).reshape((-1,) + (1,) * (len(extent) - axis_at - 1))

    factor_of = one(*cuts[0])
    for cut in cuts[1:]:
        factor_of = factor_of * one(*cut)
    return factor_of


def noise(key, extent, width, reach, cuts=(), kind=jnp.bfloat16):
    entries = jax.random.normal(key, extent, jnp.float32) * width
    if len(cuts) > 0:
        entries = block_levels(key, extent, cuts, -0.22, 0.18) * entries
    return jnp.clip(entries, min=-reach, max=reach).astype(kind)


def setup_inputs(seed: int = 0) -> dict:
    streams_of = jax.random.split(jax.random.key(seed), 5)
    return {
        "coeffs": noise(streams_of[0], (2, 3, BANDS, NZ, NY, NX), 1.0, 6.0, ((2, 2), (3, 16)), jnp.float32),
        "material": with_ends(jax.random.randint(streams_of[1], (NZ, NY, NX), 0, MATERIALS), jax.random.fold_in(streams_of[1], 1), 0, MATERIALS - 1).astype(jnp.int32),
        "inv_diag": jnp.clip(jnp.exp(jax.random.uniform(streams_of[2], (MATERIALS, 3), jnp.float32, math.log(0.1), math.log(1.0))), 0.1, 1.0),
        "inv_off": jnp.clip(jax.random.uniform(streams_of[3], (MATERIALS, 3), jnp.float32, -0.1, 0.1), -0.1, 0.1),
    }


highest = lax.Precision.HIGHEST


def reverse_bits(values, levels):
    flipped = jnp.zeros_like(values)
    for position in range(levels):
        flipped = flipped + ((values >> position) & 1) * (1 << (levels - 1 - position))
    return flipped


def signed_wave(numbers, length):
    shifted = jnp.where(numbers < length // 2, numbers, numbers - length)
    return shifted.astype(jnp.float32) / (length / 2.0)


def cross_waves(waves, field):
    first, second, third = waves
    return jnp.stack([second * field[2] - third * field[1],
                      third * field[0] - first * field[2],
                      first * field[1] - second * field[0]])


def reference(coeffs, material, inv_diag, inv_off):
    levels = N_GZ.bit_length() - 1
    rows = jnp.arange(NZ, dtype=jnp.int32)
    wave_rows = reverse_bits(rows // CZ, levels) + N_GZ * (rows % CZ)
    natural = jnp.zeros((NZ,), jnp.int32).at[wave_rows].set(rows)
    waves = (signed_wave(jnp.arange(NX, dtype=jnp.int32), NX)[None, None, :],
             signed_wave(jnp.arange(NY, dtype=jnp.int32), NY)[None, :, None],
             signed_wave(wave_rows, NZ)[:, None, None])
    onehot = (material[None] == jnp.arange(MATERIALS, dtype=jnp.int32)[:, None, None, None]).astype(jnp.float32)
    table = jnp.concatenate([inv_diag, inv_off], axis=1)
    tensor = jnp.einsum("mk,mzyx->kzyx", table, onehot, precision=highest)

    def one_band(band):
        spectral = band[0] + 1j * band[1]
        curl = cross_waves(waves, spectral)[:, natural]
        field = jnp.fft.ifftn(curl, axes=(1, 2, 3), norm="ortho")
        scaled = jnp.stack([tensor[0] * field[0] + tensor[3] * field[1] + tensor[5] * field[2],
                            tensor[3] * field[0] + tensor[1] * field[1] + tensor[4] * field[2],
                            tensor[5] * field[0] + tensor[4] * field[1] + tensor[2] * field[2]])
        back = jnp.fft.fftn(scaled, axes=(1, 2, 3), norm="ortho")[:, wave_rows]
        result = -cross_waves(waves, back)
        return jnp.stack([jnp.real(result), jnp.imag(result)]).astype(jnp.float32)

    theta = jnp.moveaxis(lax.map(one_band, jnp.moveaxis(coeffs, 2, 0)), 0, 2)
    factor = 1.0 / (NX * NY * NZ)
    real_part = (jnp.einsum("cbzyx,cezyx->be", coeffs[0], theta[0], precision=highest)
                 + jnp.einsum("cbzyx,cezyx->be", coeffs[1], theta[1], precision=highest)) * factor
    imag_part = (jnp.einsum("cbzyx,cezyx->be", coeffs[0], theta[1], precision=highest)
                 - jnp.einsum("cbzyx,cezyx->be", coeffs[1], theta[0], precision=highest)) * factor
    gram = jnp.stack([real_part, imag_part])
    return theta, gram
```

```python
import functools
import math

import jax
import jax.numpy as jnp
import numpy as np
from jax import lax
from jax.experimental import pallas as pl
from jax.experimental.pallas import tpu as pltpu
from jax.sharding import PartitionSpec as P

highest = lax.Precision.HIGHEST
half_turn = 3.141592653589793


def reverse_bits(values, levels):
    flipped = jnp.zeros_like(values)
    for position in range(levels):
        flipped = flipped + (values >> position & 1) * (1 << levels - 1 - position)
    return flipped


def signed_wave(numbers, length):
    shifted = jnp.where(numbers < length // 2, numbers, numbers - length)
    return shifted.astype(jnp.float32) / (length / 2.0)


def phase_tables(first, second, length, sign):
    product = first[:, None] * second[None, :] % length
    angle = 2.0 * half_turn / length * product.astype(jnp.float32)
    factor = 1.0 / math.sqrt(length)
    return (jnp.cos(angle) * factor, sign * jnp.sin(angle) * factor)


def cross_waves(waves, field):
    first, second, third = waves
    return jnp.stack(
        [
            second * field[:, 2] - third * field[:, 1],
            third * field[:, 0] - first * field[:, 2],
            first * field[:, 1] - second * field[:, 0],
        ],
        axis=1,
    )


def along_width(field, cosine, sine):
    breadth = field.shape[-1]
    rows = field.reshape(2, -1, breadth)
    joined = jnp.concatenate([cosine, sine], axis=1)
    real_prod = jnp.dot(rows[0], joined, precision=highest)
    imag_prod = jnp.dot(rows[1], joined, precision=highest)
    real_out = real_prod[:, :breadth] - imag_prod[:, breadth:]
    imag_out = real_prod[:, breadth:] + imag_prod[:, :breadth]
    return jnp.stack([real_out, imag_out]).reshape(field.shape)


def along_height(field, cosine, sine):
    tables = jnp.stack([cosine, sine])
    product = jnp.einsum("pcbzyx,tyk->tpcbzkx", field, tables, precision=highest)
    return jnp.stack([product[0, 0] - product[1, 1], product[1, 0] + product[0, 1]])


def along_depth(field, cosine, sine):
    tables = jnp.stack([cosine, sine])
    product = jnp.einsum("pcbzyx,tzk->tpcbkyx", field, tables, precision=highest)
    return jnp.stack([product[0, 0] - product[1, 1], product[1, 0] + product[0, 1]])


def apply_material(field, material, inv_diag, inv_off):
    materials = inv_diag.shape[0]
    onehot = (material[None] == jnp.arange(materials, dtype=jnp.int32)[:, None, None, None]).astype(
        jnp.float32
    )
    table = jnp.concatenate([inv_diag, inv_off], axis=1)
    tensor = jnp.einsum("mk,mzyx->kzyx", table, onehot, precision=highest)
    first = field[:, 0]
    second = field[:, 1]
    third = field[:, 2]
    return jnp.stack(
        [
            tensor[0] * first + tensor[3] * second + tensor[5] * third,
            tensor[3] * first + tensor[1] * second + tensor[4] * third,
            tensor[5] * first + tensor[4] * second + tensor[2] * third,
        ],
        axis=1,
    )


def on_device(coeffs, material, inv_diag, inv_off):
    groups = lax.axis_size("gz")
    levels = groups.bit_length() - 1
    depth = coeffs.shape[3]
    height = coeffs.shape[4]
    breadth = coeffs.shape[5]
    total_depth = depth * groups
    device = lax.axis_index("gz")
    local_rows = jnp.arange(depth, dtype=jnp.int32)
    waves_here = reverse_bits(device, levels) + groups * local_rows
    across = jnp.arange(breadth, dtype=jnp.int32)
    upward = jnp.arange(height, dtype=jnp.int32)
    waves = (
        signed_wave(across, breadth)[None, None, :],
        signed_wave(upward, height)[None, :, None],
        signed_wave(waves_here, total_depth)[:, None, None],
    )
    curl = cross_waves(waves, coeffs)
    all_rows = jnp.arange(total_depth, dtype=jnp.int32)
    wave_rows = reverse_bits(all_rows // depth, levels) + groups * (all_rows % depth)
    height_cos, height_sin = phase_tables(upward, upward, height, 1.0)
    width_cos, width_sin = phase_tables(across, across, breadth, 1.0)
    planar = along_height(curl, height_cos, height_sin)
    planar = along_width(planar, width_cos, width_sin)
    material_slab = lax.all_to_all(material, "gz", split_axis=1, concat_axis=0, tiled=True)
    inverse_cos, inverse_sin = phase_tables(wave_rows, all_rows, total_depth, 1.0)
    forward_cos, forward_sin = phase_tables(all_rows, wave_rows, total_depth, -1.0)
    spatial_piece = along_depth(
        lax.all_to_all(planar, "gz", split_axis=4, concat_axis=3, tiled=True),
        inverse_cos,
        inverse_sin,
    )
    scaled_piece = apply_material(spatial_piece, material_slab, inv_diag, inv_off)
    returned = along_depth(scaled_piece, forward_cos, forward_sin)
    spectral = lax.all_to_all(returned, "gz", split_axis=3, concat_axis=4, tiled=True)
    spectral = along_width(spectral, width_cos, -width_sin)
    spectral = along_height(spectral, height_cos, -height_sin)
    theta = -cross_waves(waves, spectral)
    factor = 1.0 / (breadth * height * total_depth)
    piece = lax.all_gather(coeffs, "ba", axis=2, tiled=True)
    real_part = jnp.einsum("cbzyx,cezyx->be", piece[0], theta[0], precision=highest) + jnp.einsum(
        "cbzyx,cezyx->be", piece[1], theta[1], precision=highest
    )
    imag_part = jnp.einsum("cbzyx,cezyx->be", piece[0], theta[1], precision=highest) - jnp.einsum(
        "cbzyx,cezyx->be", piece[1], theta[0], precision=highest
    )
    block = jnp.stack([real_part, imag_part]) * factor
    gram = lax.psum(block, "gz")
    return (theta, gram)


MESH = pl.DeviceIdType.MESH
single = jnp.float32
half = jnp.bfloat16


def split_table(length, extra):
    numbers = np.arange(length)
    angle = 2.0 * np.pi / length * (numbers[:, None] * numbers[None, :] % length)
    cosine = np.cos(angle) * extra / math.sqrt(length)
    sine = np.sin(angle) * extra / math.sqrt(length)
    inverse = np.block([[cosine, sine], [-sine, cosine]])
    parts = []
    for table in (inverse, inverse.T):
        high = table.astype(np.float32).astype(half)
        low = (table - high.astype(np.float64)).astype(half)
        parts += [high, low]
    return np.stack(parts)


def halves(values):
    high = values.astype(half)
    return high, (values - high.astype(single)).astype(half)


def product(first, second):
    dot = functools.partial(jnp.dot, preferred_element_type=single)
    return dot(first[0], second[0]) + (dot(first[0], second[1]) + dot(first[1], second[0]))


def twiddled(pair, step, span, sign):
    real, imag = pair
    if step == 0:
        return real, imag
    if 2 * step == span:
        return (-imag, real) if sign > 0 else (imag, -real)
    angle = math.pi * step / span
    cosine, sine = math.cos(angle), sign * math.sin(angle)
    return real * cosine - imag * sine, real * sine + imag * cosine


def to_voxels(points):
    points = list(points)
    span = 1
    while span < len(points):
        for base in range(0, len(points), 2 * span):
            for step in range(span):
                a = points[base + step]
                t = twiddled(points[base + step + span], step, span, 1.0)
                points[base + step] = (a[0] + t[0], a[1] + t[1])
                points[base + step + span] = (a[0] - t[0], a[1] - t[1])
        span *= 2
    return points


def to_waves(points):
    points = list(points)
    span = len(points) // 2
    while span >= 1:
        for base in range(0, len(points), 2 * span):
            for step in range(span):
                a, t = points[base + step], points[base + step + span]
                points[base + step] = (a[0] + t[0], a[1] + t[1])
                points[base + step + span] = twiddled(
                    (a[0] - t[0], a[1] - t[1]), step, span, -1.0
                )
        span //= 2
    return points


def operator_kernel(
    groups,
    coeffs_hbm,
    material_hbm,
    diag_hbm,
    off_hbm,
    table_hbm,
    theta_ref,
    gram_ref,
    coeffs_ref,
    material_ref,
    table_ref,
    diag_ref,
    off_ref,
    slab_ref,
    tensor_ref,
    high_ref,
    low_ref,
    back_ref,
    field_ref,
    scaled_ref,
    other_ref,
    out1_ref,
    in1_ref,
    out2_ref,
    in2_ref,
    sums_ref,
    load_sem,
    slab_send,
    slab_recv,
    half_sem,
    send1,
    recv1,
    send2,
    recv2,
    other_send,
    other_recv,
    sums_send,
    sums_recv,
):
    _, comps, bands, depth, height, breadth = coeffs_ref.shape
    total = depth * groups
    columns = height // groups
    levels = groups.bit_length() - 1
    me = lax.axis_index("gz")
    mine = lax.axis_index("ba")
    middle = groups // 2

    def offset_of(i):
        away = (i + 1) // 2
        return middle + away - 2 * away * (i % 2)

    def each_peer(body):
        def step(i, carry):
            k = offset_of(i)
            body(k, (me + k) % groups, (me + groups - k) % groups)
            return carry

        lax.fori_loop(0, groups - 1, step, 0)

    barrier = pltpu.get_barrier_semaphore()
    each_peer(
        lambda k, peer, source: pl.semaphore_signal(
            barrier, inc=1, device_id={"gz": peer}, device_id_type=MESH
        )
    )
    pl.semaphore_signal(barrier, inc=1, device_id={"ba": 1 - mine}, device_id_type=MESH)

    loads = [
        pltpu.make_async_copy(coeffs_hbm, coeffs_ref, load_sem.at[0]),
        pltpu.make_async_copy(table_hbm, table_ref, load_sem.at[1]),
        pltpu.make_async_copy(material_hbm, material_ref, load_sem.at[2]),
        pltpu.make_async_copy(diag_hbm, diag_ref, load_sem.at[3]),
        pltpu.make_async_copy(off_hbm, off_ref, load_sem.at[4]),
    ]
    for load in loads:
        load.start()

    across = lax.broadcasted_iota(jnp.int32, (1, breadth), 1)
    upward = lax.broadcasted_iota(jnp.int32, (height, 1), 0)
    wave_x = jnp.where(across < breadth // 2, across, across - breadth).astype(single) / (
        breadth / 2.0
    )
    wave_y = jnp.where(upward < height // 2, upward, upward - height).astype(single) / (
        height / 2.0
    )
    reversed_me = 0
    for position in range(levels):
        reversed_me = reversed_me + (me // (1 << position)) % 2 * (1 << (levels - 1 - position))
    waves_z = []
    for row in range(depth):
        number = reversed_me + groups * row
        signed = number - total * (number // (total // 2))
        waves_z.append(signed.astype(single) / (total / 2.0))

    def cross(parts, row):
        waves = (wave_x, wave_y, waves_z[row])
        return [
            waves[(c + 1) % 3] * parts[(c + 2) % 3] - waves[(c + 2) % 3] * parts[(c + 1) % 3]
            for c in range(3)
        ]

    def plain_table():
        return table_ref[0], table_ref[1]

    def turned_table():
        return table_ref[2], table_ref[3]

    def gather_blocks(values):
        top, bottom = values[:height], values[height:]
        return jnp.concatenate(
            [
                jnp.concatenate(
                    [
                        top[:, z * breadth : (z + 1) * breadth],
                        bottom[:, z * breadth : (z + 1) * breadth],
                    ],
                    axis=1,
                )
                for z in range(depth)
            ],
            axis=0,
        )

    def spread_blocks(values):
        return jnp.concatenate(
            [
                jnp.concatenate(
                    [
                        values[z * height : (z + 1) * height, p * breadth : (p + 1) * breadth]
                        for z in range(depth)
                    ],
                    axis=1,
                )
                for p in range(2)
            ],
            axis=0,
        )

    def make_planes(b):
        for p in range(2):
            for z in range(depth):
                curls = cross([coeffs_ref[p, c, b, z] for c in range(3)], z)
                for c in range(3):
                    high, low = halves(curls[c])
                    rows, lanes = pl.ds(p * height, height), pl.ds(z * breadth, breadth)
                    high_ref[c, rows, lanes] = high
                    low_ref[c, rows, lanes] = low

        def one(c, carry):
            tall = product(turned_table(), (high_ref[c], low_ref[c]))
            wide = product(halves(gather_blocks(tall)), plain_table())
            for p in range(2):
                for z in range(depth):
                    plane = wide[z * height : (z + 1) * height, p * breadth : (p + 1) * breadth]
                    out1_ref[b, :, c, p, z] = plane.reshape(groups, columns, breadth)
            return carry

        lax.fori_loop(0, 3, one, 0)

    def exchange(out, into, send, recv, b, peer, k):
        return pltpu.make_async_remote_copy(
            src_ref=out.at[b, peer],
            dst_ref=into.at[b, me],
            send_sem=send.at[b, k],
            recv_sem=recv.at[b, k],
            device_id={"gz": peer},
            device_id_type=MESH,
        )

    def arrival(out, into, send, recv, b, source, k):
        return pltpu.make_async_remote_copy(
            src_ref=out.at[b, source],
            dst_ref=into.at[b, source],
            send_sem=send.at[b, k],
            recv_sem=recv.at[b, k],
            device_id={"gz": source},
            device_id_type=MESH,
        )

    def start_all(out, into, send, recv, b):
        each_peer(lambda k, peer, source: exchange(out, into, send, recv, b, peer, k).start())
        into[b, me] = out[b, me]

    def finish_all(out, into, send, recv, b):
        each_peer(
            lambda k, peer, source: arrival(out, into, send, recv, b, source, k).wait_recv()
        )

    def drain_all(out, into, send, recv, b):
        each_peer(lambda k, peer, source: exchange(out, into, send, recv, b, peer, k).wait_send())

    def columns_of(peer):
        return pl.ds(pl.multiple_of(peer * columns, columns), columns)

    def slab_copy(peer, slot, k):
        return pltpu.make_async_remote_copy(
            src_ref=material_ref.at[mine, columns_of(peer), :],
            dst_ref=slab_ref.at[mine, slot],
            send_sem=slab_send.at[k],
            recv_sem=slab_recv.at[k],
            device_id={"gz": peer},
            device_id_type=MESH,
        )

    def half_copy(row):
        return pltpu.make_async_remote_copy(
            src_ref=slab_ref.at[row],
            dst_ref=slab_ref.at[row],
            send_sem=half_sem.at[0],
            recv_sem=half_sem.at[1],
            device_id={"ba": 1 - mine},
            device_id_type=MESH,
        )

    def other_copy(b):
        return pltpu.make_async_remote_copy(
            src_ref=field_ref.at[b],
            dst_ref=other_ref.at[b],
            send_sem=other_send.at[b],
            recv_sem=other_recv.at[b],
            device_id={"ba": 1 - mine},
            device_id_type=MESH,
        )

    loads[0].wait()
    loads[1].wait()
    make_planes(0)
    for load in loads[2:]:
        load.wait()
    pl.semaphore_wait(barrier, groups)
    start_all(out1_ref, in1_ref, send1, recv1, 0)
    each_peer(lambda k, peer, source: slab_copy(peer, me, k).start())
    slab_ref[mine, me] = material_ref[mine, columns_of(me), :]
    for b in range(1, bands):
        make_planes(b)
        start_all(out1_ref, in1_ref, send1, recv1, b)

    each_peer(lambda k, peer, source: slab_copy(source, source, k).wait_recv())
    half_copy(mine).start()
    half_copy(1 - mine).wait_recv()
    kinds = diag_ref.shape[0]
    for row in range(depth):
        codes = slab_ref[row]
        for entry in range(6):
            table = diag_ref if entry < 3 else off_ref
            values = jnp.full(codes.shape, table[0, entry % 3], single)
            for kind in range(1, kinds):
                values = jnp.where(codes == kind, table[kind, entry % 3], values)
            tensor_ref[entry, :, row] = values

    for b in range(bands):
        finish_all(out1_ref, in1_ref, send1, recv1, b)

        def inverse(c, carry):
            points = [
                (in1_ref[b, r // depth, c, 0, r % depth], in1_ref[b, r // depth, c, 1, r % depth])
                for r in range(total)
            ]
            for z, (real, imag) in enumerate(to_voxels(points)):
                field_ref[b, c, 0, z] = real
                field_ref[b, c, 1, z] = imag
            return carry

        lax.fori_loop(0, 3, inverse, 0)
        other_copy(b).start()

        def scale(z, carry):
            xx, yy, zz, xy, yz, zx = [
                tensor_ref[entry, z // depth, z % depth] for entry in range(6)
            ]
            for p in range(2):
                first, second, third = [field_ref[b, c, p, z] for c in range(3)]
                scaled_ref[b, 0, p, z] = xx * first + xy * second + zx * third
                scaled_ref[b, 1, p, z] = xy * first + yy * second + yz * third
                scaled_ref[b, 2, p, z] = zx * first + yz * second + zz * third
            return carry

        lax.fori_loop(0, total, scale, 0, unroll=4)

        def forward(c, carry):
            points = [(scaled_ref[b, c, 0, z], scaled_ref[b, c, 1, z]) for z in range(total)]
            for r, (real, imag) in enumerate(to_waves(points)):
                out2_ref[b, r // depth, c, 0, r % depth] = real
                out2_ref[b, r // depth, c, 1, r % depth] = imag
            return carry

        lax.fori_loop(0, 3, forward, 0)
        start_all(out2_ref, in2_ref, send2, recv2, b)

    def sums_copy(slot, peer, k):
        return pltpu.make_async_remote_copy(
            src_ref=sums_ref.at[slot],
            dst_ref=sums_ref.at[slot],
            send_sem=sums_send.at[k],
            recv_sem=sums_recv.at[k],
            device_id={"gz": peer},
            device_id_type=MESH,
        )

    def make_sums():
        def add(z, sums):
            sums = list(sums)
            for c in range(3):
                ours = [(scaled_ref[b, c, 0, z], scaled_ref[b, c, 1, z]) for b in range(bands)]
                fields = [
                    (source[a, c, 0, z], source[a, c, 1, z])
                    for source in (field_ref, other_ref)
                    for a in range(bands)
                ]
                n = 0
                for t_real, t_imag in ours:
                    for real, imag in fields:
                        sums[n] = sums[n] + (real * t_real + imag * t_imag)
                        sums[n + 1] = sums[n + 1] + (real * t_imag - imag * t_real)
                        n += 2
            return tuple(sums)

        zero = jnp.zeros((columns, breadth), single)
        sums = lax.fori_loop(0, total, add, (zero,) * (4 * bands * bands))
        sums_ref[me] = jnp.concatenate([jnp.sum(v, axis=0, keepdims=True) for v in sums], axis=0)

    half_copy(mine).wait_send()
    each_peer(lambda k, peer, source: slab_copy(peer, me, k).wait_send())
    for b in range(bands):
        drain_all(out1_ref, in1_ref, send1, recv1, b)

    for b in range(bands):
        if b == bands - 1:
            for a in range(bands):
                other_copy(a).wait_send()
                other_copy(a).wait_recv()
            make_sums()
            each_peer(lambda k, peer, source: sums_copy(me, peer, k).start())
            for a in range(b):
                drain_all(out2_ref, in2_ref, send2, recv2, a)
        finish_all(out2_ref, in2_ref, send2, recv2, b)

        def plane_of(c, carry):
            planes = jnp.concatenate(
                [
                    jnp.concatenate(
                        [in2_ref[b, :, c, p, z].reshape(height, breadth) for p in range(2)], axis=1
                    )
                    for z in range(depth)
                ],
                axis=0,
            )
            wide = product(halves(planes), turned_table())
            back_ref[c] = product(plain_table(), halves(spread_blocks(wide)))
            return carry

        lax.fori_loop(0, 3, plane_of, 0)

        for z in range(depth):
            for p in range(2):
                rows, lanes = pl.ds(p * height, height), pl.ds(z * breadth, breadth)
                crossed = cross([back_ref[c, rows, lanes] for c in range(3)], z)
                for c in range(3):
                    theta_ref[p, c, b, z] = -crossed[c]

    drain_all(out2_ref, in2_ref, send2, recv2, bands - 1)
    each_peer(lambda k, peer, source: sums_copy(source, source, k).wait_recv())
    gram_ref[...] = jnp.sum(sums_ref[...], axis=0)
    each_peer(lambda k, peer, source: sums_copy(me, peer, k).wait_send())


def on_device_kernel(coeffs, material, inv_diag, inv_off):
    groups = lax.axis_size("gz")
    _, comps, bands, depth, height, breadth = coeffs.shape
    total = depth * groups
    columns = height // groups
    table = jnp.asarray(split_table(breadth, total**-0.25))
    grams = bands * 4 * bands
    voxels = (bands, 3, 2, total, columns, breadth)
    block = (bands, groups, 3, 2, depth, columns, breadth)
    vmem = pl.BlockSpec(memory_space=pltpu.VMEM)
    hbm = pl.BlockSpec(memory_space=pltpu.HBM)
    dma = pltpu.SemaphoreType.DMA
    theta, sums = pl.pallas_call(
        functools.partial(operator_kernel, groups),
        out_shape=(
            jax.ShapeDtypeStruct(coeffs.shape, single),
            jax.ShapeDtypeStruct((grams, breadth), single),
        ),
        in_specs=[hbm, hbm, hbm, hbm, hbm],
        out_specs=(vmem, vmem),
        scratch_shapes=[
            pltpu.VMEM(coeffs.shape, single),
            pltpu.VMEM(material.shape, jnp.int32),
            pltpu.VMEM(table.shape, half),
            pltpu.SMEM(inv_diag.shape, single),
            pltpu.SMEM(inv_off.shape, single),
            pltpu.VMEM((depth, groups, columns, breadth), jnp.int32),
            pltpu.VMEM((6, groups, depth, columns, breadth), single),
            pltpu.VMEM((3, 2 * height, depth * breadth), half),
            pltpu.VMEM((3, 2 * height, depth * breadth), half),
            pltpu.VMEM((3, 2 * height, depth * breadth), single),
            pltpu.VMEM(voxels, single),
            pltpu.VMEM(voxels, single),
            pltpu.VMEM(voxels, single),
            pltpu.VMEM(block, single),
            pltpu.VMEM(block, single),
            pltpu.VMEM(block, single),
            pltpu.VMEM(block, single),
            pltpu.VMEM((groups, grams, breadth), single),
            dma((5,)),
            dma((groups,)),
            dma((groups,)),
            dma((2,)),
            dma((bands, groups)),
            dma((bands, groups)),
            dma((bands, groups)),
            dma((bands, groups)),
            dma((bands,)),
            dma((bands,)),
            dma((groups,)),
            dma((groups,)),
        ],
        compiler_params=pltpu.CompilerParams(
            collective_id=0, has_side_effects=True, vmem_limit_bytes=56 * 1024 * 1024
        ),
        name="maxwell",
    )(coeffs, material, inv_diag, inv_off, table)
    values = jnp.sum(sums, axis=1) / (breadth * height * total)
    values = values.reshape(bands, 2, bands, 2).transpose(1, 3, 2, 0)
    own, other = values[0], values[1]
    first = lax.axis_index("ba") == 0
    gram = jnp.concatenate([jnp.where(first, own, other), jnp.where(first, other, own)], axis=1)
    return (theta, gram)


def fits(coeffs):
    groups, depth, height, breadth = (
        lax.axis_size("gz"),
        coeffs.shape[3],
        coeffs.shape[4],
        coeffs.shape[5],
    )
    return (
        lax.axis_size("ba") == 2
        and depth == 2
        and height % (8 * groups) == 0
        and height == breadth
        and breadth % 128 == 0
    )


def on_either(coeffs, material, inv_diag, inv_off):
    chosen = on_device_kernel if fits(coeffs) else on_device
    return chosen(coeffs, material, inv_diag, inv_off)


def solution(mesh):
    in_specs = (P(None, None, "ba", "gz", None, None), P("gz", None, None), P(), P())
    out_specs = (P(None, None, "ba", "gz", None, None), P(None, None, "ba"))
    return jax.shard_map(
        on_either, mesh=mesh, in_specs=in_specs, out_specs=out_specs, check_vma=False
    )
```

```python
import functools
import math

import jax
import jax.numpy as jnp
import numpy as np
from jax import lax
from jax.experimental import pallas as pl
from jax.experimental.pallas import tpu as pltpu
from jax.sharding import PartitionSpec as P

highest = lax.Precision.HIGHEST
half_turn = 3.141592653589793


def reverse_bits(values, levels):
    flipped = jnp.zeros_like(values)
    for position in range(levels):
        flipped = flipped + (values >> position & 1) * (1 << levels - 1 - position)
    return flipped


def signed_wave(numbers, length):
    shifted = jnp.where(numbers < length // 2, numbers, numbers - length)
    return shifted.astype(jnp.float32) / (length / 2.0)


def phase_tables(first, second, length, sign):
    product = first[:, None] * second[None, :] % length
    angle = 2.0 * half_turn / length * product.astype(jnp.float32)
    factor = 1.0 / math.sqrt(length)
    return (jnp.cos(angle) * factor, sign * jnp.sin(angle) * factor)


def cross_waves(waves, field):
    first, second, third = waves
    return jnp.stack(
        [
            second * field[:, 2] - third * field[:, 1],
            third * field[:, 0] - first * field[:, 2],
            first * field[:, 1] - second * field[:, 0],
        ],
        axis=1,
    )


def along_width(field, cosine, sine):
    breadth = field.shape[-1]
    rows = field.reshape(2, -1, breadth)
    joined = jnp.concatenate([cosine, sine], axis=1)
    real_prod = jnp.dot(rows[0], joined, precision=highest)
    imag_prod = jnp.dot(rows[1], joined, precision=highest)
    real_out = real_prod[:, :breadth] - imag_prod[:, breadth:]
    imag_out = real_prod[:, breadth:] + imag_prod[:, :breadth]
    return jnp.stack([real_out, imag_out]).reshape(field.shape)


def along_height(field, cosine, sine):
    tables = jnp.stack([cosine, sine])
    product = jnp.einsum("pcbzyx,tyk->tpcbzkx", field, tables, precision=highest)
    return jnp.stack([product[0, 0] - product[1, 1], product[1, 0] + product[0, 1]])


def along_depth(field, cosine, sine):
    tables = jnp.stack([cosine, sine])
    product = jnp.einsum("pcbzyx,tzk->tpcbkyx", field, tables, precision=highest)
    return jnp.stack([product[0, 0] - product[1, 1], product[1, 0] + product[0, 1]])


def apply_material(field, material, inv_diag, inv_off):
    materials = inv_diag.shape[0]
    onehot = (material[None] == jnp.arange(materials, dtype=jnp.int32)[:, None, None, None]).astype(
        jnp.float32
    )
    table = jnp.concatenate([inv_diag, inv_off], axis=1)
    tensor = jnp.einsum("mk,mzyx->kzyx", table, onehot, precision=highest)
    first = field[:, 0]
    second = field[:, 1]
    third = field[:, 2]
    return jnp.stack(
        [
            tensor[0] * first + tensor[3] * second + tensor[5] * third,
            tensor[3] * first + tensor[1] * second + tensor[4] * third,
            tensor[5] * first + tensor[4] * second + tensor[2] * third,
        ],
        axis=1,
    )


def on_device(coeffs, material, inv_diag, inv_off):
    groups = lax.axis_size("gz")
    levels = groups.bit_length() - 1
    depth = coeffs.shape[3]
    height = coeffs.shape[4]
    breadth = coeffs.shape[5]
    total_depth = depth * groups
    device = lax.axis_index("gz")
    local_rows = jnp.arange(depth, dtype=jnp.int32)
    waves_here = reverse_bits(device, levels) + groups * local_rows
    across = jnp.arange(breadth, dtype=jnp.int32)
    upward = jnp.arange(height, dtype=jnp.int32)
    waves = (
        signed_wave(across, breadth)[None, None, :],
        signed_wave(upward, height)[None, :, None],
        signed_wave(waves_here, total_depth)[:, None, None],
    )
    curl = cross_waves(waves, coeffs)
    all_rows = jnp.arange(total_depth, dtype=jnp.int32)
    wave_rows = reverse_bits(all_rows // depth, levels) + groups * (all_rows % depth)
    height_cos, height_sin = phase_tables(upward, upward, height, 1.0)
    width_cos, width_sin = phase_tables(across, across, breadth, 1.0)
    planar = along_height(curl, height_cos, height_sin)
    planar = along_width(planar, width_cos, width_sin)
    material_slab = lax.all_to_all(material, "gz", split_axis=1, concat_axis=0, tiled=True)
    inverse_cos, inverse_sin = phase_tables(wave_rows, all_rows, total_depth, 1.0)
    forward_cos, forward_sin = phase_tables(all_rows, wave_rows, total_depth, -1.0)
    spatial_piece = along_depth(
        lax.all_to_all(planar, "gz", split_axis=4, concat_axis=3, tiled=True),
        inverse_cos,
        inverse_sin,
    )
    scaled_piece = apply_material(spatial_piece, material_slab, inv_diag, inv_off)
    returned = along_depth(scaled_piece, forward_cos, forward_sin)
    spectral = lax.all_to_all(returned, "gz", split_axis=3, concat_axis=4, tiled=True)
    spectral = along_width(spectral, width_cos, -width_sin)
    spectral = along_height(spectral, height_cos, -height_sin)
    theta = -cross_waves(waves, spectral)
    factor = 1.0 / (breadth * height * total_depth)
    piece = lax.all_gather(coeffs, "ba", axis=2, tiled=True)
    real_part = jnp.einsum("cbzyx,cezyx->be", piece[0], theta[0], precision=highest) + jnp.einsum(
        "cbzyx,cezyx->be", piece[1], theta[1], precision=highest
    )
    imag_part = jnp.einsum("cbzyx,cezyx->be", piece[0], theta[1], precision=highest) - jnp.einsum(
        "cbzyx,cezyx->be", piece[1], theta[0], precision=highest
    )
    block = jnp.stack([real_part, imag_part]) * factor
    gram = lax.psum(block, "gz")
    return (theta, gram)


MESH = pl.DeviceIdType.MESH
single = jnp.float32
half = jnp.bfloat16


def split_table(length, extra):
    numbers = np.arange(length)
    angle = 2.0 * np.pi / length * (numbers[:, None] * numbers[None, :] % length)
    cosine = np.cos(angle) * extra / math.sqrt(length)
    sine = np.sin(angle) * extra / math.sqrt(length)
    inverse = np.block([[cosine, sine], [-sine, cosine]])
    parts = []
    for table in (inverse, inverse.T):
        high = table.astype(np.float32).astype(half)
        low = (table - high.astype(np.float64)).astype(half)
        parts += [high, low]
    return np.stack(parts)


def halves(values):
    high = values.astype(half)
    return high, (values - high.astype(single)).astype(half)


def product(first, second):
    dot = functools.partial(jnp.dot, preferred_element_type=single)
    return dot(first[0], second[0]) + (dot(first[0], second[1]) + dot(first[1], second[0]))


def twiddled(pair, step, span, sign):
    real, imag = pair
    if step == 0:
        return real, imag
    if 2 * step == span:
        return (-imag, real) if sign > 0 else (imag, -real)
    angle = math.pi * step / span
    cosine, sine = math.cos(angle), sign * math.sin(angle)
    return real * cosine - imag * sine, real * sine + imag * cosine


def to_voxels(points):
    points = list(points)
    span = 1
    while span < len(points):
        for base in range(0, len(points), 2 * span):
            for step in range(span):
                a = points[base + step]
                t = twiddled(points[base + step + span], step, span, 1.0)
                points[base + step] = (a[0] + t[0], a[1] + t[1])
                points[base + step + span] = (a[0] - t[0], a[1] - t[1])
        span *= 2
    return points


def to_waves(points):
    points = list(points)
    span = len(points) // 2
    while span >= 1:
        for base in range(0, len(points), 2 * span):
            for step in range(span):
                a, t = points[base + step], points[base + step + span]
                points[base + step] = (a[0] + t[0], a[1] + t[1])
                points[base + step + span] = twiddled(
                    (a[0] - t[0], a[1] - t[1]), step, span, -1.0
                )
        span //= 2
    return points


def operator_kernel(
    groups,
    coeffs_hbm,
    material_hbm,
    diag_hbm,
    off_hbm,
    table_hbm,
    theta_ref,
    gram_ref,
    coeffs_ref,
    material_ref,
    table_ref,
    diag_ref,
    off_ref,
    slab_ref,
    tensor_ref,
    high_ref,
    low_ref,
    back_ref,
    field_ref,
    scaled_ref,
    other_ref,
    out1_ref,
    in1_ref,
    out2_ref,
    in2_ref,
    sums_ref,
    load_sem,
    slab_send,
    slab_recv,
    half_sem,
    send1,
    recv1,
    send2,
    recv2,
    other_send,
    other_recv,
    sums_send,
    sums_recv,
):
    _, comps, bands, depth, height, breadth = coeffs_ref.shape
    total = depth * groups
    columns = height // groups
    levels = groups.bit_length() - 1
    me = lax.axis_index("gz")
    mine = lax.axis_index("ba")
    middle = groups // 2

    def offset_of(i):
        away = (i + 1) // 2
        return middle + away - 2 * away * (i % 2)

    def each_peer(body):
        def step(i, carry):
            k = offset_of(i)
            body(k, (me + k) % groups, (me + groups - k) % groups)
            return carry

        lax.fori_loop(0, groups - 1, step, 0)

    barrier = pltpu.get_barrier_semaphore()
    each_peer(
        lambda k, peer, source: pl.semaphore_signal(
            barrier, inc=1, device_id={"gz": peer}, device_id_type=MESH
        )
    )
    pl.semaphore_signal(barrier, inc=1, device_id={"ba": 1 - mine}, device_id_type=MESH)

    loads = [
        pltpu.make_async_copy(coeffs_hbm, coeffs_ref, load_sem.at[0]),
        pltpu.make_async_copy(table_hbm, table_ref, load_sem.at[1]),
        pltpu.make_async_copy(material_hbm, material_ref, load_sem.at[2]),
        pltpu.make_async_copy(diag_hbm, diag_ref, load_sem.at[3]),
        pltpu.make_async_copy(off_hbm, off_ref, load_sem.at[4]),
    ]
    for load in loads:
        load.start()

    across = lax.broadcasted_iota(jnp.int32, (1, breadth), 1)
    upward = lax.broadcasted_iota(jnp.int32, (height, 1), 0)
    wave_x = jnp.where(across < breadth // 2, across, across - breadth).astype(single) / (
        breadth / 2.0
    )
    wave_y = jnp.where(upward < height // 2, upward, upward - height).astype(single) / (
        height / 2.0
    )
    reversed_me = 0
    for position in range(levels):
        reversed_me = reversed_me + (me // (1 << position)) % 2 * (1 << (levels - 1 - position))
    waves_z = []
    for row in range(depth):
        number = reversed_me + groups * row
        signed = number - total * (number // (total // 2))
        waves_z.append(signed.astype(single) / (total / 2.0))

    def cross(parts, row):
        waves = (wave_x, wave_y, waves_z[row])
        return [
            waves[(c + 1) % 3] * parts[(c + 2) % 3] - waves[(c + 2) % 3] * parts[(c + 1) % 3]
            for c in range(3)
        ]

    def plain_table():
        return table_ref[0], table_ref[1]

    def turned_table():
        return table_ref[2], table_ref[3]

    def gather_blocks(values):
        top, bottom = values[:height], values[height:]
        return jnp.concatenate(
            [
                jnp.concatenate(
                    [
                        top[:, z * breadth : (z + 1) * breadth],
                        bottom[:, z * breadth : (z + 1) * breadth],
                    ],
                    axis=1,
                )
                for z in range(depth)
            ],
            axis=0,
        )

    def spread_blocks(values):
        return jnp.concatenate(
            [
                jnp.concatenate(
                    [
                        values[z * height : (z + 1) * height, p * breadth : (p + 1) * breadth]
                        for z in range(depth)
                    ],
                    axis=1,
                )
                for p in range(2)
            ],
            axis=0,
        )

    def make_planes(b):
        for p in range(2):
            for z in range(depth):
                curls = cross([coeffs_ref[p, c, b, z] for c in range(3)], z)
                for c in range(3):
                    high, low = halves(curls[c])
                    rows, lanes = pl.ds(p * height, height), pl.ds(z * breadth, breadth)
                    high_ref[c, rows, lanes] = high
                    low_ref[c, rows, lanes] = low

        def one(c, carry):
            tall = product(turned_table(), (high_ref[c], low_ref[c]))
            wide = product(halves(gather_blocks(tall)), plain_table())
            for p in range(2):
                for z in range(depth):
                    plane = wide[z * height : (z + 1) * height, p * breadth : (p + 1) * breadth]
                    out1_ref[b, :, c, p, z] = plane.reshape(groups, columns, breadth)
            return carry

        lax.fori_loop(0, 3, one, 0)

    def exchange(out, into, send, recv, b, peer, k):
        return pltpu.make_async_remote_copy(
            src_ref=out.at[b, peer],
            dst_ref=into.at[b, me],
            send_sem=send.at[b, k],
            recv_sem=recv.at[b, k],
            device_id={"gz": peer},
            device_id_type=MESH,
        )

    def arrival(out, into, send, recv, b, source, k):
        return pltpu.make_async_remote_copy(
            src_ref=out.at[b, source],
            dst_ref=into.at[b, source],
            send_sem=send.at[b, k],
            recv_sem=recv.at[b, k],
            device_id={"gz": source},
            device_id_type=MESH,
        )

    def start_all(out, into, send, recv, b):
        each_peer(lambda k, peer, source: exchange(out, into, send, recv, b, peer, k).start())
        into[b, me] = out[b, me]

    def finish_all(out, into, send, recv, b):
        each_peer(
            lambda k, peer, source: arrival(out, into, send, recv, b, source, k).wait_recv()
        )

    def drain_all(out, into, send, recv, b):
        each_peer(lambda k, peer, source: exchange(out, into, send, recv, b, peer, k).wait_send())

    def columns_of(peer):
        return pl.ds(pl.multiple_of(peer * columns, columns), columns)

    def slab_copy(peer, slot, k):
        return pltpu.make_async_remote_copy(
            src_ref=material_ref.at[mine, columns_of(peer), :],
            dst_ref=slab_ref.at[mine, slot],
            send_sem=slab_send.at[k],
            recv_sem=slab_recv.at[k],
            device_id={"gz": peer},
            device_id_type=MESH,
        )

    def half_copy(row):
        return pltpu.make_async_remote_copy(
            src_ref=slab_ref.at[row],
            dst_ref=slab_ref.at[row],
            send_sem=half_sem.at[0],
            recv_sem=half_sem.at[1],
            device_id={"ba": 1 - mine},
            device_id_type=MESH,
        )

    def other_copy(b):
        return pltpu.make_async_remote_copy(
            src_ref=field_ref.at[b],
            dst_ref=other_ref.at[b],
            send_sem=other_send.at[b],
            recv_sem=other_recv.at[b],
            device_id={"ba": 1 - mine},
            device_id_type=MESH,
        )

    loads[0].wait()
    loads[1].wait()
    make_planes(0)
    for load in loads[2:]:
        load.wait()
    pl.semaphore_wait(barrier, groups)
    start_all(out1_ref, in1_ref, send1, recv1, 0)
    each_peer(lambda k, peer, source: slab_copy(peer, me, k).start())
    slab_ref[mine, me] = material_ref[mine, columns_of(me), :]
    for b in range(1, bands):
        make_planes(b)
        start_all(out1_ref, in1_ref, send1, recv1, b)

    each_peer(lambda k, peer, source: slab_copy(source, source, k).wait_recv())
    half_copy(mine).start()
    half_copy(1 - mine).wait_recv()
    kinds = diag_ref.shape[0]
    for row in range(depth):
        codes = slab_ref[row]
        for entry in range(6):
            table = diag_ref if entry < 3 else off_ref
            values = jnp.full(codes.shape, table[0, entry % 3], single)
            for kind in range(1, kinds):
                values = jnp.where(codes == kind, table[kind, entry % 3], values)
            tensor_ref[entry, :, row] = values

    for b in range(bands):
        finish_all(out1_ref, in1_ref, send1, recv1, b)

        def inverse(c, carry):
            points = [
                (in1_ref[b, r // depth, c, 0, r % depth], in1_ref[b, r // depth, c, 1, r % depth])
                for r in range(total)
            ]
            for z, (real, imag) in enumerate(to_voxels(points)):
                field_ref[b, c, 0, z] = real
                field_ref[b, c, 1, z] = imag
            return carry

        lax.fori_loop(0, 3, inverse, 0)
        other_copy(b).start()

        def scale(z, carry):
            xx, yy, zz, xy, yz, zx = [
                tensor_ref[entry, z // depth, z % depth] for entry in range(6)
            ]
            for p in range(2):
                first, second, third = [field_ref[b, c, p, z] for c in range(3)]
                scaled_ref[b, 0, p, z] = xx * first + xy * second + zx * third
                scaled_ref[b, 1, p, z] = xy * first + yy * second + yz * third
                scaled_ref[b, 2, p, z] = zx * first + yz * second + zz * third
            return carry

        lax.fori_loop(0, total, scale, 0, unroll=4)

        def forward(c, carry):
            points = [(scaled_ref[b, c, 0, z], scaled_ref[b, c, 1, z]) for z in range(total)]
            for r, (real, imag) in enumerate(to_waves(points)):
                out2_ref[b, r // depth, c, 0, r % depth] = real
                out2_ref[b, r // depth, c, 1, r % depth] = imag
            return carry

        lax.fori_loop(0, 3, forward, 0)
        start_all(out2_ref, in2_ref, send2, recv2, b)

    def sums_copy(slot, peer, k):
        return pltpu.make_async_remote_copy(
            src_ref=sums_ref.at[slot],
            dst_ref=sums_ref.at[slot],
            send_sem=sums_send.at[k],
            recv_sem=sums_recv.at[k],
            device_id={"gz": peer},
            device_id_type=MESH,
        )

    def make_sums():
        def add(z, sums):
            sums = list(sums)
            for c in range(3):
                ours = [(scaled_ref[b, c, 0, z], scaled_ref[b, c, 1, z]) for b in range(bands)]
                fields = [
                    (source[a, c, 0, z], source[a, c, 1, z])
                    for source in (field_ref, other_ref)
                    for a in range(bands)
                ]
                n = 0
                for t_real, t_imag in ours:
                    for real, imag in fields:
                        sums[n] = sums[n] + (real * t_real + imag * t_imag)
                        sums[n + 1] = sums[n + 1] + (real * t_imag - imag * t_real)
                        n += 2
            return tuple(sums)

        zero = jnp.zeros((columns, breadth), single)
        sums = lax.fori_loop(0, total, add, (zero,) * (4 * bands * bands))
        sums_ref[me] = jnp.concatenate([jnp.sum(v, axis=0, keepdims=True) for v in sums], axis=0)

    half_copy(mine).wait_send()
    each_peer(lambda k, peer, source: slab_copy(peer, me, k).wait_send())
    for b in range(bands):
        drain_all(out1_ref, in1_ref, send1, recv1, b)

    for b in range(bands):
        if b == bands - 1:
            for a in range(bands):
                other_copy(a).wait_send()
                other_copy(a).wait_recv()
            make_sums()
            each_peer(lambda k, peer, source: sums_copy(me, peer, k).start())
            for a in range(b):
                drain_all(out2_ref, in2_ref, send2, recv2, a)
        finish_all(out2_ref, in2_ref, send2, recv2, b)

        def plane_of(c, carry):
            planes = jnp.concatenate(
                [
                    jnp.concatenate(
                        [in2_ref[b, :, c, p, z].reshape(height, breadth) for p in range(2)], axis=1
                    )
                    for z in range(depth)
                ],
                axis=0,
            )
            wide = product(halves(planes), turned_table())
            back_ref[c] = product(plain_table(), halves(spread_blocks(wide)))
            return carry

        lax.fori_loop(0, 3, plane_of, 0)

        for z in range(depth):
            for p in range(2):
                rows, lanes = pl.ds(p * height, height), pl.ds(z * breadth, breadth)
                crossed = cross([back_ref[c, rows, lanes] for c in range(3)], z)
                for c in range(3):
                    theta_ref[p, c, b, z] = -crossed[c]

    drain_all(out2_ref, in2_ref, send2, recv2, bands - 1)
    each_peer(lambda k, peer, source: sums_copy(source, source, k).wait_recv())
    gram_ref[...] = jnp.sum(sums_ref[...], axis=0)
    each_peer(lambda k, peer, source: sums_copy(me, peer, k).wait_send())


def on_device_kernel(coeffs, material, inv_diag, inv_off):
    groups = lax.axis_size("gz")
    _, comps, bands, depth, height, breadth = coeffs.shape
    total = depth * groups
    columns = height // groups
    table = jnp.asarray(split_table(breadth, total**-0.25))
    grams = bands * 4 * bands
    voxels = (bands, 3, 2, total, columns, breadth)
    block = (bands, groups, 3, 2, depth, columns, breadth)
    vmem = pl.BlockSpec(memory_space=pltpu.VMEM)
    hbm = pl.BlockSpec(memory_space=pltpu.HBM)
    dma = pltpu.SemaphoreType.DMA
    coeffs, material, inv_diag, inv_off, table = [pltpu.with_memory_space_constraint(v, pltpu.HBM) for v in (coeffs, material, inv_diag, inv_off, table)]
    theta, sums = pl.pallas_call(
        functools.partial(operator_kernel, groups),
        out_shape=(
            jax.ShapeDtypeStruct(coeffs.shape, single),
            jax.ShapeDtypeStruct((grams, breadth), single),
        ),
        in_specs=[hbm, hbm, hbm, hbm, hbm],
        out_specs=(vmem, vmem),
        scratch_shapes=[
            pltpu.VMEM(coeffs.shape, single),
            pltpu.VMEM(material.shape, jnp.int32),
            pltpu.VMEM(table.shape, half),
            pltpu.SMEM(inv_diag.shape, single),
            pltpu.SMEM(inv_off.shape, single),
            pltpu.VMEM((depth, groups, columns, breadth), jnp.int32),
            pltpu.VMEM((6, groups, depth, columns, breadth), single),
            pltpu.VMEM((3, 2 * height, depth * breadth), half),
            pltpu.VMEM((3, 2 * height, depth * breadth), half),
            pltpu.VMEM((3, 2 * height, depth * breadth), single),
            pltpu.VMEM(voxels, single),
            pltpu.VMEM(voxels, single),
            pltpu.VMEM(voxels, single),
            pltpu.VMEM(block, single),
            pltpu.VMEM(block, single),
            pltpu.VMEM(block, single),
            pltpu.VMEM(block, single),
            pltpu.VMEM((groups, grams, breadth), single),
            dma((5,)),
            dma((groups,)),
            dma((groups,)),
            dma((2,)),
            dma((bands, groups)),
            dma((bands, groups)),
            dma((bands, groups)),
            dma((bands, groups)),
            dma((bands,)),
            dma((bands,)),
            dma((groups,)),
            dma((groups,)),
        ],
        compiler_params=pltpu.CompilerParams(
            collective_id=0, has_side_effects=True, vmem_limit_bytes=48 * 1024 * 1024
        ),
        name="maxwell",
    )(coeffs, material, inv_diag, inv_off, table)
    values = jnp.sum(sums, axis=1) / (breadth * height * total)
    values = values.reshape(bands, 2, bands, 2).transpose(1, 3, 2, 0)
    own, other = values[0], values[1]
    first = lax.axis_index("ba") == 0
    gram = jnp.concatenate([jnp.where(first, own, other), jnp.where(first, other, own)], axis=1)
    return (theta, gram)


def fits(coeffs):
    groups, depth, height, breadth = (
        lax.axis_size("gz"),
        coeffs.shape[3],
        coeffs.shape[4],
        coeffs.shape[5],
    )
    return (
        lax.axis_size("ba") == 2
        and depth == 2
        and height % (8 * groups) == 0
        and height == breadth
        and breadth % 128 == 0
    )


def on_either(coeffs, material, inv_diag, inv_off):
    chosen = on_device_kernel if fits(coeffs) else on_device
    return chosen(coeffs, material, inv_diag, inv_off)


def solution(mesh):
    in_specs = (P(None, None, "ba", "gz", None, None), P("gz", None, None), P(), P())
    out_specs = (P(None, None, "ba", "gz", None, None), P(None, None, "ba"))
    return jax.shard_map(
        on_either, mesh=mesh, in_specs=in_specs, out_specs=out_specs, check_vma=False
    )
```

```python
import functools
import math

import jax
import jax.numpy as jnp
import numpy as np
from jax import lax
from jax.experimental import pallas as pl
from jax.experimental.pallas import tpu as pltpu
from jax.sharding import PartitionSpec as P

highest = lax.Precision.HIGHEST
half_turn = 3.141592653589793


def reverse_bits(values, levels):
    flipped = jnp.zeros_like(values)
    for position in range(levels):
        flipped = flipped + (values >> position & 1) * (1 << levels - 1 - position)
    return flipped


def signed_wave(numbers, length):
    shifted = jnp.where(numbers < length // 2, numbers, numbers - length)
    return shifted.astype(jnp.float32) / (length / 2.0)


def phase_tables(first, second, length, sign):
    product = first[:, None] * second[None, :] % length
    angle = 2.0 * half_turn / length * product.astype(jnp.float32)
    factor = 1.0 / math.sqrt(length)
    return (jnp.cos(angle) * factor, sign * jnp.sin(angle) * factor)


def cross_waves(waves, field):
    first, second, third = waves
    return jnp.stack(
        [
            second * field[:, 2] - third * field[:, 1],
            third * field[:, 0] - first * field[:, 2],
            first * field[:, 1] - second * field[:, 0],
        ],
        axis=1,
    )


def along_width(field, cosine, sine):
    breadth = field.shape[-1]
    rows = field.reshape(2, -1, breadth)
    joined = jnp.concatenate([cosine, sine], axis=1)
    real_prod = jnp.dot(rows[0], joined, precision=highest)
    imag_prod = jnp.dot(rows[1], joined, precision=highest)
    real_out = real_prod[:, :breadth] - imag_prod[:, breadth:]
    imag_out = real_prod[:, breadth:] + imag_prod[:, :breadth]
    return jnp.stack([real_out, imag_out]).reshape(field.shape)


def along_height(field, cosine, sine):
    tables = jnp.stack([cosine, sine])
    product = jnp.einsum("pcbzyx,tyk->tpcbzkx", field, tables, precision=highest)
    return jnp.stack([product[0, 0] - product[1, 1], product[1, 0] + product[0, 1]])


def along_depth(field, cosine, sine):
    tables = jnp.stack([cosine, sine])
    product = jnp.einsum("pcbzyx,tzk->tpcbkyx", field, tables, precision=highest)
    return jnp.stack([product[0, 0] - product[1, 1], product[1, 0] + product[0, 1]])


def apply_material(field, material, inv_diag, inv_off):
    materials = inv_diag.shape[0]
    onehot = (material[None] == jnp.arange(materials, dtype=jnp.int32)[:, None, None, None]).astype(
        jnp.float32
    )
    table = jnp.concatenate([inv_diag, inv_off], axis=1)
    tensor = jnp.einsum("mk,mzyx->kzyx", table, onehot, precision=highest)
    first = field[:, 0]
    second = field[:, 1]
    third = field[:, 2]
    return jnp.stack(
        [
            tensor[0] * first + tensor[3] * second + tensor[5] * third,
            tensor[3] * first + tensor[1] * second + tensor[4] * third,
            tensor[5] * first + tensor[4] * second + tensor[2] * third,
        ],
        axis=1,
    )


def on_device(coeffs, material, inv_diag, inv_off):
    groups = lax.axis_size("gz")
    levels = groups.bit_length() - 1
    depth = coeffs.shape[3]
    height = coeffs.shape[4]
    breadth = coeffs.shape[5]
    total_depth = depth * groups
    device = lax.axis_index("gz")
    local_rows = jnp.arange(depth, dtype=jnp.int32)
    waves_here = reverse_bits(device, levels) + groups * local_rows
    across = jnp.arange(breadth, dtype=jnp.int32)
    upward = jnp.arange(height, dtype=jnp.int32)
    waves = (
        signed_wave(across, breadth)[None, None, :],
        signed_wave(upward, height)[None, :, None],
        signed_wave(waves_here, total_depth)[:, None, None],
    )
    curl = cross_waves(waves, coeffs)
    all_rows = jnp.arange(total_depth, dtype=jnp.int32)
    wave_rows = reverse_bits(all_rows // depth, levels) + groups * (all_rows % depth)
    height_cos, height_sin = phase_tables(upward, upward, height, 1.0)
    width_cos, width_sin = phase_tables(across, across, breadth, 1.0)
    planar = along_height(curl, height_cos, height_sin)
    planar = along_width(planar, width_cos, width_sin)
    material_slab = lax.all_to_all(material, "gz", split_axis=1, concat_axis=0, tiled=True)
    inverse_cos, inverse_sin = phase_tables(wave_rows, all_rows, total_depth, 1.0)
    forward_cos, forward_sin = phase_tables(all_rows, wave_rows, total_depth, -1.0)
    spatial_piece = along_depth(
        lax.all_to_all(planar, "gz", split_axis=4, concat_axis=3, tiled=True),
        inverse_cos,
        inverse_sin,
    )
    scaled_piece = apply_material(spatial_piece, material_slab, inv_diag, inv_off)
    returned = along_depth(scaled_piece, forward_cos, forward_sin)
    spectral = lax.all_to_all(returned, "gz", split_axis=3, concat_axis=4, tiled=True)
    spectral = along_width(spectral, width_cos, -width_sin)
    spectral = along_height(spectral, height_cos, -height_sin)
    theta = -cross_waves(waves, spectral)
    factor = 1.0 / (breadth * height * total_depth)
    piece = lax.all_gather(coeffs, "ba", axis=2, tiled=True)
    real_part = jnp.einsum("cbzyx,cezyx->be", piece[0], theta[0], precision=highest) + jnp.einsum(
        "cbzyx,cezyx->be", piece[1], theta[1], precision=highest
    )
    imag_part = jnp.einsum("cbzyx,cezyx->be", piece[0], theta[1], precision=highest) - jnp.einsum(
        "cbzyx,cezyx->be", piece[1], theta[0], precision=highest
    )
    block = jnp.stack([real_part, imag_part]) * factor
    gram = lax.psum(block, "gz")
    return (theta, gram)


MESH = pl.DeviceIdType.MESH
single = jnp.float32
half = jnp.bfloat16


def split_table(length, extra):
    numbers = np.arange(length)
    angle = 2.0 * np.pi / length * (numbers[:, None] * numbers[None, :] % length)
    cosine = np.cos(angle) * extra / math.sqrt(length)
    sine = np.sin(angle) * extra / math.sqrt(length)
    inverse = np.block([[cosine, sine], [-sine, cosine]])
    parts = []
    for table in (inverse, inverse.T):
        high = table.astype(np.float32).astype(half)
        low = (table - high.astype(np.float64)).astype(half)
        parts += [high, low]
    return np.stack(parts)


def halves(values):
    high = values.astype(half)
    return high, (values - high.astype(single)).astype(half)


def product(first, second):
    dot = functools.partial(jnp.dot, preferred_element_type=single)
    return dot(first[0], second[0]) + (dot(first[0], second[1]) + dot(first[1], second[0]))


def twiddled(pair, step, span, sign):
    real, imag = pair
    if step == 0:
        return real, imag
    if 2 * step == span:
        return (-imag, real) if sign > 0 else (imag, -real)
    angle = math.pi * step / span
    cosine, sine = math.cos(angle), sign * math.sin(angle)
    return real * cosine - imag * sine, real * sine + imag * cosine


def to_voxels(points):
    points = list(points)
    span = 1
    while span < len(points):
        for base in range(0, len(points), 2 * span):
            for step in range(span):
                a = points[base + step]
                t = twiddled(points[base + step + span], step, span, 1.0)
                points[base + step] = (a[0] + t[0], a[1] + t[1])
                points[base + step + span] = (a[0] - t[0], a[1] - t[1])
        span *= 2
    return points


def to_waves(points):
    points = list(points)
    span = len(points) // 2
    while span >= 1:
        for base in range(0, len(points), 2 * span):
            for step in range(span):
                a, t = points[base + step], points[base + step + span]
                points[base + step] = (a[0] + t[0], a[1] + t[1])
                points[base + step + span] = twiddled(
                    (a[0] - t[0], a[1] - t[1]), step, span, -1.0
                )
        span //= 2
    return points


def operator_kernel(
    groups,
    coeffs_hbm,
    material_hbm,
    diag_hbm,
    off_hbm,
    table_hbm,
    theta_ref,
    gram_ref,
    coeffs_ref,
    material_ref,
    table_ref,
    diag_ref,
    off_ref,
    slab_ref,
    tensor_ref,
    high_ref,
    low_ref,
    back_ref,
    pair_ref,
    other_ref,
    swap_ref,
    result_ref,
    return_ref,
    out1_ref,
    in1_ref,
    field_ref,
    scaled_ref,
    out2_ref,
    in2_ref,
    sums_ref,
    load_sem,
    slab_send,
    slab_recv,
    half_sem,
    send1,
    recv1,
    send2,
    recv2,
    swap_send,
    swap_recv,
    return_send,
    return_recv,
    other_send,
    other_recv,
    sums_send,
    sums_recv,
):
    _, comps, bands, depth, height, breadth = coeffs_ref.shape
    total = depth * groups
    members = groups // 2
    columns = height // members
    levels = groups.bit_length() - 1
    me = lax.axis_index("gz")
    mine = lax.axis_index("ba")
    side = me // members
    seat = me % members
    partner = (me + members) % groups
    mate = {"ba": 1 - mine}
    step_rows = 16
    steps = height // step_rows

    def each_peer(body):
        def step(k, carry):
            body(k, (me + k) % groups, (me + groups - k) % groups)
            return carry

        lax.fori_loop(1, groups, step, 0)

    def each_member(body):
        def step(k, carry):
            body(k, (seat + k) % members, (seat + members - k) % members)
            return carry

        lax.fori_loop(1, members, step, 0)

    barrier = pltpu.get_barrier_semaphore()
    each_peer(
        lambda k, peer, source: pl.semaphore_signal(
            barrier, inc=1, device_id={"gz": peer}, device_id_type=MESH
        )
    )
    pl.semaphore_signal(barrier, inc=1, device_id=mate, device_id_type=MESH)

    def band_load(b, n):
        return pltpu.make_async_copy(
            coeffs_hbm.at[:, :, b], coeffs_ref.at[:, :, b], load_sem.at[n]
        )

    loads = [
        band_load(1 - side, 0),
        band_load(side, 1),
        pltpu.make_async_copy(table_hbm, table_ref, load_sem.at[2]),
        pltpu.make_async_copy(material_hbm, material_ref, load_sem.at[3]),
        pltpu.make_async_copy(diag_hbm, diag_ref, load_sem.at[4]),
        pltpu.make_async_copy(off_hbm, off_ref, load_sem.at[5]),
    ]
    for load in loads:
        load.start()

    def signed(number, length):
        return number - length * (number // (length // 2))

    def row_number(owner, row):
        reversed_owner = 0
        for position in range(levels):
            bit = (owner // (1 << position)) % 2
            reversed_owner = reversed_owner + bit * (1 << (levels - 1 - position))
        return signed(reversed_owner + groups * row, total)

    def inverse_of(values):
        zero = values == 0
        return jnp.where(zero, 0.0, 1.0 / jnp.where(zero, 1, values).astype(single))

    class Waves:
        def __init__(self, owner, row, i):
            shape = (step_rows, breadth)
            nx = lax.broadcasted_iota(jnp.int32, shape, 1)
            ny = lax.broadcasted_iota(jnp.int32, shape, 0) + i * step_rows
            nx = jnp.where(nx < breadth // 2, nx, nx - breadth)
            ny = jnp.where(ny < height // 2, ny, ny - height)
            nz = jnp.full(shape, row_number(owner, row), jnp.int32)
            self.x = nx.astype(single) / (breadth / 2.0)
            self.y = ny.astype(single) / (height / 2.0)
            self.z = nz.astype(single) / (total / 2.0)
            ax, ay, az = jnp.abs(nx) * total, jnp.abs(ny) * total, jnp.abs(nz) * breadth
            self.is_x = (ax >= ay) & (ax >= az)
            self.is_y = ay >= az
            self.numbers = (nx, ny, nz)

        def cross(self, v):
            q = (self.x, self.y, self.z)
            return [
                q[(c + 1) % 3] * v[(c + 2) % 3] - q[(c + 2) % 3] * v[(c + 1) % 3]
                for c in range(3)
            ]

        def pick(self, first, second, third):
            return jnp.where(self.is_x, first, jnp.where(self.is_y, second, third))

        def inverse(self):
            nx, ny, nz = self.numbers
            scaled = self.pick(nx * total, ny * total, nz * breadth)
            return inverse_of(scaled) * (total * breadth / 2.0)

        def ratios(self):
            inverse = self.inverse()
            return (
                self.pick(self.y, self.z, self.x) * inverse,
                self.pick(self.z, self.x, self.y) * inverse,
            )

        def reduce(self, v):
            return self.pick(v[1], v[2], v[0]), self.pick(v[2], v[0], v[1])

        def rebuild(self, ratios, first, second):
            last = -(ratios[0] * first + ratios[1] * second)
            return [
                self.pick(last, second, first),
                self.pick(first, last, second),
                self.pick(second, first, last),
            ]

    def rows_of(i):
        return pl.ds(pl.multiple_of(i * step_rows, step_rows), step_rows)

    def each_step(body):
        def step(n, carry):
            body(n // steps, n % steps)
            return carry

        lax.fori_loop(0, depth * steps, step, 0)

    def put_halves(curls, p, row, i):
        at = pl.ds(pl.multiple_of(p * height + i * step_rows, step_rows), step_rows)
        lanes = pl.ds(pl.multiple_of(row * breadth, breadth), breadth)
        for c in range(3):
            high, low = halves(curls[c])
            high_ref[c, at, lanes] = high
            low_ref[c, at, lanes] = low

    def put_pair(b, p, row, i, pair):
        for n in range(2):
            pair_ref[b, row, n, p, rows_of(i), :] = pair[n]

    def away_step(row, i):
        waves = Waves(me, row, i)
        for p in range(2):
            values = [coeffs_ref[p, c, 1 - side, row, rows_of(i), :] for c in range(3)]
            put_pair(1 - side, p, row, i, waves.reduce(waves.cross(values)))

    def home_step(row, i):
        waves = Waves(me, row, i)
        for p in range(2):
            values = [coeffs_ref[p, c, side, row, rows_of(i), :] for c in range(3)]
            curls = waves.cross(values)
            put_halves(curls, p, row, i)
            put_pair(side, p, row, i, waves.reduce(curls))

    def guest_step(row, i):
        waves = Waves(partner, row, i)
        ratios = waves.ratios()
        for p in range(2):
            pair = [swap_ref[row, n, p, rows_of(i), :] for n in range(2)]
            put_halves(waves.rebuild(ratios, *pair), p, row, i)

    def plain_table():
        return table_ref[0], table_ref[1]

    def turned_table():
        return table_ref[2], table_ref[3]

    def gather_blocks(values):
        top, bottom = values[:height], values[height:]
        return jnp.concatenate(
            [
                jnp.concatenate(
                    [
                        top[:, z * breadth : (z + 1) * breadth],
                        bottom[:, z * breadth : (z + 1) * breadth],
                    ],
                    axis=1,
                )
                for z in range(depth)
            ],
            axis=0,
        )

    def spread_blocks(values):
        return jnp.concatenate(
            [
                jnp.concatenate(
                    [
                        values[z * height : (z + 1) * height, p * breadth : (p + 1) * breadth]
                        for z in range(depth)
                    ],
                    axis=1,
                )
                for p in range(2)
            ],
            axis=0,
        )

    def to_peer(out, into, send, recv, s, c, k, peer, from_at, to_at):
        return pltpu.make_async_remote_copy(
            src_ref=out.at[from_at, peer, c],
            dst_ref=into.at[to_at, seat, c],
            send_sem=send.at[s, c, k],
            recv_sem=recv.at[s, c, k],
            device_id={"gz": side * members + peer},
            device_id_type=MESH,
        )

    def from_peer(out, into, send, recv, s, c, k, source, from_at, to_at):
        return pltpu.make_async_remote_copy(
            src_ref=out.at[from_at, source, c],
            dst_ref=into.at[to_at, source, c],
            send_sem=send.at[s, c, k],
            recv_sem=recv.at[s, c, k],
            device_id={"gz": side * members + source},
            device_id_type=MESH,
        )

    def ends1(s):
        return s, (side + s) % 2

    def ends2(s):
        return (side + s) % 2, s

    def start_all(out, into, send, recv, s, c, ends):
        each_member(
            lambda k, peer, source: to_peer(
                out, into, send, recv, s, c, k, peer, *ends
            ).start()
        )
        into[ends[1], seat, c] = out[ends[0], seat, c]

    def finish_all(out, into, send, recv, s, c, ends):
        each_member(
            lambda k, peer, source: from_peer(
                out, into, send, recv, s, c, k, source, *ends
            ).wait_recv()
        )

    def drain_all(out, into, send, recv, s, c, ends):
        each_member(
            lambda k, peer, source: to_peer(
                out, into, send, recv, s, c, k, peer, *ends
            ).wait_send()
        )

    first = (out1_ref, in1_ref, send1, recv1)
    second = (out2_ref, in2_ref, send2, recv2)

    def make_planes(s):
        def one(c, carry):
            tall = product(turned_table(), (high_ref[c], low_ref[c]))
            wide = product(halves(gather_blocks(tall)), plain_table())
            for p in range(2):
                for z in range(depth):
                    plane = wide[z * height : (z + 1) * height, p * breadth : (p + 1) * breadth]
                    out1_ref[s, :, c, p, z] = plane.reshape(members, columns, breadth)
            start_all(*first, s, c, ends1(s))
            return carry

        lax.fori_loop(0, 3, one, 0)

    def swap_copy(row):
        return pltpu.make_async_remote_copy(
            src_ref=pair_ref.at[1 - side, row],
            dst_ref=swap_ref.at[row],
            send_sem=swap_send.at[row],
            recv_sem=swap_recv.at[row],
            device_id={"gz": partner},
            device_id_type=MESH,
        )

    def return_copy(row):
        return pltpu.make_async_remote_copy(
            src_ref=result_ref.at[row],
            dst_ref=return_ref.at[row],
            send_sem=return_send.at[row],
            recv_sem=return_recv.at[row],
            device_id={"gz": partner},
            device_id_type=MESH,
        )

    def other_copy(b, n):
        return pltpu.make_async_remote_copy(
            src_ref=pair_ref.at[b],
            dst_ref=other_ref.at[b],
            send_sem=other_send.at[n],
            recv_sem=other_recv.at[n],
            device_id=mate,
            device_id_type=MESH,
        )

    def columns_of(peer):
        return pl.ds(pl.multiple_of((peer % members) * columns, columns), columns)

    def slab_copy(peer, slot, k):
        return pltpu.make_async_remote_copy(
            src_ref=material_ref.at[mine, columns_of(peer), :],
            dst_ref=slab_ref.at[mine, slot],
            send_sem=slab_send.at[k],
            recv_sem=slab_recv.at[k],
            device_id={"gz": peer},
            device_id_type=MESH,
        )

    def half_copy(row):
        return pltpu.make_async_remote_copy(
            src_ref=slab_ref.at[row],
            dst_ref=slab_ref.at[row],
            send_sem=half_sem.at[0],
            recv_sem=half_sem.at[1],
            device_id=mate,
            device_id_type=MESH,
        )

    loads[0].wait()
    each_step(away_step)
    pl.semaphore_wait(barrier, groups)
    swap_copy(0).start()
    other_copy(1 - side, 0).start()
    loads[1].wait()
    each_step(home_step)
    other_copy(side, 1).start()
    loads[2].wait()
    make_planes(0)
    swap_copy(1).start()
    for load in loads[3:]:
        load.wait()
    each_peer(lambda k, peer, source: slab_copy(peer, me, k).start())
    slab_ref[mine, me] = material_ref[mine, columns_of(me), :]

    for row in range(depth):
        swap_copy(row).wait_recv()
    each_step(guest_step)
    make_planes(1)

    each_peer(lambda k, peer, source: slab_copy(source, source, k).wait_recv())
    half_copy(mine).start()
    half_copy(1 - mine).wait_recv()
    kinds = diag_ref.shape[0]

    def tensor_step(owner, carry):
        for row in range(depth):
            codes = slab_ref[row, owner]
            for entry in range(6):
                table = diag_ref if entry < 3 else off_ref
                values = jnp.full(codes.shape, table[0, entry % 3], single)
                for kind in range(1, kinds):
                    values = jnp.where(codes == kind, table[kind, entry % 3], values)
                tensor_ref[entry, owner, row] = values
        return carry

    lax.fori_loop(0, groups, tensor_step, 0)

    def part_of(n):
        return pl.ds(pl.multiple_of(n * 8, 8), 8)

    def inverse(c, carry):
        for s in range(2):
            finish_all(*first, s, c, ends1(s))

        def part(n, carry):
            points = []
            for r in range(total):
                owner, row = r // depth, r % depth
                at = (owner // members, owner % members, c)
                points.append(
                    (in1_ref[(*at, 0, row, part_of(n))], in1_ref[(*at, 1, row, part_of(n))])
                )
            for z, (real, imag) in enumerate(to_voxels(points)):
                field_ref[c, 0, z, part_of(n)] = real
                field_ref[c, 1, z, part_of(n)] = imag
            return carry

        return lax.fori_loop(0, columns // 8, part, carry)

    lax.fori_loop(0, 3, inverse, 0)

    def scale(z, carry):
        xx, yy, zz, xy, yz, zx = [tensor_ref[entry, z // depth, z % depth] for entry in range(6)]
        for p in range(2):
            fx, fy, fz = [field_ref[c, p, z] for c in range(3)]
            scaled_ref[0, p, z] = xx * fx + xy * fy + zx * fz
            scaled_ref[1, p, z] = xy * fx + yy * fy + yz * fz
            scaled_ref[2, p, z] = zx * fx + yz * fy + zz * fz
        return carry

    lax.fori_loop(0, total, scale, 0, unroll=2)

    def forward(c, carry):
        def part(n, carry):
            points = [
                (scaled_ref[c, 0, z, part_of(n)], scaled_ref[c, 1, z, part_of(n)])
                for z in range(total)
            ]
            for r, (real, imag) in enumerate(to_waves(points)):
                owner, row = r // depth, r % depth
                at = (owner // members, owner % members, c)
                out2_ref[(*at, 0, row, part_of(n))] = real
                out2_ref[(*at, 1, row, part_of(n))] = imag
            return carry

        lax.fori_loop(0, columns // 8, part, 0)
        start_all(*second, 1, c, ends2(1))
        return carry

    lax.fori_loop(0, 3, forward, 0)

    def start_home(c, carry):
        start_all(*second, 0, c, ends2(0))
        return carry

    lax.fori_loop(0, 3, start_home, 0)

    def take_planes(s):
        def one(c, carry):
            finish_all(*second, s, c, ends2(s))
            planes = jnp.concatenate(
                [
                    jnp.concatenate(
                        [in2_ref[s, :, c, p, z].reshape(height, breadth) for p in range(2)], axis=1
                    )
                    for z in range(depth)
                ],
                axis=0,
            )
            wide = product(halves(planes), turned_table())
            back_ref[c] = product(plain_table(), halves(spread_blocks(wide)))
            return carry

        lax.fori_loop(0, 3, one, 0)

    def theta_at(waves, p, row, i):
        at = pl.ds(pl.multiple_of(p * height + i * step_rows, step_rows), step_rows)
        lanes = pl.ds(pl.multiple_of(row * breadth, breadth), breadth)
        return [-v for v in waves.cross([back_ref[c, at, lanes] for c in range(3)])]

    def guest_result(row, i):
        waves = Waves(partner, row, i)
        for p in range(2):
            pair = waves.reduce(theta_at(waves, p, row, i))
            for n in range(2):
                result_ref[row, n, p, rows_of(i), :] = pair[n]

    def add_sums(waves, pairs, row, i, sums):
        inverse = waves.inverse()
        (real1, real2), (imag1, imag2) = [[inverse * v for v in pair] for pair in pairs]
        sums = list(sums)
        n = 0
        for source in (pair_ref, other_ref):
            for a in range(bands):
                one_real, one_imag = [source[a, row, 0, p, rows_of(i), :] for p in range(2)]
                two_real, two_imag = [source[a, row, 1, p, rows_of(i), :] for p in range(2)]
                real = (two_real * real1 + two_imag * imag1) - (one_real * real2 + one_imag * imag2)
                imag = (two_real * imag1 - two_imag * real1) - (one_real * imag2 - one_imag * real2)
                sums[n] = sums[n] + real
                sums[n + 1] = sums[n + 1] + imag
                n += 2
        return tuple(sums)

    def each_sum(b, body):
        zero = jnp.zeros((step_rows, breadth), single)

        def step(n, sums):
            return body(n // steps, n % steps, sums)

        sums = lax.fori_loop(0, depth * steps, step, (zero,) * (4 * bands))
        at = pl.ds(pl.multiple_of(b * 4 * bands, 4 * bands), 4 * bands)
        sums_ref[me, at, :] = jnp.concatenate(
            [jnp.sum(v, axis=0, keepdims=True) for v in sums], axis=0
        )

    def home_result(row, i, sums):
        waves = Waves(me, row, i)
        pairs = []
        for p in range(2):
            theta = theta_at(waves, p, row, i)
            for c in range(3):
                theta_ref[p, c, side, row, rows_of(i), :] = theta[c]
            pairs.append(waves.reduce(theta))
        return add_sums(waves, pairs, row, i, sums)

    def away_result(row, i, sums):
        waves = Waves(me, row, i)
        ratios = waves.ratios()
        pairs = []
        for p in range(2):
            pair = [return_ref[row, n, p, rows_of(i), :] for n in range(2)]
            theta = waves.rebuild(ratios, *pair)
            for c in range(3):
                theta_ref[p, c, 1 - side, row, rows_of(i), :] = theta[c]
            pairs.append(pair)
        return add_sums(waves, pairs, row, i, sums)

    def sums_copy(slot, peer, k):
        return pltpu.make_async_remote_copy(
            src_ref=sums_ref.at[slot],
            dst_ref=sums_ref.at[slot],
            send_sem=sums_send.at[k],
            recv_sem=sums_recv.at[k],
            device_id={"gz": peer},
            device_id_type=MESH,
        )

    take_planes(1)
    each_step(guest_result)
    for row in range(depth):
        return_copy(row).start()
    take_planes(0)
    other_copy(1 - side, 0).wait_recv()
    other_copy(side, 1).wait_recv()
    each_sum(side, home_result)

    half_copy(mine).wait_send()
    each_peer(lambda k, peer, source: slab_copy(peer, me, k).wait_send())
    for row in range(depth):
        swap_copy(row).wait_send()
    other_copy(1 - side, 0).wait_send()
    other_copy(side, 1).wait_send()

    def drain(c, carry):
        for s in range(2):
            drain_all(*first, s, c, ends1(s))
            drain_all(*second, s, c, ends2(s))
        return carry

    lax.fori_loop(0, 3, drain, 0)
    for row in range(depth):
        return_copy(row).wait_recv()
    each_sum(1 - side, away_result)
    each_peer(lambda k, peer, source: sums_copy(me, peer, k).start())
    for row in range(depth):
        return_copy(row).wait_send()
    each_peer(lambda k, peer, source: sums_copy(source, source, k).wait_recv())
    gram_ref[...] = jnp.sum(sums_ref[...], axis=0)
    each_peer(lambda k, peer, source: sums_copy(me, peer, k).wait_send())


def on_device_kernel(coeffs, material, inv_diag, inv_off):
    groups = lax.axis_size("gz")
    _, comps, bands, depth, height, breadth = coeffs.shape
    total = depth * groups
    members = groups // 2
    columns = height // members
    table = jnp.asarray(split_table(breadth, total**-0.25))
    grams = bands * 4 * bands
    voxels = (3, 2, total, columns, breadth)
    block = (2, members, 3, 2, depth, columns, breadth)
    pairs = (depth, 2, 2, height, breadth)
    vmem = pl.BlockSpec(memory_space=pltpu.VMEM)
    hbm = pl.BlockSpec(memory_space=pltpu.HBM)
    dma = pltpu.SemaphoreType.DMA
    operands = [
        pltpu.with_memory_space_constraint(v, pltpu.HBM)
        for v in (coeffs, material, inv_diag, inv_off, table)
    ]
    theta, sums = pl.pallas_call(
        functools.partial(operator_kernel, groups),
        out_shape=(
            jax.ShapeDtypeStruct(coeffs.shape, single),
            jax.ShapeDtypeStruct((grams, breadth), single),
        ),
        in_specs=[hbm, hbm, hbm, hbm, hbm],
        out_specs=(vmem, vmem),
        scratch_shapes=[
            pltpu.VMEM(coeffs.shape, single),
            pltpu.VMEM(material.shape, jnp.int32),
            pltpu.VMEM(table.shape, half),
            pltpu.SMEM(inv_diag.shape, single),
            pltpu.SMEM(inv_off.shape, single),
            pltpu.VMEM((depth, groups, columns, breadth), jnp.int32),
            pltpu.VMEM((6, groups, depth, columns, breadth), single),
            pltpu.VMEM((3, 2 * height, depth * breadth), half),
            pltpu.VMEM((3, 2 * height, depth * breadth), half),
            pltpu.VMEM((3, 2 * height, depth * breadth), single),
            pltpu.VMEM((bands, *pairs), single),
            pltpu.VMEM((bands, *pairs), single),
            pltpu.VMEM(pairs, single),
            pltpu.VMEM(pairs, single),
            pltpu.VMEM(pairs, single),
            pltpu.VMEM(block, single),
            pltpu.VMEM(block, single),
            pltpu.VMEM(voxels, single),
            pltpu.VMEM(voxels, single),
            pltpu.VMEM(block, single),
            pltpu.VMEM(block, single),
            pltpu.VMEM((groups, grams, breadth), single),
            dma((6,)),
            dma((groups,)),
            dma((groups,)),
            dma((2,)),
            dma((2, 3, members)),
            dma((2, 3, members)),
            dma((2, 3, members)),
            dma((2, 3, members)),
            dma((depth,)),
            dma((depth,)),
            dma((depth,)),
            dma((depth,)),
            dma((2,)),
            dma((2,)),
            dma((groups,)),
            dma((groups,)),
        ],
        compiler_params=pltpu.CompilerParams(
            collective_id=0, has_side_effects=True, vmem_limit_bytes=48 * 1024 * 1024
        ),
        name="maxwell",
    )(*operands)
    values = jnp.sum(sums, axis=1) / (breadth * height * total)
    values = values.reshape(bands, 2, bands, 2).transpose(1, 3, 2, 0)
    own, other = values[0], values[1]
    first = lax.axis_index("ba") == 0
    gram = jnp.concatenate([jnp.where(first, own, other), jnp.where(first, other, own)], axis=1)
    return (theta, gram)


def fits(coeffs):
    groups = lax.axis_size("gz")
    _, _, bands, depth, height, breadth = coeffs.shape
    return (
        lax.axis_size("ba") == 2
        and bands == 2
        and depth == 2
        and groups >= 4
        and height % (4 * groups) == 0
        and height % 16 == 0
        and height == breadth
        and breadth % 128 == 0
    )


def on_either(coeffs, material, inv_diag, inv_off):
    chosen = on_device_kernel if fits(coeffs) else on_device
    return chosen(coeffs, material, inv_diag, inv_off)


def solution(mesh):
    in_specs = (P(None, None, "ba", "gz", None, None), P("gz", None, None), P(), P())
    out_specs = (P(None, None, "ba", "gz", None, None), P(None, None, "ba"))
    return jax.shard_map(
        on_either, mesh=mesh, in_specs=in_specs, out_specs=out_specs, check_vma=False
    )
```

```python
import functools
import math

import jax
import jax.numpy as jnp
import numpy as np
from jax import lax
from jax.experimental import pallas as pl
from jax.experimental.pallas import tpu as pltpu
from jax.sharding import PartitionSpec as P

highest = lax.Precision.HIGHEST
half_turn = 3.141592653589793


def reverse_bits(values, levels):
    flipped = jnp.zeros_like(values)
    for position in range(levels):
        flipped = flipped + (values >> position & 1) * (1 << levels - 1 - position)
    return flipped


def signed_wave(numbers, length):
    shifted = jnp.where(numbers < length // 2, numbers, numbers - length)
    return shifted.astype(jnp.float32) / (length / 2.0)


def phase_tables(first, second, length, sign):
    product = first[:, None] * second[None, :] % length
    angle = 2.0 * half_turn / length * product.astype(jnp.float32)
    factor = 1.0 / math.sqrt(length)
    return (jnp.cos(angle) * factor, sign * jnp.sin(angle) * factor)


def cross_waves(waves, field):
    first, second, third = waves
    return jnp.stack(
        [
            second * field[:, 2] - third * field[:, 1],
            third * field[:, 0] - first * field[:, 2],
            first * field[:, 1] - second * field[:, 0],
        ],
        axis=1,
    )


def along_width(field, cosine, sine):
    breadth = field.shape[-1]
    rows = field.reshape(2, -1, breadth)
    joined = jnp.concatenate([cosine, sine], axis=1)
    real_prod = jnp.dot(rows[0], joined, precision=highest)
    imag_prod = jnp.dot(rows[1], joined, precision=highest)
    real_out = real_prod[:, :breadth] - imag_prod[:, breadth:]
    imag_out = real_prod[:, breadth:] + imag_prod[:, :breadth]
    return jnp.stack([real_out, imag_out]).reshape(field.shape)


def along_height(field, cosine, sine):
    tables = jnp.stack([cosine, sine])
    product = jnp.einsum("pcbzyx,tyk->tpcbzkx", field, tables, precision=highest)
    return jnp.stack([product[0, 0] - product[1, 1], product[1, 0] + product[0, 1]])


def along_depth(field, cosine, sine):
    tables = jnp.stack([cosine, sine])
    product = jnp.einsum("pcbzyx,tzk->tpcbkyx", field, tables, precision=highest)
    return jnp.stack([product[0, 0] - product[1, 1], product[1, 0] + product[0, 1]])


def apply_material(field, material, inv_diag, inv_off):
    materials = inv_diag.shape[0]
    onehot = (material[None] == jnp.arange(materials, dtype=jnp.int32)[:, None, None, None]).astype(
        jnp.float32
    )
    table = jnp.concatenate([inv_diag, inv_off], axis=1)
    tensor = jnp.einsum("mk,mzyx->kzyx", table, onehot, precision=highest)
    first = field[:, 0]
    second = field[:, 1]
    third = field[:, 2]
    return jnp.stack(
        [
            tensor[0] * first + tensor[3] * second + tensor[5] * third,
            tensor[3] * first + tensor[1] * second + tensor[4] * third,
            tensor[5] * first + tensor[4] * second + tensor[2] * third,
        ],
        axis=1,
    )


def on_device(coeffs, material, inv_diag, inv_off):
    groups = lax.axis_size("gz")
    levels = groups.bit_length() - 1
    depth = coeffs.shape[3]
    height = coeffs.shape[4]
    breadth = coeffs.shape[5]
    total_depth = depth * groups
    device = lax.axis_index("gz")
    local_rows = jnp.arange(depth, dtype=jnp.int32)
    waves_here = reverse_bits(device, levels) + groups * local_rows
    across = jnp.arange(breadth, dtype=jnp.int32)
    upward = jnp.arange(height, dtype=jnp.int32)
    waves = (
        signed_wave(across, breadth)[None, None, :],
        signed_wave(upward, height)[None, :, None],
        signed_wave(waves_here, total_depth)[:, None, None],
    )
    curl = cross_waves(waves, coeffs)
    all_rows = jnp.arange(total_depth, dtype=jnp.int32)
    wave_rows = reverse_bits(all_rows // depth, levels) + groups * (all_rows % depth)
    height_cos, height_sin = phase_tables(upward, upward, height, 1.0)
    width_cos, width_sin = phase_tables(across, across, breadth, 1.0)
    planar = along_height(curl, height_cos, height_sin)
    planar = along_width(planar, width_cos, width_sin)
    material_slab = lax.all_to_all(material, "gz", split_axis=1, concat_axis=0, tiled=True)
    inverse_cos, inverse_sin = phase_tables(wave_rows, all_rows, total_depth, 1.0)
    forward_cos, forward_sin = phase_tables(all_rows, wave_rows, total_depth, -1.0)
    spatial_piece = along_depth(
        lax.all_to_all(planar, "gz", split_axis=4, concat_axis=3, tiled=True),
        inverse_cos,
        inverse_sin,
    )
    scaled_piece = apply_material(spatial_piece, material_slab, inv_diag, inv_off)
    returned = along_depth(scaled_piece, forward_cos, forward_sin)
    spectral = lax.all_to_all(returned, "gz", split_axis=3, concat_axis=4, tiled=True)
    spectral = along_width(spectral, width_cos, -width_sin)
    spectral = along_height(spectral, height_cos, -height_sin)
    theta = -cross_waves(waves, spectral)
    factor = 1.0 / (breadth * height * total_depth)
    piece = lax.all_gather(coeffs, "ba", axis=2, tiled=True)
    real_part = jnp.einsum("cbzyx,cezyx->be", piece[0], theta[0], precision=highest) + jnp.einsum(
        "cbzyx,cezyx->be", piece[1], theta[1], precision=highest
    )
    imag_part = jnp.einsum("cbzyx,cezyx->be", piece[0], theta[1], precision=highest) - jnp.einsum(
        "cbzyx,cezyx->be", piece[1], theta[0], precision=highest
    )
    block = jnp.stack([real_part, imag_part]) * factor
    gram = lax.psum(block, "gz")
    return (theta, gram)


MESH = pl.DeviceIdType.MESH
single = jnp.float32
half = jnp.bfloat16


def split_table(length, extra):
    numbers = np.arange(length)
    angle = 2.0 * np.pi / length * (numbers[:, None] * numbers[None, :] % length)
    cosine = np.cos(angle) * extra / math.sqrt(length)
    sine = np.sin(angle) * extra / math.sqrt(length)
    inverse = np.block([[cosine, sine], [-sine, cosine]])
    parts = []
    for table in (inverse, inverse.T):
        high = table.astype(np.float32).astype(half)
        low = (table - high.astype(np.float64)).astype(half)
        parts += [high, low]
    return np.stack(parts)


def halves(values):
    high = values.astype(half)
    return high, (values - high.astype(single)).astype(half)


def product(first, second):
    dot = functools.partial(jnp.dot, preferred_element_type=single)
    return dot(first[0], second[0]) + (dot(first[0], second[1]) + dot(first[1], second[0]))


def twiddled(pair, step, span, sign):
    real, imag = pair
    if step == 0:
        return real, imag
    if 2 * step == span:
        return (-imag, real) if sign > 0 else (imag, -real)
    angle = math.pi * step / span
    cosine, sine = math.cos(angle), sign * math.sin(angle)
    return real * cosine - imag * sine, real * sine + imag * cosine


def to_voxels(points):
    points = list(points)
    span = 1
    while span < len(points):
        for base in range(0, len(points), 2 * span):
            for step in range(span):
                a = points[base + step]
                t = twiddled(points[base + step + span], step, span, 1.0)
                points[base + step] = (a[0] + t[0], a[1] + t[1])
                points[base + step + span] = (a[0] - t[0], a[1] - t[1])
        span *= 2
    return points


def to_waves(points):
    points = list(points)
    span = len(points) // 2
    while span >= 1:
        for base in range(0, len(points), 2 * span):
            for step in range(span):
                a, t = points[base + step], points[base + step + span]
                points[base + step] = (a[0] + t[0], a[1] + t[1])
                points[base + step + span] = twiddled(
                    (a[0] - t[0], a[1] - t[1]), step, span, -1.0
                )
        span //= 2
    return points


def operator_kernel(
    groups,
    coeffs_hbm,
    material_hbm,
    diag_hbm,
    off_hbm,
    table_hbm,
    theta_ref,
    gram_ref,
    coeffs_ref,
    material_ref,
    table_ref,
    diag_ref,
    off_ref,
    slab_ref,
    tensor_ref,
    high_ref,
    low_ref,
    back_ref,
    pair_ref,
    other_ref,
    swap_ref,
    result_ref,
    return_ref,
    out1_ref,
    in1_ref,
    field_ref,
    scaled_ref,
    out2_ref,
    in2_ref,
    sums_ref,
    load_sem,
    slab_send,
    slab_recv,
    half_sem,
    send1,
    recv1,
    send2,
    recv2,
    swap_send,
    swap_recv,
    return_send,
    return_recv,
    other_send,
    other_recv,
    sums_send,
    sums_recv,
):
    _, comps, bands, depth, height, breadth = coeffs_ref.shape
    total = depth * groups
    members = groups // 2
    columns = height // members
    levels = groups.bit_length() - 1
    me = lax.axis_index("gz")
    mine = lax.axis_index("ba")
    side = me // members
    seat = me % members
    partner = (me + members) % groups
    mate = {"ba": 1 - mine}
    step_rows = 16
    steps = height // step_rows

    def each_peer(body):
        def step(k, carry):
            body(k, (me + k) % groups, (me + groups - k) % groups)
            return carry

        lax.fori_loop(1, groups, step, 0)

    def each_member(body):
        def step(k, carry):
            body(k, (seat + k) % members, (seat + members - k) % members)
            return carry

        lax.fori_loop(1, members, step, 0)

    barrier = pltpu.get_barrier_semaphore()
    each_peer(
        lambda k, peer, source: pl.semaphore_signal(
            barrier, inc=1, device_id={"gz": peer}, device_id_type=MESH
        )
    )
    pl.semaphore_signal(barrier, inc=1, device_id=mate, device_id_type=MESH)

    def band_load(b, n):
        return pltpu.make_async_copy(
            coeffs_hbm.at[:, :, b], coeffs_ref.at[:, :, b], load_sem.at[n]
        )

    loads = [
        band_load(1 - side, 0),
        band_load(side, 1),
        pltpu.make_async_copy(table_hbm, table_ref, load_sem.at[2]),
        pltpu.make_async_copy(material_hbm, material_ref, load_sem.at[3]),
        pltpu.make_async_copy(diag_hbm, diag_ref, load_sem.at[4]),
        pltpu.make_async_copy(off_hbm, off_ref, load_sem.at[5]),
    ]
    for load in loads:
        load.start()

    def signed(number, length):
        return number - length * (number // (length // 2))

    def row_number(owner, row):
        reversed_owner = 0
        for position in range(levels):
            bit = (owner // (1 << position)) % 2
            reversed_owner = reversed_owner + bit * (1 << (levels - 1 - position))
        return signed(reversed_owner + groups * row, total)

    def inverse_of(values):
        zero = values == 0
        return jnp.where(zero, 0.0, 1.0 / jnp.where(zero, 1, values).astype(single))

    class Waves:
        def __init__(self, owner, row, i):
            shape = (step_rows, breadth)
            nx = lax.broadcasted_iota(jnp.int32, shape, 1)
            ny = lax.broadcasted_iota(jnp.int32, shape, 0) + i * step_rows
            nx = jnp.where(nx < breadth // 2, nx, nx - breadth)
            ny = jnp.where(ny < height // 2, ny, ny - height)
            nz = jnp.full(shape, row_number(owner, row), jnp.int32)
            self.x = nx.astype(single) / (breadth / 2.0)
            self.y = ny.astype(single) / (height / 2.0)
            self.z = nz.astype(single) / (total / 2.0)
            ax, ay, az = jnp.abs(nx) * total, jnp.abs(ny) * total, jnp.abs(nz) * breadth
            self.is_x = (ax >= ay) & (ax >= az)
            self.is_y = ay >= az
            self.numbers = (nx, ny, nz)

        def cross(self, v):
            q = (self.x, self.y, self.z)
            return [
                q[(c + 1) % 3] * v[(c + 2) % 3] - q[(c + 2) % 3] * v[(c + 1) % 3]
                for c in range(3)
            ]

        def pick(self, first, second, third):
            return jnp.where(self.is_x, first, jnp.where(self.is_y, second, third))

        def inverse(self):
            nx, ny, nz = self.numbers
            scaled = self.pick(nx * total, ny * total, nz * breadth)
            return inverse_of(scaled) * (total * breadth / 2.0)

        def ratios(self):
            inverse = self.inverse()
            return (
                self.pick(self.y, self.z, self.x) * inverse,
                self.pick(self.z, self.x, self.y) * inverse,
            )

        def reduce(self, v):
            return self.pick(v[1], v[2], v[0]), self.pick(v[2], v[0], v[1])

        def rebuild(self, ratios, first, second):
            last = -(ratios[0] * first + ratios[1] * second)
            return [
                self.pick(last, second, first),
                self.pick(first, last, second),
                self.pick(second, first, last),
            ]

    def rows_of(i):
        return pl.ds(pl.multiple_of(i * step_rows, step_rows), step_rows)

    def each_step(row, body):
        def step(i, carry):
            body(row, i)
            return carry

        lax.fori_loop(0, steps, step, 0)

    def each_row(body):
        def step(row, carry):
            body(row)
            return carry

        lax.fori_loop(0, depth, step, 0)

    def put_halves(curls, p, row, i):
        at = pl.ds(pl.multiple_of(p * height + i * step_rows, step_rows), step_rows)
        for c in range(3):
            high, low = halves(curls[c])
            lanes = pl.ds(c * breadth, breadth)
            high_ref[row, at, lanes] = high
            low_ref[row, at, lanes] = low

    def put_pair(b, p, row, i, pair):
        for n in range(2):
            pair_ref[b, row, n, p, rows_of(i), :] = pair[n]

    def away_step(row, i):
        waves = Waves(me, row, i)
        for p in range(2):
            values = [coeffs_ref[p, c, 1 - side, row, rows_of(i), :] for c in range(3)]
            put_pair(1 - side, p, row, i, waves.reduce(waves.cross(values)))

    def home_step(row, i):
        waves = Waves(me, row, i)
        for p in range(2):
            values = [coeffs_ref[p, c, side, row, rows_of(i), :] for c in range(3)]
            curls = waves.cross(values)
            put_halves(curls, p, row, i)
            put_pair(side, p, row, i, waves.reduce(curls))

    def guest_step(row, i):
        waves = Waves(partner, row, i)
        ratios = waves.ratios()
        for p in range(2):
            pair = [swap_ref[row, n, p, rows_of(i), :] for n in range(2)]
            put_halves(waves.rebuild(ratios, *pair), p, row, i)

    def plain_table():
        return table_ref[0], table_ref[1]

    def turned_table():
        return table_ref[2], table_ref[3]

    def gather_blocks(values):
        top, bottom = values[:height], values[height:]
        return jnp.concatenate(
            [
                jnp.concatenate(
                    [
                        top[:, z * breadth : (z + 1) * breadth],
                        bottom[:, z * breadth : (z + 1) * breadth],
                    ],
                    axis=1,
                )
                for z in range(3)
            ],
            axis=0,
        )

    def spread_blocks(values):
        return jnp.concatenate(
            [
                jnp.concatenate(
                    [
                        values[z * height : (z + 1) * height, p * breadth : (p + 1) * breadth]
                        for z in range(3)
                    ],
                    axis=1,
                )
                for p in range(2)
            ],
            axis=0,
        )

    def to_peer(out, into, send, recv, s, row, k, peer, from_at, to_at):
        return pltpu.make_async_remote_copy(
            src_ref=out.at[from_at, row, peer],
            dst_ref=into.at[to_at, row, seat],
            send_sem=send.at[s, row, k],
            recv_sem=recv.at[s, row, k],
            device_id={"gz": side * members + peer},
            device_id_type=MESH,
        )

    def from_peer(out, into, send, recv, s, row, k, source, from_at, to_at):
        return pltpu.make_async_remote_copy(
            src_ref=out.at[from_at, row, source],
            dst_ref=into.at[to_at, row, source],
            send_sem=send.at[s, row, k],
            recv_sem=recv.at[s, row, k],
            device_id={"gz": side * members + source},
            device_id_type=MESH,
        )

    def ends1(s):
        return s, (side + s) % 2

    def ends2(s):
        return (side + s) % 2, s

    def start_all(out, into, send, recv, s, row, ends):
        each_member(
            lambda k, peer, source: to_peer(
                out, into, send, recv, s, row, k, peer, *ends
            ).start()
        )
        into[ends[1], row, seat] = out[ends[0], row, seat]

    def finish_all(out, into, send, recv, s, row, ends):
        each_member(
            lambda k, peer, source: from_peer(
                out, into, send, recv, s, row, k, source, *ends
            ).wait_recv()
        )

    def drain_all(out, into, send, recv, s, row, ends):
        each_member(
            lambda k, peer, source: to_peer(
                out, into, send, recv, s, row, k, peer, *ends
            ).wait_send()
        )

    first = (out1_ref, in1_ref, send1, recv1)
    second = (out2_ref, in2_ref, send2, recv2)

    def make_planes(s, row):
        tall = product(turned_table(), (high_ref[row], low_ref[row]))
        wide = product(halves(gather_blocks(tall)), plain_table())
        for p in range(2):
            for c in range(3):
                plane = wide[c * height : (c + 1) * height, p * breadth : (p + 1) * breadth]
                out1_ref[s, row, :, c, p] = plane.reshape(members, columns, breadth)
        start_all(*first, s, row, ends1(s))

    def swap_copy(row):
        return pltpu.make_async_remote_copy(
            src_ref=pair_ref.at[1 - side, row],
            dst_ref=swap_ref.at[row],
            send_sem=swap_send.at[row],
            recv_sem=swap_recv.at[row],
            device_id={"gz": partner},
            device_id_type=MESH,
        )

    def return_copy(row):
        return pltpu.make_async_remote_copy(
            src_ref=result_ref.at[row],
            dst_ref=return_ref.at[row],
            send_sem=return_send.at[row],
            recv_sem=return_recv.at[row],
            device_id={"gz": partner},
            device_id_type=MESH,
        )

    def other_copy(b, n):
        return pltpu.make_async_remote_copy(
            src_ref=pair_ref.at[b],
            dst_ref=other_ref.at[b],
            send_sem=other_send.at[n],
            recv_sem=other_recv.at[n],
            device_id=mate,
            device_id_type=MESH,
        )

    def columns_of(peer):
        return pl.ds(pl.multiple_of((peer % members) * columns, columns), columns)

    def slab_copy(peer, slot, k):
        return pltpu.make_async_remote_copy(
            src_ref=material_ref.at[mine, columns_of(peer), :],
            dst_ref=slab_ref.at[mine, slot],
            send_sem=slab_send.at[k],
            recv_sem=slab_recv.at[k],
            device_id={"gz": peer},
            device_id_type=MESH,
        )

    def half_copy(row, part):
        at = pl.ds(pl.multiple_of(part * members, members), members)
        return pltpu.make_async_remote_copy(
            src_ref=slab_ref.at[row, at],
            dst_ref=slab_ref.at[row, at],
            send_sem=half_sem.at[0, part],
            recv_sem=half_sem.at[1, part],
            device_id=mate,
            device_id_type=MESH,
        )

    outer = (me // (members // 2)) % 3 == 0

    loads[0].wait()
    each_row(lambda row: each_step(row, away_step))
    pl.semaphore_wait(barrier, groups)
    swap_copy(0).start()

    @pl.when(jnp.logical_not(outer))
    def _():
        swap_copy(1).start()

    loads[1].wait()
    loads[2].wait()

    def home_row(row):
        each_step(row, home_step)
        make_planes(0, row)

    each_row(home_row)

    @pl.when(outer)
    def _():
        swap_copy(1).start()

    other_copy(side, 1).start()
    for load in loads[3:]:
        load.wait()
    each_peer(lambda k, peer, source: slab_copy(peer, me, k).start())
    slab_ref[mine, me] = material_ref[mine, columns_of(me), :]

    def wait_slabs(part):
        def step(k, carry):
            source = (me + groups - k) % groups

            @pl.when(source // members == part)
            def _():
                slab_copy(source, source, k).wait_recv()

            return carry

        lax.fori_loop(1, groups, step, 0)

    def guest_row(row):
        swap_copy(row).wait_recv()
        each_step(row, guest_step)
        make_planes(1, row)

    guest_row(0)
    wait_slabs(side)
    half_copy(mine, side).start()
    guest_row(1)
    wait_slabs(1 - side)
    half_copy(mine, 1 - side).start()
    other_copy(1 - side, 0).start()
    for part in range(2):
        half_copy(1 - mine, part).wait_recv()
    kinds = diag_ref.shape[0]

    def tensor_step(owner, carry):
        for row in range(depth):
            codes = slab_ref[row, owner]
            for entry in range(6):
                table = diag_ref if entry < 3 else off_ref
                values = jnp.full(codes.shape, table[0, entry % 3], single)
                for kind in range(1, kinds):
                    values = jnp.where(codes == kind, table[kind, entry % 3], values)
                tensor_ref[entry, owner, row] = values
        return carry

    lax.fori_loop(0, groups, tensor_step, 0)

    def part_of(n):
        return pl.ds(pl.multiple_of(n * 8, 8), 8)

    def finish_first(row):
        for s in range(2):
            finish_all(*first, s, row, ends1(s))

    each_row(finish_first)

    def inverse(n, carry):
        c, at = n // (columns // 8), part_of(n % (columns // 8))
        points = []
        for r in range(total):
            owner, row = r // depth, r % depth
            where = (owner // members, row, owner % members, c)
            points.append((in1_ref[(*where, 0, at)], in1_ref[(*where, 1, at)]))
        for z, (real, imag) in enumerate(to_voxels(points)):
            field_ref[c, 0, z, at] = real
            field_ref[c, 1, z, at] = imag
        return carry

    lax.fori_loop(0, 3 * (columns // 8), inverse, 0)

    def scale(z, carry):
        xx, yy, zz, xy, yz, zx = [tensor_ref[entry, z // depth, z % depth] for entry in range(6)]
        for p in range(2):
            fx, fy, fz = [field_ref[c, p, z] for c in range(3)]
            scaled_ref[0, p, z] = xx * fx + xy * fy + zx * fz
            scaled_ref[1, p, z] = xy * fx + yy * fy + yz * fz
            scaled_ref[2, p, z] = zx * fx + yz * fy + zz * fz
        return carry

    lax.fori_loop(0, total, scale, 0, unroll=2)

    def forward(n, carry):
        c, at = n // (columns // 8), part_of(n % (columns // 8))
        points = [(scaled_ref[c, 0, z, at], scaled_ref[c, 1, z, at]) for z in range(total)]
        for r, (real, imag) in enumerate(to_waves(points)):
            owner, row = r // depth, r % depth
            where = (owner // members, row, owner % members, c)
            out2_ref[(*where, 0, at)] = real
            out2_ref[(*where, 1, at)] = imag
        return carry

    lax.fori_loop(0, 3 * (columns // 8), forward, 0)
    each_row(lambda row: start_all(*second, 1, row, ends2(1)))
    each_row(lambda row: start_all(*second, 0, row, ends2(0)))

    def take_planes(s, row):
        finish_all(*second, s, row, ends2(s))
        planes = jnp.concatenate(
            [
                jnp.concatenate(
                    [in2_ref[s, row, :, c, p].reshape(height, breadth) for p in range(2)], axis=1
                )
                for c in range(3)
            ],
            axis=0,
        )
        wide = product(halves(planes), turned_table())
        back_ref[row] = product(plain_table(), halves(spread_blocks(wide)))

    def theta_at(waves, p, row, i):
        at = pl.ds(pl.multiple_of(p * height + i * step_rows, step_rows), step_rows)
        lanes = [pl.ds(c * breadth, breadth) for c in range(3)]
        return [-v for v in waves.cross([back_ref[row, at, lanes[c]] for c in range(3)])]

    def guest_result(row, i):
        waves = Waves(partner, row, i)
        for p in range(2):
            pair = waves.reduce(theta_at(waves, p, row, i))
            for n in range(2):
                result_ref[row, n, p, rows_of(i), :] = pair[n]

    def add_sums(waves, pairs, row, i, sums):
        inverse = waves.inverse()
        (real1, real2), (imag1, imag2) = [[inverse * v for v in pair] for pair in pairs]
        sums = list(sums)
        n = 0
        for source in (pair_ref, other_ref):
            for a in range(bands):
                one_real, one_imag = [source[a, row, 0, p, rows_of(i), :] for p in range(2)]
                two_real, two_imag = [source[a, row, 1, p, rows_of(i), :] for p in range(2)]
                real = (two_real * real1 + two_imag * imag1) - (one_real * real2 + one_imag * imag2)
                imag = (two_real * imag1 - two_imag * real1) - (one_real * imag2 - one_imag * real2)
                sums[n] = sums[n] + real
                sums[n + 1] = sums[n + 1] + imag
                n += 2
        return tuple(sums)

    def zero_sums():
        return (jnp.zeros((step_rows, breadth), single),) * (4 * bands)

    def each_sum(row, body, sums):
        return lax.fori_loop(0, steps, lambda i, sums: body(row, i, sums), sums)

    def keep_sums(b, sums):
        at = pl.ds(pl.multiple_of(b * 4 * bands, 4 * bands), 4 * bands)
        sums_ref[me, at, :] = jnp.concatenate(
            [jnp.sum(v, axis=0, keepdims=True) for v in sums], axis=0
        )

    def home_result(row, i, sums):
        waves = Waves(me, row, i)
        pairs = []
        for p in range(2):
            theta = theta_at(waves, p, row, i)
            for c in range(3):
                theta_ref[p, c, side, row, rows_of(i), :] = theta[c]
            pairs.append(waves.reduce(theta))
        return add_sums(waves, pairs, row, i, sums)

    def away_result(row, i, sums):
        waves = Waves(me, row, i)
        ratios = waves.ratios()
        pairs = []
        for p in range(2):
            pair = [return_ref[row, n, p, rows_of(i), :] for n in range(2)]
            theta = waves.rebuild(ratios, *pair)
            for c in range(3):
                theta_ref[p, c, 1 - side, row, rows_of(i), :] = theta[c]
            pairs.append(pair)
        return add_sums(waves, pairs, row, i, sums)

    def sums_copy(slot, peer, k):
        return pltpu.make_async_remote_copy(
            src_ref=sums_ref.at[slot],
            dst_ref=sums_ref.at[slot],
            send_sem=sums_send.at[k],
            recv_sem=sums_recv.at[k],
            device_id={"gz": peer},
            device_id_type=MESH,
        )

    def guest_back(row):
        take_planes(1, row)
        each_step(row, guest_result)
        return_copy(row).start()

    each_row(guest_back)

    def home_back(row, sums):
        take_planes(0, row)
        return each_sum(row, home_result, sums)

    other_copy(side, 1).wait_recv()
    other_copy(1 - side, 0).wait_recv()
    keep_sums(side, lax.fori_loop(0, depth, home_back, zero_sums()))

    for part in range(2):
        half_copy(mine, part).wait_send()
    each_peer(lambda k, peer, source: slab_copy(peer, me, k).wait_send())
    for row in range(depth):
        swap_copy(row).wait_send()
    other_copy(1 - side, 0).wait_send()
    other_copy(side, 1).wait_send()

    def drain(row):
        for s in range(2):
            drain_all(*first, s, row, ends1(s))
            drain_all(*second, s, row, ends2(s))

    each_row(drain)

    def away_back(row, sums):
        return_copy(row).wait_recv()
        return each_sum(row, away_result, sums)

    keep_sums(1 - side, lax.fori_loop(0, depth, away_back, zero_sums()))
    each_peer(lambda k, peer, source: sums_copy(me, peer, k).start())
    for row in range(depth):
        return_copy(row).wait_send()
    each_peer(lambda k, peer, source: sums_copy(source, source, k).wait_recv())
    gram_ref[...] = jnp.sum(sums_ref[...], axis=0)
    each_peer(lambda k, peer, source: sums_copy(me, peer, k).wait_send())


def on_device_kernel(coeffs, material, inv_diag, inv_off):
    groups = lax.axis_size("gz")
    _, comps, bands, depth, height, breadth = coeffs.shape
    total = depth * groups
    members = groups // 2
    columns = height // members
    table = jnp.asarray(split_table(breadth, total**-0.25))
    grams = bands * 4 * bands
    voxels = (3, 2, total, columns, breadth)
    block = (2, depth, members, 3, 2, columns, breadth)
    pairs = (depth, 2, 2, height, breadth)
    vmem = pl.BlockSpec(memory_space=pltpu.VMEM)
    hbm = pl.BlockSpec(memory_space=pltpu.HBM)
    dma = pltpu.SemaphoreType.DMA
    operands = [
        pltpu.with_memory_space_constraint(v, pltpu.HBM)
        for v in (coeffs, material, inv_diag, inv_off, table)
    ]
    theta, sums = pl.pallas_call(
        functools.partial(operator_kernel, groups),
        out_shape=(
            jax.ShapeDtypeStruct(coeffs.shape, single),
            jax.ShapeDtypeStruct((grams, breadth), single),
        ),
        in_specs=[hbm, hbm, hbm, hbm, hbm],
        out_specs=(vmem, vmem),
        scratch_shapes=[
            pltpu.VMEM(coeffs.shape, single),
            pltpu.VMEM(material.shape, jnp.int32),
            pltpu.VMEM(table.shape, half),
            pltpu.SMEM(inv_diag.shape, single),
            pltpu.SMEM(inv_off.shape, single),
            pltpu.VMEM((depth, groups, columns, breadth), jnp.int32),
            pltpu.VMEM((6, groups, depth, columns, breadth), single),
            pltpu.VMEM((depth, 2 * height, 3 * breadth), half),
            pltpu.VMEM((depth, 2 * height, 3 * breadth), half),
            pltpu.VMEM((depth, 2 * height, 3 * breadth), single),
            pltpu.VMEM((bands, *pairs), single),
            pltpu.VMEM((bands, *pairs), single),
            pltpu.VMEM(pairs, single),
            pltpu.VMEM(pairs, single),
            pltpu.VMEM(pairs, single),
            pltpu.VMEM(block, single),
            pltpu.VMEM(block, single),
            pltpu.VMEM(voxels, single),
            pltpu.VMEM(voxels, single),
            pltpu.VMEM(block, single),
            pltpu.VMEM(block, single),
            pltpu.VMEM((groups, grams, breadth), single),
            dma((6,)),
            dma((groups,)),
            dma((groups,)),
            dma((2, 2)),
            dma((2, depth, members)),
            dma((2, depth, members)),
            dma((2, depth, members)),
            dma((2, depth, members)),
            dma((depth,)),
            dma((depth,)),
            dma((depth,)),
            dma((depth,)),
            dma((2,)),
            dma((2,)),
            dma((groups,)),
            dma((groups,)),
        ],
        compiler_params=pltpu.CompilerParams(
            collective_id=0, has_side_effects=True, vmem_limit_bytes=48 * 1024 * 1024
        ),
        name="maxwell",
    )(*operands)
    values = jnp.sum(sums, axis=1) / (breadth * height * total)
    values = values.reshape(bands, 2, bands, 2).transpose(1, 3, 2, 0)
    own, other = values[0], values[1]
    first = lax.axis_index("ba") == 0
    gram = jnp.concatenate([jnp.where(first, own, other), jnp.where(first, other, own)], axis=1)
    return (theta, gram)


def fits(coeffs):
    groups = lax.axis_size("gz")
    _, _, bands, depth, height, breadth = coeffs.shape
    return (
        lax.axis_size("ba") == 2
        and bands == 2
        and depth == 2
        and groups >= 4
        and height % (4 * groups) == 0
        and height % 16 == 0
        and height == breadth
        and breadth % 128 == 0
    )


def on_either(coeffs, material, inv_diag, inv_off):
    chosen = on_device_kernel if fits(coeffs) else on_device
    return chosen(coeffs, material, inv_diag, inv_off)


def solution(mesh):
    in_specs = (P(None, None, "ba", "gz", None, None), P("gz", None, None), P(), P())
    out_specs = (P(None, None, "ba", "gz", None, None), P(None, None, "ba"))
    return jax.shard_map(
        on_either, mesh=mesh, in_specs=in_specs, out_specs=out_specs, check_vma=False
    )
```

```python
import functools
import math

import jax
import jax.numpy as jnp
import numpy as np
from jax import lax
from jax.experimental import pallas as pl
from jax.experimental.pallas import tpu as pltpu
from jax.sharding import PartitionSpec as P

highest = lax.Precision.HIGHEST
half_turn = 3.141592653589793


def reverse_bits(values, levels):
    flipped = jnp.zeros_like(values)
    for position in range(levels):
        flipped = flipped + (values >> position & 1) * (1 << levels - 1 - position)
    return flipped


def signed_wave(numbers, length):
    shifted = jnp.where(numbers < length // 2, numbers, numbers - length)
    return shifted.astype(jnp.float32) / (length / 2.0)


def phase_tables(first, second, length, sign):
    product = first[:, None] * second[None, :] % length
    angle = 2.0 * half_turn / length * product.astype(jnp.float32)
    factor = 1.0 / math.sqrt(length)
    return (jnp.cos(angle) * factor, sign * jnp.sin(angle) * factor)


def cross_waves(waves, field):
    first, second, third = waves
    return jnp.stack(
        [
            second * field[:, 2] - third * field[:, 1],
            third * field[:, 0] - first * field[:, 2],
            first * field[:, 1] - second * field[:, 0],
        ],
        axis=1,
    )


def along_width(field, cosine, sine):
    breadth = field.shape[-1]
    rows = field.reshape(2, -1, breadth)
    joined = jnp.concatenate([cosine, sine], axis=1)
    real_prod = jnp.dot(rows[0], joined, precision=highest)
    imag_prod = jnp.dot(rows[1], joined, precision=highest)
    real_out = real_prod[:, :breadth] - imag_prod[:, breadth:]
    imag_out = real_prod[:, breadth:] + imag_prod[:, :breadth]
    return jnp.stack([real_out, imag_out]).reshape(field.shape)


def along_height(field, cosine, sine):
    tables = jnp.stack([cosine, sine])
    product = jnp.einsum("pcbzyx,tyk->tpcbzkx", field, tables, precision=highest)
    return jnp.stack([product[0, 0] - product[1, 1], product[1, 0] + product[0, 1]])


def along_depth(field, cosine, sine):
    tables = jnp.stack([cosine, sine])
    product = jnp.einsum("pcbzyx,tzk->tpcbkyx", field, tables, precision=highest)
    return jnp.stack([product[0, 0] - product[1, 1], product[1, 0] + product[0, 1]])


def apply_material(field, material, inv_diag, inv_off):
    materials = inv_diag.shape[0]
    onehot = (material[None] == jnp.arange(materials, dtype=jnp.int32)[:, None, None, None]).astype(
        jnp.float32
    )
    table = jnp.concatenate([inv_diag, inv_off], axis=1)
    tensor = jnp.einsum("mk,mzyx->kzyx", table, onehot, precision=highest)
    first = field[:, 0]
    second = field[:, 1]
    third = field[:, 2]
    return jnp.stack(
        [
            tensor[0] * first + tensor[3] * second + tensor[5] * third,
            tensor[3] * first + tensor[1] * second + tensor[4] * third,
            tensor[5] * first + tensor[4] * second + tensor[2] * third,
        ],
        axis=1,
    )


def on_device(coeffs, material, inv_diag, inv_off):
    groups = lax.axis_size("gz")
    levels = groups.bit_length() - 1
    depth = coeffs.shape[3]
    height = coeffs.shape[4]
    breadth = coeffs.shape[5]
    total_depth = depth * groups
    device = lax.axis_index("gz")
    local_rows = jnp.arange(depth, dtype=jnp.int32)
    waves_here = reverse_bits(device, levels) + groups * local_rows
    across = jnp.arange(breadth, dtype=jnp.int32)
    upward = jnp.arange(height, dtype=jnp.int32)
    waves = (
        signed_wave(across, breadth)[None, None, :],
        signed_wave(upward, height)[None, :, None],
        signed_wave(waves_here, total_depth)[:, None, None],
    )
    curl = cross_waves(waves, coeffs)
    all_rows = jnp.arange(total_depth, dtype=jnp.int32)
    wave_rows = reverse_bits(all_rows // depth, levels) + groups * (all_rows % depth)
    height_cos, height_sin = phase_tables(upward, upward, height, 1.0)
    width_cos, width_sin = phase_tables(across, across, breadth, 1.0)
    planar = along_height(curl, height_cos, height_sin)
    planar = along_width(planar, width_cos, width_sin)
    material_slab = lax.all_to_all(material, "gz", split_axis=1, concat_axis=0, tiled=True)
    inverse_cos, inverse_sin = phase_tables(wave_rows, all_rows, total_depth, 1.0)
    forward_cos, forward_sin = phase_tables(all_rows, wave_rows, total_depth, -1.0)
    spatial_piece = along_depth(
        lax.all_to_all(planar, "gz", split_axis=4, concat_axis=3, tiled=True),
        inverse_cos,
        inverse_sin,
    )
    scaled_piece = apply_material(spatial_piece, material_slab, inv_diag, inv_off)
    returned = along_depth(scaled_piece, forward_cos, forward_sin)
    spectral = lax.all_to_all(returned, "gz", split_axis=3, concat_axis=4, tiled=True)
    spectral = along_width(spectral, width_cos, -width_sin)
    spectral = along_height(spectral, height_cos, -height_sin)
    theta = -cross_waves(waves, spectral)
    factor = 1.0 / (breadth * height * total_depth)
    piece = lax.all_gather(coeffs, "ba", axis=2, tiled=True)
    real_part = jnp.einsum("cbzyx,cezyx->be", piece[0], theta[0], precision=highest) + jnp.einsum(
        "cbzyx,cezyx->be", piece[1], theta[1], precision=highest
    )
    imag_part = jnp.einsum("cbzyx,cezyx->be", piece[0], theta[1], precision=highest) - jnp.einsum(
        "cbzyx,cezyx->be", piece[1], theta[0], precision=highest
    )
    block = jnp.stack([real_part, imag_part]) * factor
    gram = lax.psum(block, "gz")
    return (theta, gram)


MESH = pl.DeviceIdType.MESH
single = jnp.float32
half = jnp.bfloat16


def split_table(length, extra):
    numbers = np.arange(length)
    angle = 2.0 * np.pi / length * (numbers[:, None] * numbers[None, :] % length)
    cosine = np.cos(angle) * extra / math.sqrt(length)
    sine = np.sin(angle) * extra / math.sqrt(length)
    inverse = np.block([[cosine, sine], [-sine, cosine]])
    parts = []
    for table in (inverse, inverse.T):
        high = table.astype(np.float32).astype(half)
        low = (table - high.astype(np.float64)).astype(half)
        parts += [high, low]
    return np.stack(parts)


def halves(values):
    high = values.astype(half)
    return high, (values - high.astype(single)).astype(half)


def product(first, second):
    dot = functools.partial(jnp.dot, preferred_element_type=single)
    return dot(first[0], second[0]) + (dot(first[0], second[1]) + dot(first[1], second[0]))


def twiddled(pair, step, span, sign):
    real, imag = pair
    if step == 0:
        return real, imag
    if 2 * step == span:
        return (-imag, real) if sign > 0 else (imag, -real)
    angle = math.pi * step / span
    cosine, sine = math.cos(angle), sign * math.sin(angle)
    return real * cosine - imag * sine, real * sine + imag * cosine


def to_voxels(points):
    points = list(points)
    span = 1
    while span < len(points):
        for base in range(0, len(points), 2 * span):
            for step in range(span):
                a = points[base + step]
                t = twiddled(points[base + step + span], step, span, 1.0)
                points[base + step] = (a[0] + t[0], a[1] + t[1])
                points[base + step + span] = (a[0] - t[0], a[1] - t[1])
        span *= 2
    return points


def to_waves(points):
    points = list(points)
    span = len(points) // 2
    while span >= 1:
        for base in range(0, len(points), 2 * span):
            for step in range(span):
                a, t = points[base + step], points[base + step + span]
                points[base + step] = (a[0] + t[0], a[1] + t[1])
                points[base + step + span] = twiddled(
                    (a[0] - t[0], a[1] - t[1]), step, span, -1.0
                )
        span //= 2
    return points


def operator_kernel(
    groups,
    coeffs_hbm,
    material_hbm,
    diag_hbm,
    off_hbm,
    table_hbm,
    theta_ref,
    gram_ref,
    coeffs_ref,
    material_ref,
    table_ref,
    diag_ref,
    off_ref,
    slab_ref,
    tensor_ref,
    high_ref,
    low_ref,
    back_ref,
    pair_ref,
    other_ref,
    swap_ref,
    result_ref,
    return_ref,
    out1_ref,
    in1_ref,
    field_ref,
    scaled_ref,
    out2_ref,
    in2_ref,
    out3_ref,
    in3_ref,
    acc_ref,
    sums_ref,
    load_sem,
    slab_send,
    slab_recv,
    half_sem,
    send1,
    recv1,
    send2,
    recv2,
    send3,
    recv3,
    send4,
    recv4,
    swap_send,
    swap_recv,
    return_send,
    return_recv,
    other_send,
    other_recv,
    sums_send,
    sums_recv,
):
    _, comps, bands, depth, height, breadth = coeffs_ref.shape
    total = depth * groups
    members = groups // 2
    columns = height // members
    levels = groups.bit_length() - 1
    me = lax.axis_index("gz")
    mine = lax.axis_index("ba")
    side = me // members
    seat = me % members
    partner = (me + members) % groups
    pack = members // 2
    inner = seat // pack == 1 - side
    outer = jnp.logical_not(inner)
    odd = seat % 2 == 1
    direct = jnp.logical_and(inner, jnp.logical_not(odd))
    second_guest = jnp.logical_or(inner, odd)
    mate = {"ba": 1 - mine}
    step_rows = 16
    steps = height // step_rows

    def each_peer(body):
        def step(k, carry):
            body(k, (me + k) % groups, (me + groups - k) % groups)
            return carry

        lax.fori_loop(1, groups, step, 0)

    def each_member(body):
        def step(k, carry):
            body(k, (seat + k) % members, (seat + members - k) % members)
            return carry

        lax.fori_loop(1, members, step, 0)

    barrier = pltpu.get_barrier_semaphore()
    each_peer(
        lambda k, peer, source: pl.semaphore_signal(
            barrier, inc=1, device_id={"gz": peer}, device_id_type=MESH
        )
    )
    pl.semaphore_signal(barrier, inc=1, device_id=mate, device_id_type=MESH)

    def row_load(b, row, n):
        return pltpu.make_async_copy(
            coeffs_hbm.at[:, :, b, row], coeffs_ref.at[:, :, b, row], load_sem.at[n, row]
        )

    loads = [
        pltpu.make_async_copy(table_hbm, table_ref, load_sem.at[2, 0]),
        pltpu.make_async_copy(material_hbm, material_ref, load_sem.at[2, 1]),
        pltpu.make_async_copy(diag_hbm, diag_ref, load_sem.at[3, 0]),
        pltpu.make_async_copy(off_hbm, off_ref, load_sem.at[3, 1]),
    ]
    for row in range(depth):
        row_load(1 - side, row, 0).start()
    for row in range(depth):
        row_load(side, row, 1).start()
    for load in loads:
        load.start()

    def signed(number, length):
        return number - length * (number // (length // 2))

    def row_number(owner, row):
        reversed_owner = 0
        for position in range(levels):
            bit = (owner // (1 << position)) % 2
            reversed_owner = reversed_owner + bit * (1 << (levels - 1 - position))
        return signed(reversed_owner + groups * row, total)

    def inverse_of(values):
        zero = values == 0
        return jnp.where(zero, 0.0, 1.0 / jnp.where(zero, 1, values).astype(single))

    class Waves:
        def __init__(self, owner, row, i):
            shape = (step_rows, breadth)
            nx = lax.broadcasted_iota(jnp.int32, shape, 1)
            ny = lax.broadcasted_iota(jnp.int32, shape, 0) + i * step_rows
            nx = jnp.where(nx < breadth // 2, nx, nx - breadth)
            ny = jnp.where(ny < height // 2, ny, ny - height)
            nz = jnp.full(shape, row_number(owner, row), jnp.int32)
            self.x = nx.astype(single) / (breadth / 2.0)
            self.y = ny.astype(single) / (height / 2.0)
            self.z = nz.astype(single) / (total / 2.0)
            ax, ay, az = jnp.abs(nx) * total, jnp.abs(ny) * total, jnp.abs(nz) * breadth
            self.is_x = (ax >= ay) & (ax >= az)
            self.is_y = ay >= az
            self.numbers = (nx, ny, nz)

        def cross(self, v):
            q = (self.x, self.y, self.z)
            return [
                q[(c + 1) % 3] * v[(c + 2) % 3] - q[(c + 2) % 3] * v[(c + 1) % 3]
                for c in range(3)
            ]

        def pick(self, first, second, third):
            return jnp.where(self.is_x, first, jnp.where(self.is_y, second, third))

        def inverse(self):
            nx, ny, nz = self.numbers
            scaled = self.pick(nx * total, ny * total, nz * breadth)
            return inverse_of(scaled) * (total * breadth / 2.0)

        def ratios(self):
            inverse = self.inverse()
            return (
                self.pick(self.y, self.z, self.x) * inverse,
                self.pick(self.z, self.x, self.y) * inverse,
            )

        def reduce(self, v):
            return self.pick(v[1], v[2], v[0]), self.pick(v[2], v[0], v[1])

        def rebuild(self, ratios, first, second):
            last = -(ratios[0] * first + ratios[1] * second)
            return [
                self.pick(last, second, first),
                self.pick(first, last, second),
                self.pick(second, first, last),
            ]

    def rows_of(i):
        return pl.ds(pl.multiple_of(i * step_rows, step_rows), step_rows)

    def each_step(row, body):
        def step(i, carry):
            body(row, i)
            return carry

        lax.fori_loop(0, steps, step, 0)

    def each_row(body):
        def step(row, carry):
            body(row)
            return carry

        lax.fori_loop(0, depth, step, 0)

    def put_halves(curls, p, row, i):
        at = pl.ds(pl.multiple_of(p * height + i * step_rows, step_rows), step_rows)
        for c in range(3):
            high, low = halves(curls[c])
            lanes = pl.ds(c * breadth, breadth)
            high_ref[row, at, lanes] = high
            low_ref[row, at, lanes] = low

    def put_pair(b, p, row, i, pair):
        for n in range(2):
            pair_ref[b, row, n, p, rows_of(i), :] = pair[n]

    def away_step(row, i):
        waves = Waves(me, row, i)
        for p in range(2):
            values = [coeffs_ref[p, c, 1 - side, row, rows_of(i), :] for c in range(3)]
            put_pair(1 - side, p, row, i, waves.reduce(waves.cross(values)))

    def home_step(row, i):
        waves = Waves(me, row, i)
        for p in range(2):
            values = [coeffs_ref[p, c, side, row, rows_of(i), :] for c in range(3)]
            curls = waves.cross(values)
            put_halves(curls, p, row, i)
            put_pair(side, p, row, i, waves.reduce(curls))

    def direct_step(row, i):
        waves = Waves(me, row, i)
        for p in range(2):
            values = [coeffs_ref[p, c, 1 - side, row, rows_of(i), :] for c in range(3)]
            put_halves(waves.cross(values), p, row, i)

    def guest_step(row, i):
        waves = Waves(partner, row, i)
        ratios = waves.ratios()
        for p in range(2):
            pair = [swap_ref[row, n, p, rows_of(i), :] for n in range(2)]
            put_halves(waves.rebuild(ratios, *pair), p, row, i)

    def plain_table():
        return table_ref[0], table_ref[1]

    def turned_table():
        return table_ref[2], table_ref[3]

    def gather_blocks(values):
        top, bottom = values[:height], values[height:]
        return jnp.concatenate(
            [
                jnp.concatenate(
                    [
                        top[:, z * breadth : (z + 1) * breadth],
                        bottom[:, z * breadth : (z + 1) * breadth],
                    ],
                    axis=1,
                )
                for z in range(3)
            ],
            axis=0,
        )

    def spread_blocks(values):
        return jnp.concatenate(
            [
                jnp.concatenate(
                    [
                        values[z * height : (z + 1) * height, p * breadth : (p + 1) * breadth]
                        for z in range(3)
                    ],
                    axis=1,
                )
                for p in range(2)
            ],
            axis=0,
        )

    def to_peer(out, into, send, recv, s, row, k, peer, from_at, to_at):
        return pltpu.make_async_remote_copy(
            src_ref=out.at[from_at, row, peer],
            dst_ref=into.at[to_at, row, seat],
            send_sem=send.at[s, row, k],
            recv_sem=recv.at[s, row, k],
            device_id={"gz": side * members + peer},
            device_id_type=MESH,
        )

    def from_peer(out, into, send, recv, s, row, k, source, from_at, to_at):
        return pltpu.make_async_remote_copy(
            src_ref=out.at[from_at, row, source],
            dst_ref=into.at[to_at, row, source],
            send_sem=send.at[s, row, k],
            recv_sem=recv.at[s, row, k],
            device_id={"gz": side * members + source},
            device_id_type=MESH,
        )

    def ends1(s):
        return s, (side + s) % 2

    def ends2(s):
        return (side + s) % 2, s

    def start_all(out, into, send, recv, s, row, ends):
        each_member(
            lambda k, peer, source: to_peer(
                out, into, send, recv, s, row, k, peer, *ends
            ).start()
        )
        into[ends[1], row, seat] = out[ends[0], row, seat]

    def is_inner(peer):
        return peer // pack == 1 - side

    def each_inner(body):
        def one(k, peer, source):
            pl.when(is_inner(peer))(lambda: body(k, peer))

        each_member(one)

    def each_second_source(body):
        def one(k, peer, source):
            has_guest = jnp.logical_or(is_inner(source), source % 2 == 1)
            pl.when(has_guest)(lambda: body(k, source))

        each_member(one)

    def across(peer):
        return {"gz": (1 - side) * members + peer}

    def direct_copy(peer):
        return pltpu.make_async_remote_copy(
            src_ref=out3_ref.at[peer],
            dst_ref=in1_ref.at[side, 1, seat],
            send_sem=send3.at[peer],
            recv_sem=recv3.at[seat % pack // 2],
            device_id=across(peer),
            device_id_type=MESH,
        )

    def direct_arrival(n):
        source = side * pack + 2 * n
        return pltpu.make_async_remote_copy(
            src_ref=out3_ref.at[source],
            dst_ref=in1_ref.at[1 - side, 1, source],
            send_sem=send3.at[source],
            recv_sem=recv3.at[n],
            device_id=across(source),
            device_id_type=MESH,
        )

    def direct_result(n):
        peer = side * pack + n
        return pltpu.make_async_remote_copy(
            src_ref=out2_ref.at[1 - side, 1, peer],
            dst_ref=in3_ref.at[seat],
            send_sem=send4.at[n],
            recv_sem=recv4.at[seat],
            device_id=across(peer),
            device_id_type=MESH,
        )

    def result_arrival(source):
        return pltpu.make_async_remote_copy(
            src_ref=out2_ref.at[1 - side, 1, source],
            dst_ref=in3_ref.at[source],
            send_sem=send4.at[source % pack],
            recv_sem=recv4.at[source],
            device_id=across(source),
            device_id_type=MESH,
        )

    def each_of(count, body):
        def step(n, carry):
            body(n)
            return carry

        lax.fori_loop(0, count, step, 0)

    def finish_all(out, into, send, recv, s, row, ends):
        each_member(
            lambda k, peer, source: from_peer(
                out, into, send, recv, s, row, k, source, *ends
            ).wait_recv()
        )

    def drain_all(out, into, send, recv, s, row, ends):
        each_member(
            lambda k, peer, source: to_peer(
                out, into, send, recv, s, row, k, peer, *ends
            ).wait_send()
        )

    first = (out1_ref, in1_ref, send1, recv1)
    second = (out2_ref, in2_ref, send2, recv2)

    def planes_into(put, row):
        tall = product(turned_table(), (high_ref[row], low_ref[row]))
        wide = product(halves(gather_blocks(tall)), plain_table())
        for p in range(2):
            for c in range(3):
                plane = wide[c * height : (c + 1) * height, p * breadth : (p + 1) * breadth]
                put(c, p, plane.reshape(members, columns, breadth))

    def make_planes(s, row):
        def put(c, p, block):
            out1_ref[s, row, :, c, p] = block

        planes_into(put, row)

    def swap_copy(row):
        return pltpu.make_async_remote_copy(
            src_ref=pair_ref.at[1 - side, row],
            dst_ref=swap_ref.at[row],
            send_sem=swap_send.at[row],
            recv_sem=swap_recv.at[row],
            device_id={"gz": partner},
            device_id_type=MESH,
        )

    def return_copy(row):
        return pltpu.make_async_remote_copy(
            src_ref=result_ref.at[row],
            dst_ref=return_ref.at[row],
            send_sem=return_send.at[row],
            recv_sem=return_recv.at[row],
            device_id={"gz": partner},
            device_id_type=MESH,
        )

    def other_copy(b, n):
        return pltpu.make_async_remote_copy(
            src_ref=pair_ref.at[b],
            dst_ref=other_ref.at[b],
            send_sem=other_send.at[n],
            recv_sem=other_recv.at[n],
            device_id=mate,
            device_id_type=MESH,
        )

    def columns_of(peer):
        return pl.ds(pl.multiple_of((peer % members) * columns, columns), columns)

    def slab_copy(peer, slot, k):
        return pltpu.make_async_remote_copy(
            src_ref=material_ref.at[mine, columns_of(peer), :],
            dst_ref=slab_ref.at[mine, slot],
            send_sem=slab_send.at[k],
            recv_sem=slab_recv.at[k],
            device_id={"gz": peer},
            device_id_type=MESH,
        )

    def half_copy(row, part):
        at = pl.ds(pl.multiple_of(part * members, members), members)
        return pltpu.make_async_remote_copy(
            src_ref=slab_ref.at[row, at],
            dst_ref=slab_ref.at[row, at],
            send_sem=half_sem.at[0, part],
            recv_sem=half_sem.at[1, part],
            device_id=mate,
            device_id_type=MESH,
        )

    def away_row(row):
        row_load(1 - side, row, 0).wait()
        each_step(row, away_step)

    def home_row(row):
        row_load(side, row, 1).wait()
        each_step(row, home_step)
        make_planes(0, row)
        start_all(*first, 0, row, ends1(0))

    def start_slabs(base):
        def step(k, carry):
            peer = base * members + (seat + k) % members
            slab_copy(peer, me, (peer + groups - me) % groups).start()
            return carry

        return step

    def wait_slabs(base):
        def step(k, carry):
            source = base * members + (seat + members - k) % members
            slab_copy(source, source, (me + groups - source) % groups).wait_recv()
            return carry

        return step

    away_row(0)
    pl.semaphore_wait(barrier, groups)
    swap_copy(0).start()
    for load in loads:
        load.wait()
    lax.fori_loop(1, members, start_slabs(side), 0)
    lax.fori_loop(0, members, start_slabs(1 - side), 0)
    away_row(1)
    pl.when(jnp.logical_not(direct))(lambda: swap_copy(1).start())
    slab_ref[mine, me] = material_ref[mine, columns_of(me), :]
    home_row(0)
    home_row(1)

    def make_direct():
        each_step(1, direct_step)

        def put(c, p, block):
            out3_ref[:, c, p] = block

        planes_into(put, 1)

    def send_direct():
        each_of(members, lambda n: direct_copy((seat + n) % members).start())

    pl.when(direct)(make_direct)
    other_copy(side, 1).start()
    acc_ref[...] = jnp.zeros(acc_ref.shape, single)

    def guest_row(row):
        swap_copy(row).wait_recv()
        each_step(row, guest_step)
        make_planes(1, row)
        start_all(*first, 1, row, ends1(1))

    guest_row(0)
    lax.fori_loop(1, members, wait_slabs(side), 0)
    half_copy(mine, side).start()
    pl.when(inner)(lambda: guest_row(1))
    lax.fori_loop(0, members, wait_slabs(1 - side), 0)
    half_copy(mine, 1 - side).start()
    pl.when(direct)(send_direct)
    pl.when(jnp.logical_and(outer, odd))(lambda: guest_row(1))
    half_copy(1 - mine, side).wait_recv()
    half_copy(1 - mine, 1 - side).wait_recv()
    kinds = diag_ref.shape[0]

    def tensor_step(owner, carry):
        for row in range(depth):
            codes = slab_ref[row, owner]
            for entry in range(6):
                table = diag_ref if entry < 3 else off_ref
                values = jnp.full(codes.shape, table[0, entry % 3], single)
                for kind in range(1, kinds):
                    values = jnp.where(codes == kind, table[kind, entry % 3], values)
                tensor_ref[entry, owner, row] = values
        return carry

    lax.fori_loop(0, groups, tensor_step, 0)

    def part_of(n):
        return pl.ds(pl.multiple_of(n * 8, 8), 8)

    each_row(lambda row: finish_all(*first, 0, row, ends1(0)))
    finish_all(*first, 1, 0, ends1(1))
    each_second_source(lambda k, source: from_peer(*first, 1, 1, k, source, *ends1(1)).wait_recv())
    each_of(pack // 2, lambda n: direct_arrival(n).wait_recv())

    def inverse(n, carry):
        c, at = n // (columns // 8), part_of(n % (columns // 8))
        points = []
        for r in range(total):
            owner, row = r // depth, r % depth
            where = (owner // members, row, owner % members, c)
            points.append((in1_ref[(*where, 0, at)], in1_ref[(*where, 1, at)]))
        for z, (real, imag) in enumerate(to_voxels(points)):
            field_ref[c, 0, z, at] = real
            field_ref[c, 1, z, at] = imag
        return carry

    lax.fori_loop(0, 3 * (columns // 8), inverse, 0)

    def scale(z, carry):
        xx, yy, zz, xy, yz, zx = [tensor_ref[entry, z // depth, z % depth] for entry in range(6)]
        for p in range(2):
            fx, fy, fz = [field_ref[c, p, z] for c in range(3)]
            scaled_ref[0, p, z] = xx * fx + xy * fy + zx * fz
            scaled_ref[1, p, z] = xy * fx + yy * fy + yz * fz
            scaled_ref[2, p, z] = zx * fx + yz * fy + zz * fz
        return carry

    lax.fori_loop(0, total, scale, 0, unroll=2)

    def forward(n, carry):
        c, at = n // (columns // 8), part_of(n % (columns // 8))
        points = [(scaled_ref[c, 0, z, at], scaled_ref[c, 1, z, at]) for z in range(total)]
        for r, (real, imag) in enumerate(to_waves(points)):
            owner, row = r // depth, r % depth
            where = (owner // members, row, owner % members, c)
            out2_ref[(*where, 0, at)] = real
            out2_ref[(*where, 1, at)] = imag
        return carry

    lax.fori_loop(0, 3 * (columns // 8), forward, 0)
    start_all(*second, 1, 0, ends2(1))
    each_of(pack, lambda n: direct_result((seat + n) % pack).start())
    each_inner(lambda k, peer: to_peer(*second, 1, 1, k, peer, *ends2(1)).start())

    def keep_guest():
        in2_ref[1, 1, seat] = out2_ref[1 - side, 1, seat]

    pl.when(inner)(keep_guest)

    def start_home():
        each_row(lambda row: start_all(*second, 0, row, ends2(0)))

    pl.when(inner)(start_home)
    other_copy(1 - side, 0).start()

    def planes_back(get, row):
        planes = jnp.concatenate(
            [
                jnp.concatenate(
                    [get(c, p).reshape(height, breadth) for p in range(2)], axis=1
                )
                for c in range(3)
            ],
            axis=0,
        )
        wide = product(halves(planes), turned_table())
        back_ref[row] = product(plain_table(), halves(spread_blocks(wide)))

    def take_planes(s, row):
        finish_all(*second, s, row, ends2(s))
        planes_back(lambda c, p: in2_ref[s, row, :, c, p], row)

    def theta_at(waves, p, row, i):
        at = pl.ds(pl.multiple_of(p * height + i * step_rows, step_rows), step_rows)
        lanes = [pl.ds(c * breadth, breadth) for c in range(3)]
        return [-v for v in waves.cross([back_ref[row, at, lanes[c]] for c in range(3)])]

    def guest_result(row, i):
        waves = Waves(partner, row, i)
        for p in range(2):
            pair = waves.reduce(theta_at(waves, p, row, i))
            for n in range(2):
                result_ref[row, n, p, rows_of(i), :] = pair[n]

    def add_sums(waves, pairs, row, i, sums):
        inverse = waves.inverse()
        (real1, real2), (imag1, imag2) = [[inverse * v for v in pair] for pair in pairs]
        sums = list(sums)
        n = 0
        for source in (pair_ref, other_ref):
            for a in range(bands):
                one_real, one_imag = [source[a, row, 0, p, rows_of(i), :] for p in range(2)]
                two_real, two_imag = [source[a, row, 1, p, rows_of(i), :] for p in range(2)]
                real = (two_real * real1 + two_imag * imag1) - (one_real * real2 + one_imag * imag2)
                imag = (two_real * imag1 - two_imag * real1) - (one_real * imag2 - one_imag * real2)
                sums[n] = sums[n] + real
                sums[n + 1] = sums[n + 1] + imag
                n += 2
        return tuple(sums)

    def each_sum(row, b, body):
        def step(i, sums):
            return body(row, i, sums)

        sums = lax.fori_loop(0, steps, step, tuple(acc_ref[b, n] for n in range(4 * bands)))
        for n in range(4 * bands):
            acc_ref[b, n] = sums[n]

    def keep_sums(b):
        sums = [acc_ref[b, n] for n in range(4 * bands)]
        lane = lax.broadcasted_iota(jnp.int32, (1, breadth), 1)
        rows = [jnp.zeros((1, breadth), single)] * 2
        n = 0
        for source in (mine, 1 - mine):
            for a in range(bands):
                for p in range(2):
                    value = jnp.sum(jnp.sum(sums[n], axis=0, keepdims=True), axis=1, keepdims=True)
                    rows[p] = rows[p] + jnp.where(lane == source * bands + a, value, 0.0)
                    n += 1
        sums_ref[me, b] = jnp.concatenate(rows, axis=0) * (1.0 / (breadth * height * total))

    def result_of(b):
        def result(row, i, sums):
            waves = Waves(me, row, i)
            pairs = []
            for p in range(2):
                theta = theta_at(waves, p, row, i)
                for c in range(3):
                    theta_ref[p, c, b, row, rows_of(i), :] = theta[c]
                pairs.append(waves.reduce(theta))
            return add_sums(waves, pairs, row, i, sums)

        return result

    def away_result(row, i, sums):
        waves = Waves(me, row, i)
        ratios = waves.ratios()
        pairs = []
        for p in range(2):
            pair = [return_ref[row, n, p, rows_of(i), :] for n in range(2)]
            theta = waves.rebuild(ratios, *pair)
            for c in range(3):
                theta_ref[p, c, 1 - side, row, rows_of(i), :] = theta[c]
            pairs.append(pair)
        return add_sums(waves, pairs, row, i, sums)

    def sums_copy(slot, peer, k):
        return pltpu.make_async_remote_copy(
            src_ref=sums_ref.at[slot],
            dst_ref=sums_ref.at[slot],
            send_sem=sums_send.at[k],
            recv_sem=sums_recv.at[k],
            device_id={"gz": peer},
            device_id_type=MESH,
        )

    def guest_back(row):
        take_planes(1, row)
        each_step(row, guest_result)
        return_copy(row).start()

    guest_back(0)
    pl.when(outer)(start_home)
    pl.when(inner)(lambda: guest_back(1))
    other_copy(side, 1).wait_recv()
    other_copy(1 - side, 0).wait_recv()

    def take_direct():
        each_of(members, lambda n: result_arrival(n).wait_recv())
        planes_back(lambda c, p: in3_ref[:, c, p], 1)
        each_sum(1, 1 - side, result_of(1 - side))

    pl.when(inner)(take_direct)

    def home_back(row):
        take_planes(0, row)
        each_sum(row, side, result_of(side))

    home_back(0)
    home_back(1)
    keep_sums(side)

    def away_back(row):
        return_copy(row).wait_recv()
        each_sum(row, 1 - side, away_result)

    away_back(0)
    pl.when(outer)(lambda: away_back(1))
    keep_sums(1 - side)
    each_peer(lambda k, peer, source: sums_copy(me, peer, k).start())
    half_copy(mine, side).wait_send()
    half_copy(mine, 1 - side).wait_send()
    each_peer(lambda k, peer, source: slab_copy(peer, me, k).wait_send())
    other_copy(1 - side, 0).wait_send()
    other_copy(side, 1).wait_send()
    swap_copy(0).wait_send()
    return_copy(0).wait_send()
    pl.when(jnp.logical_not(direct))(lambda: swap_copy(1).wait_send())

    pl.when(direct)(lambda: each_of(members, lambda n: direct_copy(n).wait_send()))
    pl.when(second_guest)(lambda: drain_all(*first, 1, 1, ends1(1)))
    pl.when(inner)(lambda: return_copy(1).wait_send())
    each_inner(lambda k, peer: to_peer(*second, 1, 1, k, peer, *ends2(1)).wait_send())
    each_of(pack, lambda n: direct_result(n).wait_send())
    drain_all(*first, 1, 0, ends1(1))
    drain_all(*second, 1, 0, ends2(1))
    each_row(lambda row: drain_all(*first, 0, row, ends1(0)))
    each_row(lambda row: drain_all(*second, 0, row, ends2(0)))
    each_peer(lambda k, peer, source: sums_copy(source, source, k).wait_recv())
    grams = jnp.sum(sums_ref[...], axis=0)
    for p in range(2):
        for b in range(bands):
            gram_ref[p, b : b + 1, :] = grams[b, p : p + 1, : 2 * bands]
    each_peer(lambda k, peer, source: sums_copy(me, peer, k).wait_send())


def on_device_kernel(coeffs, material, inv_diag, inv_off):
    groups = lax.axis_size("gz")
    _, comps, bands, depth, height, breadth = coeffs.shape
    total = depth * groups
    members = groups // 2
    columns = height // members
    table = jnp.asarray(split_table(breadth, total**-0.25))
    voxels = (3, 2, total, columns, breadth)
    block = (2, depth, members, 3, 2, columns, breadth)
    pairs = (depth, 2, 2, height, breadth)
    vmem = pl.BlockSpec(memory_space=pltpu.VMEM)
    hbm = pl.BlockSpec(memory_space=pltpu.HBM)
    dma = pltpu.SemaphoreType.DMA
    operands = [
        pltpu.with_memory_space_constraint(v, pltpu.HBM)
        for v in (coeffs, material, inv_diag, inv_off, table)
    ]
    theta, gram = pl.pallas_call(
        functools.partial(operator_kernel, groups),
        out_shape=(
            jax.ShapeDtypeStruct(coeffs.shape, single),
            jax.ShapeDtypeStruct((2, bands, 2 * bands), single),
        ),
        in_specs=[hbm, hbm, hbm, hbm, hbm],
        out_specs=(vmem, vmem),
        scratch_shapes=[
            pltpu.VMEM(coeffs.shape, single),
            pltpu.VMEM(material.shape, jnp.int32),
            pltpu.VMEM(table.shape, half),
            pltpu.SMEM(inv_diag.shape, single),
            pltpu.SMEM(inv_off.shape, single),
            pltpu.VMEM((depth, groups, columns, breadth), jnp.int32),
            pltpu.VMEM((6, groups, depth, columns, breadth), single),
            pltpu.VMEM((depth, 2 * height, 3 * breadth), half),
            pltpu.VMEM((depth, 2 * height, 3 * breadth), half),
            pltpu.VMEM((depth, 2 * height, 3 * breadth), single),
            pltpu.VMEM((bands, *pairs), single),
            pltpu.VMEM((bands, *pairs), single),
            pltpu.VMEM(pairs, single),
            pltpu.VMEM(pairs, single),
            pltpu.VMEM(pairs, single),
            pltpu.VMEM(block, single),
            pltpu.VMEM(block, single),
            pltpu.VMEM(voxels, single),
            pltpu.VMEM(voxels, single),
            pltpu.VMEM(block, single),
            pltpu.VMEM(block, single),
            pltpu.VMEM(block[2:], single),
            pltpu.VMEM(block[2:], single),
            pltpu.VMEM((bands, 4 * bands, 16, breadth), single),
            pltpu.VMEM((groups, bands, 2, breadth), single),
            dma((4, depth)),
            dma((groups,)),
            dma((groups,)),
            dma((2, 2)),
            dma((2, depth, members)),
            dma((2, depth, members)),
            dma((2, depth, members)),
            dma((2, depth, members)),
            dma((members,)),
            dma((members // 4,)),
            dma((members // 2,)),
            dma((members,)),
            dma((depth,)),
            dma((depth,)),
            dma((depth,)),
            dma((depth,)),
            dma((2,)),
            dma((2,)),
            dma((groups,)),
            dma((groups,)),
        ],
        compiler_params=pltpu.CompilerParams(
            collective_id=0, has_side_effects=True, vmem_limit_bytes=48 * 1024 * 1024
        ),
        name="maxwell",
    )(*operands)
    return (theta, gram.transpose(0, 2, 1))


def fits(coeffs):
    groups = lax.axis_size("gz")
    _, _, bands, depth, height, breadth = coeffs.shape
    return (
        lax.axis_size("ba") == 2
        and bands == 2
        and depth == 2
        and groups >= 8
        and height % (4 * groups) == 0
        and height % 16 == 0
        and height == breadth
        and breadth % 128 == 0
    )


def on_either(coeffs, material, inv_diag, inv_off):
    chosen = on_device_kernel if fits(coeffs) else on_device
    return chosen(coeffs, material, inv_diag, inv_off)


def solution(mesh):
    in_specs = (P(None, None, "ba", "gz", None, None), P("gz", None, None), P(), P())
    out_specs = (P(None, None, "ba", "gz", None, None), P(None, None, "ba"))
    return jax.shard_map(
        on_either, mesh=mesh, in_specs=in_specs, out_specs=out_specs, check_vma=False
    )
```

```python
import functools
import math

import jax
import jax.numpy as jnp
import numpy as np
from jax import lax
from jax.experimental import pallas as pl
from jax.experimental.pallas import tpu as pltpu
from jax.sharding import PartitionSpec as P

highest = lax.Precision.HIGHEST
half_turn = 3.141592653589793


def reverse_bits(values, levels):
    flipped = jnp.zeros_like(values)
    for position in range(levels):
        flipped = flipped + (values >> position & 1) * (1 << levels - 1 - position)
    return flipped


def signed_wave(numbers, length):
    shifted = jnp.where(numbers < length // 2, numbers, numbers - length)
    return shifted.astype(jnp.float32) / (length / 2.0)


def phase_tables(first, second, length, sign):
    product = first[:, None] * second[None, :] % length
    angle = 2.0 * half_turn / length * product.astype(jnp.float32)
    factor = 1.0 / math.sqrt(length)
    return (jnp.cos(angle) * factor, sign * jnp.sin(angle) * factor)


def cross_waves(waves, field):
    first, second, third = waves
    return jnp.stack(
        [
            second * field[:, 2] - third * field[:, 1],
            third * field[:, 0] - first * field[:, 2],
            first * field[:, 1] - second * field[:, 0],
        ],
        axis=1,
    )


def along_width(field, cosine, sine):
    breadth = field.shape[-1]
    rows = field.reshape(2, -1, breadth)
    joined = jnp.concatenate([cosine, sine], axis=1)
    real_prod = jnp.dot(rows[0], joined, precision=highest)
    imag_prod = jnp.dot(rows[1], joined, precision=highest)
    real_out = real_prod[:, :breadth] - imag_prod[:, breadth:]
    imag_out = real_prod[:, breadth:] + imag_prod[:, :breadth]
    return jnp.stack([real_out, imag_out]).reshape(field.shape)


def along_height(field, cosine, sine):
    tables = jnp.stack([cosine, sine])
    product = jnp.einsum("pcbzyx,tyk->tpcbzkx", field, tables, precision=highest)
    return jnp.stack([product[0, 0] - product[1, 1], product[1, 0] + product[0, 1]])


def along_depth(field, cosine, sine):
    tables = jnp.stack([cosine, sine])
    product = jnp.einsum("pcbzyx,tzk->tpcbkyx", field, tables, precision=highest)
    return jnp.stack([product[0, 0] - product[1, 1], product[1, 0] + product[0, 1]])


def apply_material(field, material, inv_diag, inv_off):
    materials = inv_diag.shape[0]
    onehot = (material[None] == jnp.arange(materials, dtype=jnp.int32)[:, None, None, None]).astype(
        jnp.float32
    )
    table = jnp.concatenate([inv_diag, inv_off], axis=1)
    tensor = jnp.einsum("mk,mzyx->kzyx", table, onehot, precision=highest)
    first = field[:, 0]
    second = field[:, 1]
    third = field[:, 2]
    return jnp.stack(
        [
            tensor[0] * first + tensor[3] * second + tensor[5] * third,
            tensor[3] * first + tensor[1] * second + tensor[4] * third,
            tensor[5] * first + tensor[4] * second + tensor[2] * third,
        ],
        axis=1,
    )


def on_device(coeffs, material, inv_diag, inv_off):
    groups = lax.axis_size("gz")
    levels = groups.bit_length() - 1
    depth = coeffs.shape[3]
    height = coeffs.shape[4]
    breadth = coeffs.shape[5]
    total_depth = depth * groups
    device = lax.axis_index("gz")
    local_rows = jnp.arange(depth, dtype=jnp.int32)
    waves_here = reverse_bits(device, levels) + groups * local_rows
    across = jnp.arange(breadth, dtype=jnp.int32)
    upward = jnp.arange(height, dtype=jnp.int32)
    waves = (
        signed_wave(across, breadth)[None, None, :],
        signed_wave(upward, height)[None, :, None],
        signed_wave(waves_here, total_depth)[:, None, None],
    )
    curl = cross_waves(waves, coeffs)
    all_rows = jnp.arange(total_depth, dtype=jnp.int32)
    wave_rows = reverse_bits(all_rows // depth, levels) + groups * (all_rows % depth)
    height_cos, height_sin = phase_tables(upward, upward, height, 1.0)
    width_cos, width_sin = phase_tables(across, across, breadth, 1.0)
    planar = along_height(curl, height_cos, height_sin)
    planar = along_width(planar, width_cos, width_sin)
    material_slab = lax.all_to_all(material, "gz", split_axis=1, concat_axis=0, tiled=True)
    inverse_cos, inverse_sin = phase_tables(wave_rows, all_rows, total_depth, 1.0)
    forward_cos, forward_sin = phase_tables(all_rows, wave_rows, total_depth, -1.0)
    spatial_piece = along_depth(
        lax.all_to_all(planar, "gz", split_axis=4, concat_axis=3, tiled=True),
        inverse_cos,
        inverse_sin,
    )
    scaled_piece = apply_material(spatial_piece, material_slab, inv_diag, inv_off)
    returned = along_depth(scaled_piece, forward_cos, forward_sin)
    spectral = lax.all_to_all(returned, "gz", split_axis=3, concat_axis=4, tiled=True)
    spectral = along_width(spectral, width_cos, -width_sin)
    spectral = along_height(spectral, height_cos, -height_sin)
    theta = -cross_waves(waves, spectral)
    factor = 1.0 / (breadth * height * total_depth)
    piece = lax.all_gather(coeffs, "ba", axis=2, tiled=True)
    real_part = jnp.einsum("cbzyx,cezyx->be", piece[0], theta[0], precision=highest) + jnp.einsum(
        "cbzyx,cezyx->be", piece[1], theta[1], precision=highest
    )
    imag_part = jnp.einsum("cbzyx,cezyx->be", piece[0], theta[1], precision=highest) - jnp.einsum(
        "cbzyx,cezyx->be", piece[1], theta[0], precision=highest
    )
    block = jnp.stack([real_part, imag_part]) * factor
    gram = lax.psum(block, "gz")
    return (theta, gram)


MESH = pl.DeviceIdType.MESH
single = jnp.float32
half = jnp.bfloat16


def split_table(length, extra):
    numbers = np.arange(length)
    angle = 2.0 * np.pi / length * (numbers[:, None] * numbers[None, :] % length)
    cosine = np.cos(angle) * extra / math.sqrt(length)
    sine = np.sin(angle) * extra / math.sqrt(length)
    inverse = np.block([[cosine, sine], [-sine, cosine]])
    parts = []
    for table in (inverse, inverse.T):
        high = table.astype(np.float32).astype(half)
        low = (table - high.astype(np.float64)).astype(half)
        parts += [high, low]
    return np.stack(parts)


def halves(values):
    high = values.astype(half)
    return high, (values - high.astype(single)).astype(half)


def product(first, second):
    dot = functools.partial(jnp.dot, preferred_element_type=single)
    return dot(first[0], second[0]) + (dot(first[0], second[1]) + dot(first[1], second[0]))


def twiddled(pair, step, span, sign):
    real, imag = pair
    if step == 0:
        return real, imag
    if 2 * step == span:
        return (-imag, real) if sign > 0 else (imag, -real)
    angle = math.pi * step / span
    cosine, sine = math.cos(angle), sign * math.sin(angle)
    return real * cosine - imag * sine, real * sine + imag * cosine


def to_voxels(points):
    points = list(points)
    span = 1
    while span < len(points):
        for base in range(0, len(points), 2 * span):
            for step in range(span):
                a = points[base + step]
                t = twiddled(points[base + step + span], step, span, 1.0)
                points[base + step] = (a[0] + t[0], a[1] + t[1])
                points[base + step + span] = (a[0] - t[0], a[1] - t[1])
        span *= 2
    return points


def to_waves(points):
    points = list(points)
    span = len(points) // 2
    while span >= 1:
        for base in range(0, len(points), 2 * span):
            for step in range(span):
                a, t = points[base + step], points[base + step + span]
                points[base + step] = (a[0] + t[0], a[1] + t[1])
                points[base + step + span] = twiddled(
                    (a[0] - t[0], a[1] - t[1]), step, span, -1.0
                )
        span //= 2
    return points


def operator_kernel(
    groups,
    coeffs_hbm,
    material_hbm,
    diag_hbm,
    off_hbm,
    table_hbm,
    theta_ref,
    gram_ref,
    coeffs_ref,
    material_ref,
    table_ref,
    diag_ref,
    off_ref,
    slab_ref,
    tensor_ref,
    high_ref,
    low_ref,
    back_ref,
    pair_ref,
    other_ref,
    swap_ref,
    result_ref,
    return_ref,
    out1_ref,
    in1_ref,
    field_ref,
    scaled_ref,
    out2_ref,
    in2_ref,
    out3_ref,
    in3_ref,
    acc_ref,
    sums_ref,
    load_sem,
    slab_send,
    slab_recv,
    half_sem,
    send1,
    recv1,
    send2,
    recv2,
    send3,
    recv3,
    send4,
    recv4,
    part_send,
    part_recv,
    swap_send,
    swap_recv,
    return_send,
    return_recv,
    other_send,
    other_recv,
    sums_send,
    sums_recv,
):
    _, comps, bands, depth, height, breadth = coeffs_ref.shape
    total = depth * groups
    members = groups // 2
    columns = height // members
    levels = groups.bit_length() - 1
    me = lax.axis_index("gz")
    mine = lax.axis_index("ba")
    side = me // members
    seat = me % members
    partner = (me + members) % groups
    pack = members // 2
    inner = seat // pack == 1 - side
    outer = jnp.logical_not(inner)
    odd = seat % 2 == 1
    direct = jnp.logical_and(inner, jnp.logical_not(odd))
    second_guest = jnp.logical_or(inner, odd)
    mate = {"ba": 1 - mine}
    step_rows = 16
    steps = height // step_rows

    def each_peer(body):
        def step(k, carry):
            body(k, (me + k) % groups, (me + groups - k) % groups)
            return carry

        lax.fori_loop(1, groups, step, 0)

    def each_member(body):
        def step(k, carry):
            body(k, (seat + k) % members, (seat + members - k) % members)
            return carry

        lax.fori_loop(1, members, step, 0)

    barrier = pltpu.get_barrier_semaphore()
    each_peer(
        lambda k, peer, source: pl.semaphore_signal(
            barrier, inc=1, device_id={"gz": peer}, device_id_type=MESH
        )
    )
    pl.semaphore_signal(barrier, inc=1, device_id=mate, device_id_type=MESH)

    def row_load(b, row, n):
        return pltpu.make_async_copy(
            coeffs_hbm.at[:, :, b, row], coeffs_ref.at[:, :, b, row], load_sem.at[n, row]
        )

    loads = [
        pltpu.make_async_copy(table_hbm, table_ref, load_sem.at[2, 0]),
        pltpu.make_async_copy(material_hbm, material_ref, load_sem.at[2, 1]),
        pltpu.make_async_copy(diag_hbm, diag_ref, load_sem.at[3, 0]),
        pltpu.make_async_copy(off_hbm, off_ref, load_sem.at[3, 1]),
    ]
    for row in range(depth):
        row_load(1 - side, row, 0).start()
    for row in range(depth):
        row_load(side, row, 1).start()
    for load in loads:
        load.start()

    def signed(number, length):
        return number - length * (number // (length // 2))

    def row_number(owner, row):
        reversed_owner = 0
        for position in range(levels):
            bit = (owner // (1 << position)) % 2
            reversed_owner = reversed_owner + bit * (1 << (levels - 1 - position))
        return signed(reversed_owner + groups * row, total)

    def inverse_of(values):
        zero = values == 0
        return jnp.where(zero, 0.0, 1.0 / jnp.where(zero, 1, values).astype(single))

    class Waves:
        def __init__(self, owner, row, i):
            shape = (step_rows, breadth)
            nx = lax.broadcasted_iota(jnp.int32, shape, 1)
            ny = lax.broadcasted_iota(jnp.int32, shape, 0) + i * step_rows
            nx = jnp.where(nx < breadth // 2, nx, nx - breadth)
            ny = jnp.where(ny < height // 2, ny, ny - height)
            nz = jnp.full(shape, row_number(owner, row), jnp.int32)
            self.x = nx.astype(single) / (breadth / 2.0)
            self.y = ny.astype(single) / (height / 2.0)
            self.z = nz.astype(single) / (total / 2.0)
            ax, ay, az = jnp.abs(nx) * total, jnp.abs(ny) * total, jnp.abs(nz) * breadth
            self.is_x = (ax >= ay) & (ax >= az)
            self.is_y = ay >= az
            self.numbers = (nx, ny, nz)

        def cross(self, v):
            q = (self.x, self.y, self.z)
            return [
                q[(c + 1) % 3] * v[(c + 2) % 3] - q[(c + 2) % 3] * v[(c + 1) % 3]
                for c in range(3)
            ]

        def pick(self, first, second, third):
            return jnp.where(self.is_x, first, jnp.where(self.is_y, second, third))

        def inverse(self):
            nx, ny, nz = self.numbers
            scaled = self.pick(nx * total, ny * total, nz * breadth)
            return inverse_of(scaled) * (total * breadth / 2.0)

        def ratios(self):
            inverse = self.inverse()
            return (
                self.pick(self.y, self.z, self.x) * inverse,
                self.pick(self.z, self.x, self.y) * inverse,
            )

        def reduce(self, v):
            return self.pick(v[1], v[2], v[0]), self.pick(v[2], v[0], v[1])

        def rebuild(self, ratios, first, second):
            last = -(ratios[0] * first + ratios[1] * second)
            return [
                self.pick(last, second, first),
                self.pick(first, last, second),
                self.pick(second, first, last),
            ]

    def rows_of(i):
        return pl.ds(pl.multiple_of(i * step_rows, step_rows), step_rows)

    def each_step(row, body):
        def step(i, carry):
            body(row, i)
            return carry

        lax.fori_loop(0, steps, step, 0)

    def each_row(body):
        def step(row, carry):
            body(row)
            return carry

        lax.fori_loop(0, depth, step, 0)

    def put_halves(curls, p, row, i):
        at = pl.ds(pl.multiple_of(p * height + i * step_rows, step_rows), step_rows)
        for c in range(3):
            high, low = halves(curls[c])
            lanes = pl.ds(c * breadth, breadth)
            high_ref[row, at, lanes] = high
            low_ref[row, at, lanes] = low

    def put_pair(b, p, row, i, pair):
        for n in range(2):
            pair_ref[b, row, n, p, rows_of(i), :] = pair[n]

    def away_step(row, i):
        waves = Waves(me, row, i)
        for p in range(2):
            values = [coeffs_ref[p, c, 1 - side, row, rows_of(i), :] for c in range(3)]
            put_pair(1 - side, p, row, i, waves.reduce(waves.cross(values)))

    def home_step(row, i):
        waves = Waves(me, row, i)
        for p in range(2):
            values = [coeffs_ref[p, c, side, row, rows_of(i), :] for c in range(3)]
            curls = waves.cross(values)
            put_halves(curls, p, row, i)
            put_pair(side, p, row, i, waves.reduce(curls))

    def direct_step(row, i):
        waves = Waves(me, row, i)
        for p in range(2):
            values = [coeffs_ref[p, c, 1 - side, row, rows_of(i), :] for c in range(3)]
            put_halves(waves.cross(values), p, row, i)

    def guest_step(row, i):
        waves = Waves(partner, row, i)
        ratios = waves.ratios()
        for p in range(2):
            pair = [swap_ref[row, n, p, rows_of(i), :] for n in range(2)]
            put_halves(waves.rebuild(ratios, *pair), p, row, i)

    def plain_table():
        return table_ref[0], table_ref[1]

    def turned_table():
        return table_ref[2], table_ref[3]

    def gather_blocks(values):
        top, bottom = values[:height], values[height:]
        return jnp.concatenate(
            [
                jnp.concatenate(
                    [
                        top[:, z * breadth : (z + 1) * breadth],
                        bottom[:, z * breadth : (z + 1) * breadth],
                    ],
                    axis=1,
                )
                for z in range(3)
            ],
            axis=0,
        )

    def spread_blocks(values):
        return jnp.concatenate(
            [
                jnp.concatenate(
                    [
                        values[z * height : (z + 1) * height, p * breadth : (p + 1) * breadth]
                        for z in range(3)
                    ],
                    axis=1,
                )
                for p in range(2)
            ],
            axis=0,
        )

    def to_peer(out, into, send, recv, s, row, k, peer, from_at, to_at):
        return pltpu.make_async_remote_copy(
            src_ref=out.at[from_at, row, peer],
            dst_ref=into.at[to_at, row, seat],
            send_sem=send.at[s, row, k],
            recv_sem=recv.at[s, row, k],
            device_id={"gz": side * members + peer},
            device_id_type=MESH,
        )

    def from_peer(out, into, send, recv, s, row, k, source, from_at, to_at):
        return pltpu.make_async_remote_copy(
            src_ref=out.at[from_at, row, source],
            dst_ref=into.at[to_at, row, source],
            send_sem=send.at[s, row, k],
            recv_sem=recv.at[s, row, k],
            device_id={"gz": side * members + source},
            device_id_type=MESH,
        )

    def ends1(s):
        return s, (side + s) % 2

    def ends2(s):
        return (side + s) % 2, s

    def start_all(out, into, send, recv, s, row, ends):
        each_member(
            lambda k, peer, source: to_peer(
                out, into, send, recv, s, row, k, peer, *ends
            ).start()
        )
        into[ends[1], row, seat] = out[ends[0], row, seat]

    def is_inner(peer):
        return peer // pack == 1 - side

    def each_inner(body):
        def one(k, peer, source):
            pl.when(is_inner(peer))(lambda: body(k, peer))

        each_member(one)

    def each_second_source(body):
        def one(k, peer, source):
            has_guest = jnp.logical_or(is_inner(source), source % 2 == 1)
            pl.when(has_guest)(lambda: body(k, source))

        each_member(one)

    def across(peer):
        return {"gz": (1 - side) * members + peer}

    def direct_copy(peer):
        return pltpu.make_async_remote_copy(
            src_ref=out3_ref.at[peer],
            dst_ref=in1_ref.at[side, 1, seat],
            send_sem=send3.at[peer],
            recv_sem=recv3.at[seat % pack // 2],
            device_id=across(peer),
            device_id_type=MESH,
        )

    def direct_arrival(n):
        source = side * pack + 2 * n
        return pltpu.make_async_remote_copy(
            src_ref=out3_ref.at[source],
            dst_ref=in1_ref.at[1 - side, 1, source],
            send_sem=send3.at[source],
            recv_sem=recv3.at[n],
            device_id=across(source),
            device_id_type=MESH,
        )

    def direct_result(n):
        peer = side * pack + n
        return pltpu.make_async_remote_copy(
            src_ref=out2_ref.at[1 - side, 1, peer],
            dst_ref=in3_ref.at[seat],
            send_sem=send4.at[n],
            recv_sem=recv4.at[seat],
            device_id=across(peer),
            device_id_type=MESH,
        )

    def result_arrival(source):
        return pltpu.make_async_remote_copy(
            src_ref=out2_ref.at[1 - side, 1, source],
            dst_ref=in3_ref.at[source],
            send_sem=send4.at[source % pack],
            recv_sem=recv4.at[source],
            device_id=across(source),
            device_id_type=MESH,
        )

    def each_of(count, body):
        def step(n, carry):
            body(n)
            return carry

        lax.fori_loop(0, count, step, 0)

    def finish_all(out, into, send, recv, s, row, ends):
        each_member(
            lambda k, peer, source: from_peer(
                out, into, send, recv, s, row, k, source, *ends
            ).wait_recv()
        )

    def drain_all(out, into, send, recv, s, row, ends):
        each_member(
            lambda k, peer, source: to_peer(
                out, into, send, recv, s, row, k, peer, *ends
            ).wait_send()
        )

    first = (out1_ref, in1_ref, send1, recv1)
    second = (out2_ref, in2_ref, send2, recv2)

    def planes_into(put, row):
        tall = product(turned_table(), (high_ref[row], low_ref[row]))
        wide = product(halves(gather_blocks(tall)), plain_table())
        for p in range(2):
            for c in range(3):
                plane = wide[c * height : (c + 1) * height, p * breadth : (p + 1) * breadth]
                put(c, p, plane.reshape(members, columns, breadth))

    def make_planes(s, row):
        def put(c, p, block):
            out1_ref[s, row, :, c, p] = block

        planes_into(put, row)

    def swap_copy(row):
        return pltpu.make_async_remote_copy(
            src_ref=pair_ref.at[1 - side, row],
            dst_ref=swap_ref.at[row],
            send_sem=swap_send.at[row],
            recv_sem=swap_recv.at[row],
            device_id={"gz": partner},
            device_id_type=MESH,
        )

    def return_copy(row):
        return pltpu.make_async_remote_copy(
            src_ref=result_ref.at[row],
            dst_ref=return_ref.at[row],
            send_sem=return_send.at[row],
            recv_sem=return_recv.at[row],
            device_id={"gz": partner},
            device_id_type=MESH,
        )

    def other_copy(b, n):
        return pltpu.make_async_remote_copy(
            src_ref=pair_ref.at[b],
            dst_ref=other_ref.at[b],
            send_sem=other_send.at[n],
            recv_sem=other_recv.at[n],
            device_id=mate,
            device_id_type=MESH,
        )

    def columns_of(peer):
        return pl.ds(pl.multiple_of((peer % members) * columns, columns), columns)

    def slab_copy(peer, slot, k):
        return pltpu.make_async_remote_copy(
            src_ref=material_ref.at[mine, columns_of(peer), :],
            dst_ref=slab_ref.at[mine, slot],
            send_sem=slab_send.at[k],
            recv_sem=slab_recv.at[k],
            device_id={"gz": peer},
            device_id_type=MESH,
        )

    def half_copy(row, part):
        at = pl.ds(pl.multiple_of(part * members, members), members)
        return pltpu.make_async_remote_copy(
            src_ref=slab_ref.at[row, at],
            dst_ref=slab_ref.at[row, at],
            send_sem=half_sem.at[0, part],
            recv_sem=half_sem.at[1, part],
            device_id=mate,
            device_id_type=MESH,
        )

    def away_row(row):
        row_load(1 - side, row, 0).wait()
        each_step(row, away_step)

    def home_row(row):
        row_load(side, row, 1).wait()
        each_step(row, home_step)
        make_planes(0, row)
        start_all(*first, 0, row, ends1(0))

    def start_slabs(base):
        def step(k, carry):
            peer = base * members + (seat + k) % members
            slab_copy(peer, me, (peer + groups - me) % groups).start()
            return carry

        return step

    def wait_slabs(base):
        def step(k, carry):
            source = base * members + (seat + members - k) % members
            slab_copy(source, source, (me + groups - source) % groups).wait_recv()
            return carry

        return step

    away_row(0)
    pl.semaphore_wait(barrier, groups)
    swap_copy(0).start()
    for load in loads:
        load.wait()
    lax.fori_loop(1, members, start_slabs(side), 0)
    lax.fori_loop(0, members, start_slabs(1 - side), 0)
    away_row(1)
    pl.when(jnp.logical_not(direct))(lambda: swap_copy(1).start())
    slab_ref[mine, me] = material_ref[mine, columns_of(me), :]
    home_row(0)
    home_row(1)

    def make_direct():
        each_step(1, direct_step)

        def put(c, p, block):
            out3_ref[:, c, p] = block

        planes_into(put, 1)

    def send_direct():
        each_of(members, lambda n: direct_copy((seat + n) % members).start())

    pl.when(direct)(make_direct)
    other_copy(side, 1).start()
    acc_ref[...] = jnp.zeros(acc_ref.shape, single)

    def guest_row(row):
        swap_copy(row).wait_recv()
        each_step(row, guest_step)
        make_planes(1, row)
        start_all(*first, 1, row, ends1(1))

    guest_row(0)
    lax.fori_loop(1, members, wait_slabs(side), 0)
    half_copy(mine, side).start()
    pl.when(inner)(lambda: guest_row(1))
    lax.fori_loop(0, members, wait_slabs(1 - side), 0)
    half_copy(mine, 1 - side).start()
    pl.when(direct)(send_direct)
    pl.when(jnp.logical_and(outer, odd))(lambda: guest_row(1))
    half_copy(1 - mine, side).wait_recv()
    half_copy(1 - mine, 1 - side).wait_recv()
    kinds = diag_ref.shape[0]

    def tensor_step(owner, carry):
        for row in range(depth):
            codes = slab_ref[row, owner]
            for entry in range(6):
                table = diag_ref if entry < 3 else off_ref
                values = jnp.full(codes.shape, table[0, entry % 3], single)
                for kind in range(1, kinds):
                    values = jnp.where(codes == kind, table[kind, entry % 3], values)
                tensor_ref[entry, owner, row] = values
        return carry

    lax.fori_loop(0, groups, tensor_step, 0)

    def part_of(n):
        return pl.ds(pl.multiple_of(n * 8, 8), 8)

    each_row(lambda row: finish_all(*first, 0, row, ends1(0)))
    finish_all(*first, 1, 0, ends1(1))
    each_second_source(lambda k, source: from_peer(*first, 1, 1, k, source, *ends1(1)).wait_recv())
    each_of(pack // 2, lambda n: direct_arrival(n).wait_recv())

    def inverse(at, c):
        points = []
        for r in range(total):
            owner, row = r // depth, r % depth
            where = (owner // members, row, owner % members, c)
            points.append((in1_ref[(*where, 0, at)], in1_ref[(*where, 1, at)]))
        for z, (real, imag) in enumerate(to_voxels(points)):
            field_ref[c, 0, z, at] = real
            field_ref[c, 1, z, at] = imag

    def scale(at, z):
        entries = [tensor_ref[entry, z // depth, z % depth, at] for entry in range(6)]
        xx, yy, zz, xy, yz, zx = entries
        for p in range(2):
            fx, fy, fz = [field_ref[c, p, z, at] for c in range(3)]
            scaled_ref[0, p, z, at] = xx * fx + xy * fy + zx * fz
            scaled_ref[1, p, z, at] = xy * fx + yy * fy + yz * fz
            scaled_ref[2, p, z, at] = zx * fx + yz * fy + zz * fz

    def forward(at, c):
        points = [(scaled_ref[c, 0, z, at], scaled_ref[c, 1, z, at]) for z in range(total)]
        for r, (real, imag) in enumerate(to_waves(points)):
            owner, row = r // depth, r % depth
            where = (owner // members, row, owner % members, c)
            out2_ref[(*where, 0, at)] = real
            out2_ref[(*where, 1, at)] = imag

    parts = columns // 8

    def part_copy(n, k, peer, other):
        at = part_of(n)
        return pltpu.make_async_remote_copy(
            src_ref=out2_ref.at[1 - side, 0, peer, :, :, at],
            dst_ref=in2_ref.at[1, 0, other, :, :, at],
            send_sem=part_send.at[n, k],
            recv_sem=part_recv.at[n, k],
            device_id={"gz": side * members + peer},
            device_id_type=MESH,
        )

    def voxel_part(n):
        at = part_of(n)
        each_of(3, functools.partial(inverse, at))

        def scale_step(z, carry):
            scale(at, z)
            return carry

        lax.fori_loop(0, total, scale_step, 0, unroll=4)
        each_of(3, functools.partial(forward, at))
        each_member(lambda k, peer, source: part_copy(n, k, peer, seat).start())

    each_of(parts, voxel_part)
    in2_ref[1, 0, seat] = out2_ref[1 - side, 0, seat]
    each_of(pack, lambda n: direct_result((seat + n) % pack).start())
    each_inner(lambda k, peer: to_peer(*second, 1, 1, k, peer, *ends2(1)).start())

    def keep_guest():
        in2_ref[1, 1, seat] = out2_ref[1 - side, 1, seat]

    pl.when(inner)(keep_guest)

    def start_home(row):
        start_all(*second, 0, row, ends2(0))

    start_home(0)
    pl.when(inner)(lambda: start_home(1))
    other_copy(1 - side, 0).start()

    def planes_back(get, row):
        planes = jnp.concatenate(
            [
                jnp.concatenate(
                    [get(c, p).reshape(height, breadth) for p in range(2)], axis=1
                )
                for c in range(3)
            ],
            axis=0,
        )
        wide = product(halves(planes), turned_table())
        back_ref[row] = product(plain_table(), halves(spread_blocks(wide)))

    def take_planes(s, row):
        planes_back(lambda c, p: in2_ref[s, row, :, c, p], row)

    def theta_at(waves, p, row, i):
        at = pl.ds(pl.multiple_of(p * height + i * step_rows, step_rows), step_rows)
        lanes = [pl.ds(c * breadth, breadth) for c in range(3)]
        return [-v for v in waves.cross([back_ref[row, at, lanes[c]] for c in range(3)])]

    def guest_result(row, i):
        waves = Waves(partner, row, i)
        for p in range(2):
            pair = waves.reduce(theta_at(waves, p, row, i))
            for n in range(2):
                result_ref[row, n, p, rows_of(i), :] = pair[n]

    def add_sums(waves, pairs, row, i, sums):
        inverse = waves.inverse()
        (real1, real2), (imag1, imag2) = [[inverse * v for v in pair] for pair in pairs]
        sums = list(sums)
        n = 0
        for source in (pair_ref, other_ref):
            for a in range(bands):
                one_real, one_imag = [source[a, row, 0, p, rows_of(i), :] for p in range(2)]
                two_real, two_imag = [source[a, row, 1, p, rows_of(i), :] for p in range(2)]
                real = (two_real * real1 + two_imag * imag1) - (one_real * real2 + one_imag * imag2)
                imag = (two_real * imag1 - two_imag * real1) - (one_real * imag2 - one_imag * real2)
                sums[n] = sums[n] + real
                sums[n + 1] = sums[n + 1] + imag
                n += 2
        return tuple(sums)

    def each_sum(row, b, body):
        def step(i, sums):
            return body(row, i, sums)

        sums = lax.fori_loop(0, steps, step, tuple(acc_ref[b, n] for n in range(4 * bands)))
        for n in range(4 * bands):
            acc_ref[b, n] = sums[n]

    def keep_sums(b):
        sums = [acc_ref[b, n] for n in range(4 * bands)]
        lane = lax.broadcasted_iota(jnp.int32, (1, breadth), 1)
        rows = [jnp.zeros((1, breadth), single)] * 2
        n = 0
        for source in (mine, 1 - mine):
            for a in range(bands):
                for p in range(2):
                    value = jnp.sum(jnp.sum(sums[n], axis=0, keepdims=True), axis=1, keepdims=True)
                    rows[p] = rows[p] + jnp.where(lane == source * bands + a, value, 0.0)
                    n += 1
        sums_ref[me, b] = jnp.concatenate(rows, axis=0) * (1.0 / (breadth * height * total))

    def result_of(b):
        def result(row, i, sums):
            waves = Waves(me, row, i)
            pairs = []
            for p in range(2):
                theta = theta_at(waves, p, row, i)
                for c in range(3):
                    theta_ref[p, c, b, row, rows_of(i), :] = theta[c]
                pairs.append(waves.reduce(theta))
            return add_sums(waves, pairs, row, i, sums)

        return result

    def away_result(row, i, sums):
        waves = Waves(me, row, i)
        ratios = waves.ratios()
        pairs = []
        for p in range(2):
            pair = [return_ref[row, n, p, rows_of(i), :] for n in range(2)]
            theta = waves.rebuild(ratios, *pair)
            for c in range(3):
                theta_ref[p, c, 1 - side, row, rows_of(i), :] = theta[c]
            pairs.append(pair)
        return add_sums(waves, pairs, row, i, sums)

    def sums_copy(slot, peer, k):
        return pltpu.make_async_remote_copy(
            src_ref=sums_ref.at[slot],
            dst_ref=sums_ref.at[slot],
            send_sem=sums_send.at[k],
            recv_sem=sums_recv.at[k],
            device_id={"gz": peer},
            device_id_type=MESH,
        )

    def guest_back(row):
        take_planes(1, row)
        each_step(row, guest_result)
        return_copy(row).start()

    def finish_parts(n):
        each_member(lambda k, peer, source: part_copy(n, k, source, source).wait_recv())

    def second_back():
        finish_all(*second, 1, 1, ends2(1))
        guest_back(1)

    each_of(parts, finish_parts)
    guest_back(0)
    pl.when(outer)(lambda: start_home(1))
    pl.when(inner)(second_back)
    other_copy(side, 1).wait_recv()
    other_copy(1 - side, 0).wait_recv()

    def take_direct():
        each_of(members, lambda n: result_arrival(n).wait_recv())
        planes_back(lambda c, p: in3_ref[:, c, p], 1)
        each_sum(1, 1 - side, result_of(1 - side))

    pl.when(inner)(take_direct)

    def home_back(row):
        finish_all(*second, 0, row, ends2(0))
        take_planes(0, row)
        each_sum(row, side, result_of(side))

    home_back(0)
    home_back(1)
    keep_sums(side)

    def away_back(row):
        return_copy(row).wait_recv()
        each_sum(row, 1 - side, away_result)

    away_back(0)
    pl.when(outer)(lambda: away_back(1))
    keep_sums(1 - side)
    each_peer(lambda k, peer, source: sums_copy(me, peer, k).start())
    half_copy(mine, side).wait_send()
    half_copy(mine, 1 - side).wait_send()
    each_peer(lambda k, peer, source: slab_copy(peer, me, k).wait_send())
    other_copy(1 - side, 0).wait_send()
    other_copy(side, 1).wait_send()
    swap_copy(0).wait_send()
    return_copy(0).wait_send()
    pl.when(jnp.logical_not(direct))(lambda: swap_copy(1).wait_send())

    pl.when(direct)(lambda: each_of(members, lambda n: direct_copy(n).wait_send()))
    pl.when(second_guest)(lambda: drain_all(*first, 1, 1, ends1(1)))
    pl.when(inner)(lambda: return_copy(1).wait_send())
    each_inner(lambda k, peer: to_peer(*second, 1, 1, k, peer, *ends2(1)).wait_send())
    each_of(pack, lambda n: direct_result(n).wait_send())
    drain_all(*first, 1, 0, ends1(1))

    def drain_parts(n):
        each_member(lambda k, peer, source: part_copy(n, k, peer, seat).wait_send())

    each_of(parts, drain_parts)
    each_row(lambda row: drain_all(*first, 0, row, ends1(0)))
    each_row(lambda row: drain_all(*second, 0, row, ends2(0)))
    each_peer(lambda k, peer, source: sums_copy(source, source, k).wait_recv())
    grams = jnp.sum(sums_ref[...], axis=0)
    for p in range(2):
        for b in range(bands):
            gram_ref[p, b : b + 1, :] = grams[b, p : p + 1, : 2 * bands]
    each_peer(lambda k, peer, source: sums_copy(me, peer, k).wait_send())


def deliver_kernel(theta_ref, gram_ref, theta_out, gram_out, theta_sem, gram_sem):
    copies = [pltpu.make_async_copy(gram_ref, gram_out, gram_sem)]
    for p in range(2):
        for c in range(3):
            copies.append(
                pltpu.make_async_copy(theta_ref.at[p, c], theta_out.at[p, c], theta_sem.at[p, c])
            )
    for copy in copies:
        copy.start()
    for copy in copies:
        copy.wait()


def on_device_kernel(coeffs, material, inv_diag, inv_off):
    groups = lax.axis_size("gz")
    _, comps, bands, depth, height, breadth = coeffs.shape
    total = depth * groups
    members = groups // 2
    columns = height // members
    table = jnp.asarray(split_table(breadth, total**-0.25))
    voxels = (3, 2, total, columns, breadth)
    block = (2, depth, members, 3, 2, columns, breadth)
    pairs = (depth, 2, 2, height, breadth)
    vmem = pl.BlockSpec(memory_space=pltpu.VMEM)
    hbm = pl.BlockSpec(memory_space=pltpu.HBM)
    dma = pltpu.SemaphoreType.DMA
    operands = [
        pltpu.with_memory_space_constraint(v, pltpu.HBM)
        for v in (coeffs, material, inv_diag, inv_off, table)
    ]
    theta, gram = pl.pallas_call(
        functools.partial(operator_kernel, groups),
        out_shape=(
            jax.ShapeDtypeStruct(coeffs.shape, single),
            jax.ShapeDtypeStruct((2, bands, 2 * bands), single),
        ),
        in_specs=[hbm, hbm, hbm, hbm, hbm],
        out_specs=(vmem, vmem),
        scratch_shapes=[
            pltpu.VMEM(coeffs.shape, single),
            pltpu.VMEM(material.shape, jnp.int32),
            pltpu.VMEM(table.shape, half),
            pltpu.SMEM(inv_diag.shape, single),
            pltpu.SMEM(inv_off.shape, single),
            pltpu.VMEM((depth, groups, columns, breadth), jnp.int32),
            pltpu.VMEM((6, groups, depth, columns, breadth), single),
            pltpu.VMEM((depth, 2 * height, 3 * breadth), half),
            pltpu.VMEM((depth, 2 * height, 3 * breadth), half),
            pltpu.VMEM((depth, 2 * height, 3 * breadth), single),
            pltpu.VMEM((bands, *pairs), single),
            pltpu.VMEM((bands, *pairs), single),
            pltpu.VMEM(pairs, single),
            pltpu.VMEM(pairs, single),
            pltpu.VMEM(pairs, single),
            pltpu.VMEM(block, single),
            pltpu.VMEM(block, single),
            pltpu.VMEM(voxels, single),
            pltpu.VMEM(voxels, single),
            pltpu.VMEM(block, single),
            pltpu.VMEM(block, single),
            pltpu.VMEM(block[2:], single),
            pltpu.VMEM(block[2:], single),
            pltpu.VMEM((bands, 4 * bands, 16, breadth), single),
            pltpu.VMEM((groups, bands, 2, breadth), single),
            dma((4, depth)),
            dma((groups,)),
            dma((groups,)),
            dma((2, 2)),
            dma((2, depth, members)),
            dma((2, depth, members)),
            dma((2, depth, members)),
            dma((2, depth, members)),
            dma((members,)),
            dma((members // 4,)),
            dma((members // 2,)),
            dma((members,)),
            dma((columns // 8, members)),
            dma((columns // 8, members)),
            dma((depth,)),
            dma((depth,)),
            dma((depth,)),
            dma((depth,)),
            dma((2,)),
            dma((2,)),
            dma((groups,)),
            dma((groups,)),
        ],
        compiler_params=pltpu.CompilerParams(
            collective_id=0, has_side_effects=True, vmem_limit_bytes=48 * 1024 * 1024
        ),
        name="maxwell",
    )(*operands)
    theta, gram = pl.pallas_call(
        deliver_kernel,
        out_shape=(
            jax.ShapeDtypeStruct(theta.shape, single),
            jax.ShapeDtypeStruct(gram.shape, single),
        ),
        in_specs=[vmem, vmem],
        out_specs=(hbm, hbm),
        scratch_shapes=[dma((2, 3)), dma(())],
        compiler_params=pltpu.CompilerParams(vmem_limit_bytes=8 * 1024 * 1024),
        name="deliver",
    )(theta, gram)
    return (theta, gram.transpose(0, 2, 1))


def fits(coeffs):
    groups = lax.axis_size("gz")
    _, _, bands, depth, height, breadth = coeffs.shape
    return (
        lax.axis_size("ba") == 2
        and bands == 2
        and depth == 2
        and groups >= 8
        and height % (4 * groups) == 0
        and height % 16 == 0
        and height == breadth
        and breadth % 128 == 0
    )


def on_either(coeffs, material, inv_diag, inv_off):
    chosen = on_device_kernel if fits(coeffs) else on_device
    return chosen(coeffs, material, inv_diag, inv_off)


def solution(mesh):
    in_specs = (P(None, None, "ba", "gz", None, None), P("gz", None, None), P(), P())
    out_specs = (P(None, None, "ba", "gz", None, None), P(None, None, "ba"))
    return jax.shard_map(
        on_either, mesh=mesh, in_specs=in_specs, out_specs=out_specs, check_vma=False
    )
```

```python
import functools
import math

import jax
import jax.numpy as jnp
import numpy as np
from jax import lax
from jax.experimental import pallas as pl
from jax.experimental.pallas import tpu as pltpu
from jax.sharding import PartitionSpec as P

highest = lax.Precision.HIGHEST
half_turn = 3.141592653589793


def reverse_bits(values, levels):
    flipped = jnp.zeros_like(values)
    for position in range(levels):
        flipped = flipped + (values >> position & 1) * (1 << levels - 1 - position)
    return flipped


def signed_wave(numbers, length):
    shifted = jnp.where(numbers < length // 2, numbers, numbers - length)
    return shifted.astype(jnp.float32) / (length / 2.0)


def phase_tables(first, second, length, sign):
    product = first[:, None] * second[None, :] % length
    angle = 2.0 * half_turn / length * product.astype(jnp.float32)
    factor = 1.0 / math.sqrt(length)
    return (jnp.cos(angle) * factor, sign * jnp.sin(angle) * factor)


def cross_waves(waves, field):
    first, second, third = waves
    return jnp.stack(
        [
            second * field[:, 2] - third * field[:, 1],
            third * field[:, 0] - first * field[:, 2],
            first * field[:, 1] - second * field[:, 0],
        ],
        axis=1,
    )


def along_width(field, cosine, sine):
    breadth = field.shape[-1]
    rows = field.reshape(2, -1, breadth)
    joined = jnp.concatenate([cosine, sine], axis=1)
    real_prod = jnp.dot(rows[0], joined, precision=highest)
    imag_prod = jnp.dot(rows[1], joined, precision=highest)
    real_out = real_prod[:, :breadth] - imag_prod[:, breadth:]
    imag_out = real_prod[:, breadth:] + imag_prod[:, :breadth]
    return jnp.stack([real_out, imag_out]).reshape(field.shape)


def along_height(field, cosine, sine):
    tables = jnp.stack([cosine, sine])
    product = jnp.einsum("pcbzyx,tyk->tpcbzkx", field, tables, precision=highest)
    return jnp.stack([product[0, 0] - product[1, 1], product[1, 0] + product[0, 1]])


def along_depth(field, cosine, sine):
    tables = jnp.stack([cosine, sine])
    product = jnp.einsum("pcbzyx,tzk->tpcbkyx", field, tables, precision=highest)
    return jnp.stack([product[0, 0] - product[1, 1], product[1, 0] + product[0, 1]])


def apply_material(field, material, inv_diag, inv_off):
    materials = inv_diag.shape[0]
    onehot = (material[None] == jnp.arange(materials, dtype=jnp.int32)[:, None, None, None]).astype(
        jnp.float32
    )
    table = jnp.concatenate([inv_diag, inv_off], axis=1)
    tensor = jnp.einsum("mk,mzyx->kzyx", table, onehot, precision=highest)
    first = field[:, 0]
    second = field[:, 1]
    third = field[:, 2]
    return jnp.stack(
        [
            tensor[0] * first + tensor[3] * second + tensor[5] * third,
            tensor[3] * first + tensor[1] * second + tensor[4] * third,
            tensor[5] * first + tensor[4] * second + tensor[2] * third,
        ],
        axis=1,
    )


def on_device(coeffs, material, inv_diag, inv_off):
    groups = lax.axis_size("gz")
    levels = groups.bit_length() - 1
    depth = coeffs.shape[3]
    height = coeffs.shape[4]
    breadth = coeffs.shape[5]
    total_depth = depth * groups
    device = lax.axis_index("gz")
    local_rows = jnp.arange(depth, dtype=jnp.int32)
    waves_here = reverse_bits(device, levels) + groups * local_rows
    across = jnp.arange(breadth, dtype=jnp.int32)
    upward = jnp.arange(height, dtype=jnp.int32)
    waves = (
        signed_wave(across, breadth)[None, None, :],
        signed_wave(upward, height)[None, :, None],
        signed_wave(waves_here, total_depth)[:, None, None],
    )
    curl = cross_waves(waves, coeffs)
    all_rows = jnp.arange(total_depth, dtype=jnp.int32)
    wave_rows = reverse_bits(all_rows // depth, levels) + groups * (all_rows % depth)
    height_cos, height_sin = phase_tables(upward, upward, height, 1.0)
    width_cos, width_sin = phase_tables(across, across, breadth, 1.0)
    planar = along_height(curl, height_cos, height_sin)
    planar = along_width(planar, width_cos, width_sin)
    material_slab = lax.all_to_all(material, "gz", split_axis=1, concat_axis=0, tiled=True)
    inverse_cos, inverse_sin = phase_tables(wave_rows, all_rows, total_depth, 1.0)
    forward_cos, forward_sin = phase_tables(all_rows, wave_rows, total_depth, -1.0)
    spatial_piece = along_depth(
        lax.all_to_all(planar, "gz", split_axis=4, concat_axis=3, tiled=True),
        inverse_cos,
        inverse_sin,
    )
    scaled_piece = apply_material(spatial_piece, material_slab, inv_diag, inv_off)
    returned = along_depth(scaled_piece, forward_cos, forward_sin)
    spectral = lax.all_to_all(returned, "gz", split_axis=3, concat_axis=4, tiled=True)
    spectral = along_width(spectral, width_cos, -width_sin)
    spectral = along_height(spectral, height_cos, -height_sin)
    theta = -cross_waves(waves, spectral)
    factor = 1.0 / (breadth * height * total_depth)
    piece = lax.all_gather(coeffs, "ba", axis=2, tiled=True)
    real_part = jnp.einsum("cbzyx,cezyx->be", piece[0], theta[0], precision=highest) + jnp.einsum(
        "cbzyx,cezyx->be", piece[1], theta[1], precision=highest
    )
    imag_part = jnp.einsum("cbzyx,cezyx->be", piece[0], theta[1], precision=highest) - jnp.einsum(
        "cbzyx,cezyx->be", piece[1], theta[0], precision=highest
    )
    block = jnp.stack([real_part, imag_part]) * factor
    gram = lax.psum(block, "gz")
    return (theta, gram)


MESH = pl.DeviceIdType.MESH
single = jnp.float32
half = jnp.bfloat16


def split_table(length, extra):
    numbers = np.arange(length)
    angle = 2.0 * np.pi / length * (numbers[:, None] * numbers[None, :] % length)
    cosine = np.cos(angle) * extra / math.sqrt(length)
    sine = np.sin(angle) * extra / math.sqrt(length)
    inverse = np.block([[cosine, sine], [-sine, cosine]])
    parts = []
    for table in (inverse, inverse.T):
        high = table.astype(np.float32).astype(half)
        low = (table - high.astype(np.float64)).astype(half)
        parts += [high, low]
    return np.stack(parts)


def halves(values):
    high = values.astype(half)
    return high, (values - high.astype(single)).astype(half)


def product(first, second):
    dot = functools.partial(jnp.dot, preferred_element_type=single)
    return dot(first[0], second[0]) + (dot(first[0], second[1]) + dot(first[1], second[0]))


def twiddled(pair, step, span, sign):
    real, imag = pair
    if step == 0:
        return real, imag
    if 2 * step == span:
        return (-imag, real) if sign > 0 else (imag, -real)
    angle = math.pi * step / span
    cosine, sine = math.cos(angle), sign * math.sin(angle)
    return real * cosine - imag * sine, real * sine + imag * cosine


def to_voxels(points):
    points = list(points)
    span = 1
    while span < len(points):
        for base in range(0, len(points), 2 * span):
            for step in range(span):
                a = points[base + step]
                t = twiddled(points[base + step + span], step, span, 1.0)
                points[base + step] = (a[0] + t[0], a[1] + t[1])
                points[base + step + span] = (a[0] - t[0], a[1] - t[1])
        span *= 2
    return points


def to_waves(points):
    points = list(points)
    span = len(points) // 2
    while span >= 1:
        for base in range(0, len(points), 2 * span):
            for step in range(span):
                a, t = points[base + step], points[base + step + span]
                points[base + step] = (a[0] + t[0], a[1] + t[1])
                points[base + step + span] = twiddled(
                    (a[0] - t[0], a[1] - t[1]), step, span, -1.0
                )
        span //= 2
    return points


def operator_kernel(
    groups,
    coeffs_hbm,
    material_hbm,
    diag_hbm,
    off_hbm,
    table_hbm,
    theta_ref,
    gram_ref,
    coeffs_ref,
    material_ref,
    table_ref,
    diag_ref,
    off_ref,
    slab_ref,
    tensor_ref,
    high_ref,
    low_ref,
    back_ref,
    pair_ref,
    other_ref,
    swap_ref,
    result_ref,
    return_ref,
    out1_ref,
    in1_ref,
    field_ref,
    scaled_ref,
    out2_ref,
    in2_ref,
    out3_ref,
    in3_ref,
    acc_ref,
    sums_ref,
    load_sem,
    slab_send,
    slab_recv,
    half_sem,
    send1,
    recv1,
    send2,
    recv2,
    far_sem,
    swap_send,
    swap_recv,
    return_send,
    return_recv,
    other_send,
    other_recv,
    sums_sem,
):
    _, comps, bands, depth, height, breadth = coeffs_ref.shape
    total = depth * groups
    members = groups // 2
    columns = height // members
    levels = groups.bit_length() - 1
    me = lax.axis_index("gz")
    mine = lax.axis_index("ba")
    side = me // members
    seat = me % members
    partner = (me + members) % groups
    pack = members // 2
    inner = seat // pack == 1 - side
    outer = jnp.logical_not(inner)
    odd = seat % 2 == 1
    direct = jnp.logical_and(inner, jnp.logical_not(odd))
    second_guest = jnp.logical_or(inner, odd)
    mate = {"ba": 1 - mine}
    step_rows = 16
    steps = height // step_rows

    def each_peer(body):
        def step(k, carry):
            body((me + k) % groups)
            return carry

        lax.fori_loop(1, groups, step, 0)

    def each_member(body):
        def step(k, carry):
            body(k, (seat + k) % members)
            return carry

        lax.fori_loop(1, members, step, 0)

    barrier = pltpu.get_barrier_semaphore()
    each_peer(
        lambda peer: pl.semaphore_signal(
            barrier, inc=1, device_id={"gz": peer}, device_id_type=MESH
        )
    )
    pl.semaphore_signal(barrier, inc=1, device_id=mate, device_id_type=MESH)

    def row_load(b, row, n):
        return pltpu.make_async_copy(
            coeffs_hbm.at[:, :, b, row], coeffs_ref.at[:, :, b, row], load_sem.at[n, row]
        )

    loads = [
        pltpu.make_async_copy(table_hbm, table_ref, load_sem.at[2, 0]),
        pltpu.make_async_copy(material_hbm, material_ref, load_sem.at[2, 1]),
        pltpu.make_async_copy(diag_hbm, diag_ref, load_sem.at[3, 0]),
        pltpu.make_async_copy(off_hbm, off_ref, load_sem.at[3, 1]),
    ]
    for row in range(depth):
        row_load(1 - side, row, 0).start()
    for row in range(depth):
        row_load(side, row, 1).start()
    for load in loads:
        load.start()

    def signed(number, length):
        return number - length * (number // (length // 2))

    def row_number(owner, row):
        reversed_owner = 0
        for position in range(levels):
            bit = (owner // (1 << position)) % 2
            reversed_owner = reversed_owner + bit * (1 << (levels - 1 - position))
        return signed(reversed_owner + groups * row, total)

    def inverse_of(values):
        zero = values == 0
        return jnp.where(zero, 0.0, 1.0 / jnp.where(zero, 1, values).astype(single))

    class Waves:
        def __init__(self, owner, row, i):
            shape = (step_rows, breadth)
            nx = lax.broadcasted_iota(jnp.int32, shape, 1)
            ny = lax.broadcasted_iota(jnp.int32, shape, 0) + i * step_rows
            nx = jnp.where(nx < breadth // 2, nx, nx - breadth)
            ny = jnp.where(ny < height // 2, ny, ny - height)
            nz = jnp.full(shape, row_number(owner, row), jnp.int32)
            self.x = nx.astype(single) / (breadth / 2.0)
            self.y = ny.astype(single) / (height / 2.0)
            self.z = nz.astype(single) / (total / 2.0)
            ax, ay, az = jnp.abs(nx) * total, jnp.abs(ny) * total, jnp.abs(nz) * breadth
            self.is_x = (ax >= ay) & (ax >= az)
            self.is_y = ay >= az
            self.numbers = (nx, ny, nz)

        def cross(self, v):
            q = (self.x, self.y, self.z)
            return [
                q[(c + 1) % 3] * v[(c + 2) % 3] - q[(c + 2) % 3] * v[(c + 1) % 3]
                for c in range(3)
            ]

        def pick(self, first, second, third):
            return jnp.where(self.is_x, first, jnp.where(self.is_y, second, third))

        def inverse(self):
            nx, ny, nz = self.numbers
            scaled = self.pick(nx * total, ny * total, nz * breadth)
            return inverse_of(scaled) * (total * breadth / 2.0)

        def ratios(self):
            inverse = self.inverse()
            return (
                self.pick(self.y, self.z, self.x) * inverse,
                self.pick(self.z, self.x, self.y) * inverse,
            )

        def reduce(self, v):
            return self.pick(v[1], v[2], v[0]), self.pick(v[2], v[0], v[1])

        def rebuild(self, ratios, first, second):
            last = -(ratios[0] * first + ratios[1] * second)
            return [
                self.pick(last, second, first),
                self.pick(first, last, second),
                self.pick(second, first, last),
            ]

    def rows_of(i):
        return pl.ds(pl.multiple_of(i * step_rows, step_rows), step_rows)

    def each_step(row, body):
        def step(i, carry):
            body(row, i)
            return carry

        lax.fori_loop(0, steps, step, 0)

    def each_row(body):
        def step(row, carry):
            body(row)
            return carry

        lax.fori_loop(0, depth, step, 0)

    def put_halves(curls, p, row, i):
        at = pl.ds(pl.multiple_of(p * height + i * step_rows, step_rows), step_rows)
        for c in range(3):
            high, low = halves(curls[c])
            lanes = pl.ds(c * breadth, breadth)
            high_ref[row, at, lanes] = high
            low_ref[row, at, lanes] = low

    def put_pair(b, p, row, i, pair):
        for n in range(2):
            pair_ref[b, row, n, p, rows_of(i), :] = pair[n]

    def away_step(row, i):
        waves = Waves(me, row, i)
        for p in range(2):
            values = [coeffs_ref[p, c, 1 - side, row, rows_of(i), :] for c in range(3)]
            put_pair(1 - side, p, row, i, waves.reduce(waves.cross(values)))

    def home_step(row, i):
        waves = Waves(me, row, i)
        for p in range(2):
            values = [coeffs_ref[p, c, side, row, rows_of(i), :] for c in range(3)]
            curls = waves.cross(values)
            put_halves(curls, p, row, i)
            put_pair(side, p, row, i, waves.reduce(curls))

    def direct_step(row, i):
        waves = Waves(me, row, i)
        for p in range(2):
            values = [coeffs_ref[p, c, 1 - side, row, rows_of(i), :] for c in range(3)]
            put_halves(waves.cross(values), p, row, i)

    def guest_step(row, i):
        waves = Waves(partner, row, i)
        ratios = waves.ratios()
        for p in range(2):
            pair = [swap_ref[row, n, p, rows_of(i), :] for n in range(2)]
            put_halves(waves.rebuild(ratios, *pair), p, row, i)

    def plain_table():
        return table_ref[0], table_ref[1]

    def turned_table():
        return table_ref[2], table_ref[3]

    def gather_blocks(values):
        top, bottom = values[:height], values[height:]
        return jnp.concatenate(
            [
                jnp.concatenate(
                    [
                        top[:, z * breadth : (z + 1) * breadth],
                        bottom[:, z * breadth : (z + 1) * breadth],
                    ],
                    axis=1,
                )
                for z in range(3)
            ],
            axis=0,
        )

    def spread_blocks(values):
        return jnp.concatenate(
            [
                jnp.concatenate(
                    [
                        values[z * height : (z + 1) * height, p * breadth : (p + 1) * breadth]
                        for z in range(3)
                    ],
                    axis=1,
                )
                for p in range(2)
            ],
            axis=0,
        )

    def to_peer(out, into, send, recv, s, row, peer, from_at, to_at):
        return pltpu.make_async_remote_copy(
            src_ref=out.at[from_at, row, peer],
            dst_ref=into.at[to_at, row, seat],
            send_sem=send.at[s, row],
            recv_sem=recv.at[s, row],
            device_id={"gz": side * members + peer},
            device_id_type=MESH,
        )

    def blocks(count, out, into, send, recv, s, row, from_at, to_at):
        return pltpu.make_async_remote_copy(
            src_ref=out.at[from_at, row, pl.ds(0, count)],
            dst_ref=into.at[to_at, row, pl.ds(0, count)],
            send_sem=send.at[s, row],
            recv_sem=recv.at[s, row],
            device_id={"gz": side * members + (seat + 1) % members},
            device_id_type=MESH,
        )

    def ends1(s):
        return s, (side + s) % 2

    def ends2(s):
        return (side + s) % 2, s

    def start_all(out, into, send, recv, s, row, ends):
        each_member(lambda k, peer: to_peer(out, into, send, recv, s, row, peer, *ends).start())
        into[ends[1], row, seat] = out[ends[0], row, seat]

    def finish_all(out, into, send, recv, s, row, ends):
        blocks(members - 1, out, into, send, recv, s, row, *ends).wait_recv()

    def drain_all(out, into, send, recv, s, row, ends):
        blocks(members - 1, out, into, send, recv, s, row, *ends).wait_send()

    def is_inner(peer):
        return peer // pack == 1 - side

    def each_inner(body):
        def one(k, peer):
            pl.when(is_inner(peer))(lambda: body(k, peer))

        each_member(one)

    def across(peer):
        return {"gz": (1 - side) * members + peer}

    def direct_copy(peer):
        return pltpu.make_async_remote_copy(
            src_ref=out3_ref.at[peer],
            dst_ref=in1_ref.at[side, 1, seat],
            send_sem=far_sem.at[0],
            recv_sem=far_sem.at[1],
            device_id=across(peer),
            device_id_type=MESH,
        )

    def direct_blocks(count):
        return pltpu.make_async_remote_copy(
            src_ref=out3_ref.at[pl.ds(0, count)],
            dst_ref=in1_ref.at[1 - side, 1, pl.ds(0, count)],
            send_sem=far_sem.at[0],
            recv_sem=far_sem.at[1],
            device_id=across(seat),
            device_id_type=MESH,
        )

    def direct_result(n):
        peer = side * pack + n
        return pltpu.make_async_remote_copy(
            src_ref=out2_ref.at[1 - side, 1, peer],
            dst_ref=in3_ref.at[seat],
            send_sem=far_sem.at[2],
            recv_sem=far_sem.at[3],
            device_id=across(peer),
            device_id_type=MESH,
        )

    def result_blocks(count):
        return pltpu.make_async_remote_copy(
            src_ref=out2_ref.at[1 - side, 1, pl.ds(0, count)],
            dst_ref=in3_ref.at[pl.ds(0, count)],
            send_sem=far_sem.at[2],
            recv_sem=far_sem.at[3],
            device_id=across(seat),
            device_id_type=MESH,
        )

    def each_of(count, body):
        def step(n, carry):
            body(n)
            return carry

        lax.fori_loop(0, count, step, 0)

    first = (out1_ref, in1_ref, send1, recv1)
    second = (out2_ref, in2_ref, send2, recv2)

    def planes_into(put, row):
        tall = product(turned_table(), (high_ref[row], low_ref[row]))
        wide = product(halves(gather_blocks(tall)), plain_table())
        for p in range(2):
            for c in range(3):
                plane = wide[c * height : (c + 1) * height, p * breadth : (p + 1) * breadth]
                put(c, p, plane.reshape(members, columns, breadth))

    def make_planes(s, row):
        def put(c, p, block):
            out1_ref[s, row, :, c, p] = block

        planes_into(put, row)

    def swap_copy(row):
        return pltpu.make_async_remote_copy(
            src_ref=pair_ref.at[1 - side, row],
            dst_ref=swap_ref.at[row],
            send_sem=swap_send.at[row],
            recv_sem=swap_recv.at[row],
            device_id={"gz": partner},
            device_id_type=MESH,
        )

    def return_copy(row):
        return pltpu.make_async_remote_copy(
            src_ref=result_ref.at[row],
            dst_ref=return_ref.at[row],
            send_sem=return_send.at[row],
            recv_sem=return_recv.at[row],
            device_id={"gz": partner},
            device_id_type=MESH,
        )

    def other_copy(b, n):
        return pltpu.make_async_remote_copy(
            src_ref=pair_ref.at[b],
            dst_ref=other_ref.at[b],
            send_sem=other_send.at[n],
            recv_sem=other_recv.at[n],
            device_id=mate,
            device_id_type=MESH,
        )

    def columns_of(peer):
        return pl.ds(pl.multiple_of((peer % members) * columns, columns), columns)

    def slab_copy(peer, n):
        return pltpu.make_async_remote_copy(
            src_ref=material_ref.at[mine, columns_of(peer), :],
            dst_ref=slab_ref.at[mine, me],
            send_sem=slab_send.at[n],
            recv_sem=slab_recv.at[n],
            device_id={"gz": peer},
            device_id_type=MESH,
        )

    def slab_blocks(n):
        slots = slab_ref.at[mine, pl.ds(0, members - 1 + n)]
        return pltpu.make_async_remote_copy(
            src_ref=slots,
            dst_ref=slots,
            send_sem=slab_send.at[n],
            recv_sem=slab_recv.at[n],
            device_id={"gz": partner},
            device_id_type=MESH,
        )

    def half_copy(row, part):
        at = pl.ds(pl.multiple_of(part * members, members), members)
        return pltpu.make_async_remote_copy(
            src_ref=slab_ref.at[row, at],
            dst_ref=slab_ref.at[row, at],
            send_sem=half_sem.at[0, part],
            recv_sem=half_sem.at[1, part],
            device_id=mate,
            device_id_type=MESH,
        )

    def away_row(row):
        row_load(1 - side, row, 0).wait()
        each_step(row, away_step)

    def home_row(row):
        row_load(side, row, 1).wait()
        each_step(row, home_step)
        make_planes(0, row)
        start_all(*first, 0, row, ends1(0))

    def start_slab(base, n):
        def step(k, carry):
            slab_copy(base * members + (seat + k) % members, n).start()
            return carry

        lax.fori_loop(1 - n, members, step, 0)

    away_row(0)
    pl.semaphore_wait(barrier, groups)
    swap_copy(0).start()
    for load in loads:
        load.wait()
    start_slab(side, 0)
    start_slab(1 - side, 1)
    away_row(1)
    pl.when(jnp.logical_not(direct))(lambda: swap_copy(1).start())
    slab_ref[mine, me] = material_ref[mine, columns_of(me), :]
    home_row(0)
    home_row(1)

    def make_direct():
        each_step(1, direct_step)

        def put(c, p, block):
            out3_ref[:, c, p] = block

        planes_into(put, 1)

    def send_direct():
        each_of(members, lambda n: direct_copy((seat + n) % members).start())

    pl.when(direct)(make_direct)
    other_copy(side, 1).start()
    acc_ref[...] = jnp.zeros(acc_ref.shape, single)

    def guest_row(row):
        swap_copy(row).wait_recv()
        each_step(row, guest_step)
        make_planes(1, row)
        start_all(*first, 1, row, ends1(1))

    guest_row(0)
    slab_blocks(0).wait_recv()
    half_copy(mine, side).start()
    pl.when(inner)(lambda: guest_row(1))
    slab_blocks(1).wait_recv()
    half_copy(mine, 1 - side).start()
    pl.when(direct)(send_direct)
    pl.when(jnp.logical_and(outer, odd))(lambda: guest_row(1))
    half_copy(1 - mine, side).wait_recv()
    half_copy(1 - mine, 1 - side).wait_recv()
    kinds = diag_ref.shape[0]

    def tensor_step(owner, carry):
        for row in range(depth):
            codes = slab_ref[row, owner]
            for entry in range(6):
                table = diag_ref if entry < 3 else off_ref
                values = jnp.full(codes.shape, table[0, entry % 3], single)
                for kind in range(1, kinds):
                    values = jnp.where(codes == kind, table[kind, entry % 3], values)
                tensor_ref[entry, owner, row] = values
        return carry

    lax.fori_loop(0, groups, tensor_step, 0)

    def part_of(n):
        return pl.ds(pl.multiple_of(n * 8, 8), 8)

    each_row(lambda row: finish_all(*first, 0, row, ends1(0)))
    finish_all(*first, 1, 0, ends1(1))

    def finish_second(count):
        blocks(count, *first, 1, 1, *ends1(1)).wait_recv()

    guests = pack + pack // 2
    pl.when(second_guest)(lambda: finish_second(guests - 1))
    pl.when(jnp.logical_not(second_guest))(lambda: finish_second(guests))
    direct_blocks(pack // 2).wait_recv()

    def inverse(at, c):
        points = []
        for r in range(total):
            owner, row = r // depth, r % depth
            where = (owner // members, row, owner % members, c)
            points.append((in1_ref[(*where, 0, at)], in1_ref[(*where, 1, at)]))
        for z, (real, imag) in enumerate(to_voxels(points)):
            field_ref[c, 0, z, at] = real
            field_ref[c, 1, z, at] = imag

    def scale(at, z):
        entries = [tensor_ref[entry, z // depth, z % depth, at] for entry in range(6)]
        xx, yy, zz, xy, yz, zx = entries
        for p in range(2):
            fx, fy, fz = [field_ref[c, p, z, at] for c in range(3)]
            scaled_ref[0, p, z, at] = xx * fx + xy * fy + zx * fz
            scaled_ref[1, p, z, at] = xy * fx + yy * fy + yz * fz
            scaled_ref[2, p, z, at] = zx * fx + yz * fy + zz * fz

    def forward(at, c):
        points = [(scaled_ref[c, 0, z, at], scaled_ref[c, 1, z, at]) for z in range(total)]
        for r, (real, imag) in enumerate(to_waves(points)):
            owner, row = r // depth, r % depth
            where = (owner // members, row, owner % members, c)
            out2_ref[(*where, 0, at)] = real
            out2_ref[(*where, 1, at)] = imag

    parts = columns // 8

    def part_copy(n, peer):
        at = part_of(n)
        return pltpu.make_async_remote_copy(
            src_ref=out2_ref.at[1 - side, 0, peer, :, :, at],
            dst_ref=in2_ref.at[1, 0, seat, :, :, at],
            send_sem=send2.at[1, 0],
            recv_sem=recv2.at[1, 0],
            device_id={"gz": side * members + peer},
            device_id_type=MESH,
        )

    def voxel_part(n):
        at = part_of(n)
        each_of(3, functools.partial(inverse, at))

        def scale_step(z, carry):
            scale(at, z)
            return carry

        lax.fori_loop(0, total, scale_step, 0, unroll=4)
        each_of(3, functools.partial(forward, at))
        each_member(lambda k, peer: part_copy(n, peer).start())

    each_of(parts, voxel_part)
    in2_ref[1, 0, seat] = out2_ref[1 - side, 0, seat]
    each_of(pack, lambda n: direct_result((seat + n) % pack).start())
    each_inner(lambda k, peer: to_peer(*second, 1, 1, peer, *ends2(1)).start())

    def keep_guest():
        in2_ref[1, 1, seat] = out2_ref[1 - side, 1, seat]

    pl.when(inner)(keep_guest)

    def start_home(row):
        start_all(*second, 0, row, ends2(0))

    start_home(0)
    pl.when(inner)(lambda: start_home(1))
    other_copy(1 - side, 0).start()

    def planes_back(get, row):
        planes = jnp.concatenate(
            [
                jnp.concatenate(
                    [get(c, p).reshape(height, breadth) for p in range(2)], axis=1
                )
                for c in range(3)
            ],
            axis=0,
        )
        wide = product(halves(planes), turned_table())
        back_ref[row] = product(plain_table(), halves(spread_blocks(wide)))

    def take_planes(s, row):
        planes_back(lambda c, p: in2_ref[s, row, :, c, p], row)

    def theta_at(waves, p, row, i):
        at = pl.ds(pl.multiple_of(p * height + i * step_rows, step_rows), step_rows)
        lanes = [pl.ds(c * breadth, breadth) for c in range(3)]
        return [-v for v in waves.cross([back_ref[row, at, lanes[c]] for c in range(3)])]

    def guest_result(row, i):
        waves = Waves(partner, row, i)
        for p in range(2):
            pair = waves.reduce(theta_at(waves, p, row, i))
            for n in range(2):
                result_ref[row, n, p, rows_of(i), :] = pair[n]

    def add_sums(waves, pairs, row, i, sums):
        inverse = waves.inverse()
        (real1, real2), (imag1, imag2) = [[inverse * v for v in pair] for pair in pairs]
        sums = list(sums)
        n = 0
        for source in (pair_ref, other_ref):
            for a in range(bands):
                one_real, one_imag = [source[a, row, 0, p, rows_of(i), :] for p in range(2)]
                two_real, two_imag = [source[a, row, 1, p, rows_of(i), :] for p in range(2)]
                real = (two_real * real1 + two_imag * imag1) - (one_real * real2 + one_imag * imag2)
                imag = (two_real * imag1 - two_imag * real1) - (one_real * imag2 - one_imag * real2)
                sums[n] = sums[n] + real
                sums[n + 1] = sums[n + 1] + imag
                n += 2
        return tuple(sums)

    def each_sum(row, b, body):
        def step(i, sums):
            return body(row, i, sums)

        sums = lax.fori_loop(0, steps, step, tuple(acc_ref[b, n] for n in range(4 * bands)))
        for n in range(4 * bands):
            acc_ref[b, n] = sums[n]

    def keep_sums(b):
        sums = [acc_ref[b, n] for n in range(4 * bands)]
        lane = lax.broadcasted_iota(jnp.int32, (1, breadth), 1)
        rows = [jnp.zeros((1, breadth), single)] * 2
        n = 0
        for source in (mine, 1 - mine):
            for a in range(bands):
                for p in range(2):
                    value = jnp.sum(jnp.sum(sums[n], axis=0, keepdims=True), axis=1, keepdims=True)
                    rows[p] = rows[p] + jnp.where(lane == source * bands + a, value, 0.0)
                    n += 1
        sums_ref[me, b] = jnp.concatenate(rows, axis=0) * (1.0 / (breadth * height * total))

    def result_of(b):
        def result(row, i, sums):
            waves = Waves(me, row, i)
            pairs = []
            for p in range(2):
                theta = theta_at(waves, p, row, i)
                for c in range(3):
                    theta_ref[p, c, b, row, rows_of(i), :] = theta[c]
                pairs.append(waves.reduce(theta))
            return add_sums(waves, pairs, row, i, sums)

        return result

    def away_result(row, i, sums):
        waves = Waves(me, row, i)
        ratios = waves.ratios()
        pairs = []
        for p in range(2):
            pair = [return_ref[row, n, p, rows_of(i), :] for n in range(2)]
            theta = waves.rebuild(ratios, *pair)
            for c in range(3):
                theta_ref[p, c, 1 - side, row, rows_of(i), :] = theta[c]
            pairs.append(pair)
        return add_sums(waves, pairs, row, i, sums)

    def sums_copy(peer):
        return pltpu.make_async_remote_copy(
            src_ref=sums_ref.at[me],
            dst_ref=sums_ref.at[me],
            send_sem=sums_sem.at[0],
            recv_sem=sums_sem.at[1],
            device_id={"gz": peer},
            device_id_type=MESH,
        )

    def sums_blocks():
        slots = sums_ref.at[pl.ds(0, groups - 1)]
        return pltpu.make_async_remote_copy(
            src_ref=slots,
            dst_ref=slots,
            send_sem=sums_sem.at[0],
            recv_sem=sums_sem.at[1],
            device_id={"gz": partner},
            device_id_type=MESH,
        )

    def guest_back(row):
        take_planes(1, row)
        each_step(row, guest_result)
        return_copy(row).start()

    def second_back():
        finish_all(*second, 1, 1, ends2(1))
        guest_back(1)

    finish_all(*second, 1, 0, ends2(1))
    guest_back(0)
    pl.when(outer)(lambda: start_home(1))
    pl.when(inner)(second_back)
    other_copy(side, 1).wait_recv()
    other_copy(1 - side, 0).wait_recv()

    def take_direct():
        result_blocks(members).wait_recv()
        planes_back(lambda c, p: in3_ref[:, c, p], 1)
        each_sum(1, 1 - side, result_of(1 - side))

    pl.when(inner)(take_direct)

    def home_back(row):
        finish_all(*second, 0, row, ends2(0))
        take_planes(0, row)
        each_sum(row, side, result_of(side))

    home_back(0)
    home_back(1)
    keep_sums(side)

    def away_back(row):
        return_copy(row).wait_recv()
        each_sum(row, 1 - side, away_result)

    away_back(0)
    pl.when(outer)(lambda: away_back(1))
    keep_sums(1 - side)
    each_peer(lambda peer: sums_copy(peer).start())
    half_copy(mine, side).wait_send()
    half_copy(mine, 1 - side).wait_send()
    slab_blocks(0).wait_send()
    slab_blocks(1).wait_send()
    other_copy(1 - side, 0).wait_send()
    other_copy(side, 1).wait_send()
    swap_copy(0).wait_send()
    return_copy(0).wait_send()
    pl.when(jnp.logical_not(direct))(lambda: swap_copy(1).wait_send())

    pl.when(direct)(lambda: direct_blocks(members).wait_send())
    pl.when(second_guest)(lambda: drain_all(*first, 1, 1, ends1(1)))
    pl.when(inner)(lambda: return_copy(1).wait_send())
    pl.when(inner)(lambda: blocks(pack - 1, *second, 1, 1, *ends2(1)).wait_send())
    pl.when(outer)(lambda: blocks(pack, *second, 1, 1, *ends2(1)).wait_send())
    result_blocks(pack).wait_send()
    drain_all(*first, 1, 0, ends1(1))
    drain_all(*second, 1, 0, ends2(1))
    each_row(lambda row: drain_all(*first, 0, row, ends1(0)))
    each_row(lambda row: drain_all(*second, 0, row, ends2(0)))
    sums_blocks().wait_recv()
    grams = jnp.sum(sums_ref[...], axis=0)
    for p in range(2):
        for b in range(bands):
            gram_ref[p, b : b + 1, :] = grams[b, p : p + 1, : 2 * bands]
    sums_blocks().wait_send()


def deliver_kernel(theta_ref, gram_ref, theta_out, gram_out, theta_sem, gram_sem):
    copies = [pltpu.make_async_copy(gram_ref, gram_out, gram_sem)]
    for p in range(2):
        for c in range(3):
            copies.append(
                pltpu.make_async_copy(theta_ref.at[p, c], theta_out.at[p, c], theta_sem.at[p, c])
            )
    for copy in copies:
        copy.start()
    for copy in copies:
        copy.wait()


def on_device_kernel(coeffs, material, inv_diag, inv_off):
    groups = lax.axis_size("gz")
    _, comps, bands, depth, height, breadth = coeffs.shape
    total = depth * groups
    members = groups // 2
    columns = height // members
    table = jnp.asarray(split_table(breadth, total**-0.25))
    voxels = (3, 2, total, columns, breadth)
    block = (2, depth, members, 3, 2, columns, breadth)
    pairs = (depth, 2, 2, height, breadth)
    vmem = pl.BlockSpec(memory_space=pltpu.VMEM)
    hbm = pl.BlockSpec(memory_space=pltpu.HBM)
    dma = pltpu.SemaphoreType.DMA
    operands = [
        pltpu.with_memory_space_constraint(v, pltpu.HBM)
        for v in (coeffs, material, inv_diag, inv_off, table)
    ]
    theta, gram = pl.pallas_call(
        functools.partial(operator_kernel, groups),
        out_shape=(
            jax.ShapeDtypeStruct(coeffs.shape, single),
            jax.ShapeDtypeStruct((2, bands, 2 * bands), single),
        ),
        in_specs=[hbm, hbm, hbm, hbm, hbm],
        out_specs=(vmem, vmem),
        scratch_shapes=[
            pltpu.VMEM(coeffs.shape, single),
            pltpu.VMEM(material.shape, jnp.int32),
            pltpu.VMEM(table.shape, half),
            pltpu.SMEM(inv_diag.shape, single),
            pltpu.SMEM(inv_off.shape, single),
            pltpu.VMEM((depth, groups, columns, breadth), jnp.int32),
            pltpu.VMEM((6, groups, depth, columns, breadth), single),
            pltpu.VMEM((depth, 2 * height, 3 * breadth), half),
            pltpu.VMEM((depth, 2 * height, 3 * breadth), half),
            pltpu.VMEM((depth, 2 * height, 3 * breadth), single),
            pltpu.VMEM((bands, *pairs), single),
            pltpu.VMEM((bands, *pairs), single),
            pltpu.VMEM(pairs, single),
            pltpu.VMEM(pairs, single),
            pltpu.VMEM(pairs, single),
            pltpu.VMEM(block, single),
            pltpu.VMEM(block, single),
            pltpu.VMEM(voxels, single),
            pltpu.VMEM(voxels, single),
            pltpu.VMEM(block, single),
            pltpu.VMEM(block, single),
            pltpu.VMEM(block[2:], single),
            pltpu.VMEM(block[2:], single),
            pltpu.VMEM((bands, 4 * bands, 16, breadth), single),
            pltpu.VMEM((groups, bands, 2, breadth), single),
            dma((4, depth)),
            dma((2,)),
            dma((2,)),
            dma((2, 2)),
            dma((2, depth)),
            dma((2, depth)),
            dma((2, depth)),
            dma((2, depth)),
            dma((4,)),
            dma((depth,)),
            dma((depth,)),
            dma((depth,)),
            dma((depth,)),
            dma((2,)),
            dma((2,)),
            dma((2,)),
        ],
        compiler_params=pltpu.CompilerParams(
            collective_id=0, has_side_effects=True, vmem_limit_bytes=48 * 1024 * 1024
        ),
        name="maxwell",
    )(*operands)
    theta, gram = pl.pallas_call(
        deliver_kernel,
        out_shape=(
            jax.ShapeDtypeStruct(theta.shape, single),
            jax.ShapeDtypeStruct(gram.shape, single),
        ),
        in_specs=[vmem, vmem],
        out_specs=(hbm, hbm),
        scratch_shapes=[dma((2, 3)), dma(())],
        compiler_params=pltpu.CompilerParams(vmem_limit_bytes=8 * 1024 * 1024),
        name="deliver",
    )(theta, gram)
    return (theta, gram.transpose(0, 2, 1))


def fits(coeffs):
    groups = lax.axis_size("gz")
    _, _, bands, depth, height, breadth = coeffs.shape
    return (
        lax.axis_size("ba") == 2
        and bands == 2
        and depth == 2
        and groups >= 8
        and height % (4 * groups) == 0
        and height % 16 == 0
        and height == breadth
        and breadth % 128 == 0
    )


def on_either(coeffs, material, inv_diag, inv_off):
    chosen = on_device_kernel if fits(coeffs) else on_device
    return chosen(coeffs, material, inv_diag, inv_off)


def solution(mesh):
    in_specs = (P(None, None, "ba", "gz", None, None), P("gz", None, None), P(), P())
    out_specs = (P(None, None, "ba", "gz", None, None), P(None, None, "ba"))
    return jax.shard_map(
        on_either, mesh=mesh, in_specs=in_specs, out_specs=out_specs, check_vma=False
    )
```

```python
import functools
import math

import jax
import jax.numpy as jnp
import numpy as np
from jax import lax
from jax.experimental import pallas as pl
from jax.experimental.pallas import tpu as pltpu
from jax.sharding import PartitionSpec as P

highest = lax.Precision.HIGHEST
half_turn = 3.141592653589793


def reverse_bits(values, levels):
    flipped = jnp.zeros_like(values)
    for position in range(levels):
        flipped = flipped + (values >> position & 1) * (1 << levels - 1 - position)
    return flipped


def signed_wave(numbers, length):
    shifted = jnp.where(numbers < length // 2, numbers, numbers - length)
    return shifted.astype(jnp.float32) / (length / 2.0)


def phase_tables(first, second, length, sign):
    product = first[:, None] * second[None, :] % length
    angle = 2.0 * half_turn / length * product.astype(jnp.float32)
    factor = 1.0 / math.sqrt(length)
    return (jnp.cos(angle) * factor, sign * jnp.sin(angle) * factor)


def cross_waves(waves, field):
    first, second, third = waves
    return jnp.stack(
        [
            second * field[:, 2] - third * field[:, 1],
            third * field[:, 0] - first * field[:, 2],
            first * field[:, 1] - second * field[:, 0],
        ],
        axis=1,
    )


def along_width(field, cosine, sine):
    breadth = field.shape[-1]
    rows = field.reshape(2, -1, breadth)
    joined = jnp.concatenate([cosine, sine], axis=1)
    real_prod = jnp.dot(rows[0], joined, precision=highest)
    imag_prod = jnp.dot(rows[1], joined, precision=highest)
    real_out = real_prod[:, :breadth] - imag_prod[:, breadth:]
    imag_out = real_prod[:, breadth:] + imag_prod[:, :breadth]
    return jnp.stack([real_out, imag_out]).reshape(field.shape)


def along_height(field, cosine, sine):
    tables = jnp.stack([cosine, sine])
    product = jnp.einsum("pcbzyx,tyk->tpcbzkx", field, tables, precision=highest)
    return jnp.stack([product[0, 0] - product[1, 1], product[1, 0] + product[0, 1]])


def along_depth(field, cosine, sine):
    tables = jnp.stack([cosine, sine])
    product = jnp.einsum("pcbzyx,tzk->tpcbkyx", field, tables, precision=highest)
    return jnp.stack([product[0, 0] - product[1, 1], product[1, 0] + product[0, 1]])


def apply_material(field, material, inv_diag, inv_off):
    materials = inv_diag.shape[0]
    onehot = (material[None] == jnp.arange(materials, dtype=jnp.int32)[:, None, None, None]).astype(
        jnp.float32
    )
    table = jnp.concatenate([inv_diag, inv_off], axis=1)
    tensor = jnp.einsum("mk,mzyx->kzyx", table, onehot, precision=highest)
    first = field[:, 0]
    second = field[:, 1]
    third = field[:, 2]
    return jnp.stack(
        [
            tensor[0] * first + tensor[3] * second + tensor[5] * third,
            tensor[3] * first + tensor[1] * second + tensor[4] * third,
            tensor[5] * first + tensor[4] * second + tensor[2] * third,
        ],
        axis=1,
    )


def on_device(coeffs, material, inv_diag, inv_off):
    groups = lax.axis_size("gz")
    levels = groups.bit_length() - 1
    depth = coeffs.shape[3]
    height = coeffs.shape[4]
    breadth = coeffs.shape[5]
    total_depth = depth * groups
    device = lax.axis_index("gz")
    local_rows = jnp.arange(depth, dtype=jnp.int32)
    waves_here = reverse_bits(device, levels) + groups * local_rows
    across = jnp.arange(breadth, dtype=jnp.int32)
    upward = jnp.arange(height, dtype=jnp.int32)
    waves = (
        signed_wave(across, breadth)[None, None, :],
        signed_wave(upward, height)[None, :, None],
        signed_wave(waves_here, total_depth)[:, None, None],
    )
    curl = cross_waves(waves, coeffs)
    all_rows = jnp.arange(total_depth, dtype=jnp.int32)
    wave_rows = reverse_bits(all_rows // depth, levels) + groups * (all_rows % depth)
    height_cos, height_sin = phase_tables(upward, upward, height, 1.0)
    width_cos, width_sin = phase_tables(across, across, breadth, 1.0)
    planar = along_height(curl, height_cos, height_sin)
    planar = along_width(planar, width_cos, width_sin)
    material_slab = lax.all_to_all(material, "gz", split_axis=1, concat_axis=0, tiled=True)
    inverse_cos, inverse_sin = phase_tables(wave_rows, all_rows, total_depth, 1.0)
    forward_cos, forward_sin = phase_tables(all_rows, wave_rows, total_depth, -1.0)
    spatial_piece = along_depth(
        lax.all_to_all(planar, "gz", split_axis=4, concat_axis=3, tiled=True),
        inverse_cos,
        inverse_sin,
    )
    scaled_piece = apply_material(spatial_piece, material_slab, inv_diag, inv_off)
    returned = along_depth(scaled_piece, forward_cos, forward_sin)
    spectral = lax.all_to_all(returned, "gz", split_axis=3, concat_axis=4, tiled=True)
    spectral = along_width(spectral, width_cos, -width_sin)
    spectral = along_height(spectral, height_cos, -height_sin)
    theta = -cross_waves(waves, spectral)
    factor = 1.0 / (breadth * height * total_depth)
    piece = lax.all_gather(coeffs, "ba", axis=2, tiled=True)
    real_part = jnp.einsum("cbzyx,cezyx->be", piece[0], theta[0], precision=highest) + jnp.einsum(
        "cbzyx,cezyx->be", piece[1], theta[1], precision=highest
    )
    imag_part = jnp.einsum("cbzyx,cezyx->be", piece[0], theta[1], precision=highest) - jnp.einsum(
        "cbzyx,cezyx->be", piece[1], theta[0], precision=highest
    )
    block = jnp.stack([real_part, imag_part]) * factor
    gram = lax.psum(block, "gz")
    return (theta, gram)


MESH = pl.DeviceIdType.MESH
single = jnp.float32
half = jnp.bfloat16


def split_table(length, extra):
    numbers = np.arange(length)
    angle = 2.0 * np.pi / length * (numbers[:, None] * numbers[None, :] % length)
    cosine = np.cos(angle) * extra / math.sqrt(length)
    sine = np.sin(angle) * extra / math.sqrt(length)
    inverse = np.block([[cosine, sine], [-sine, cosine]])
    parts = []
    for table in (inverse, inverse.T):
        high = table.astype(np.float32).astype(half)
        low = (table - high.astype(np.float64)).astype(half)
        parts += [high, low]
    return np.stack(parts)


def halves(values):
    high = values.astype(half)
    return high, (values - high.astype(single)).astype(half)


def product(first, second):
    dot = functools.partial(jnp.dot, preferred_element_type=single)
    return dot(first[0], second[0]) + (dot(first[0], second[1]) + dot(first[1], second[0]))


def twiddled(pair, step, span, sign):
    real, imag = pair
    if step == 0:
        return real, imag
    if 2 * step == span:
        return (-imag, real) if sign > 0 else (imag, -real)
    angle = math.pi * step / span
    cosine, sine = math.cos(angle), sign * math.sin(angle)
    return real * cosine - imag * sine, real * sine + imag * cosine


def to_voxels(points):
    points = list(points)
    span = 1
    while span < len(points):
        for base in range(0, len(points), 2 * span):
            for step in range(span):
                a = points[base + step]
                t = twiddled(points[base + step + span], step, span, 1.0)
                points[base + step] = (a[0] + t[0], a[1] + t[1])
                points[base + step + span] = (a[0] - t[0], a[1] - t[1])
        span *= 2
    return points


def to_waves(points):
    points = list(points)
    span = len(points) // 2
    while span >= 1:
        for base in range(0, len(points), 2 * span):
            for step in range(span):
                a, t = points[base + step], points[base + step + span]
                points[base + step] = (a[0] + t[0], a[1] + t[1])
                points[base + step + span] = twiddled(
                    (a[0] - t[0], a[1] - t[1]), step, span, -1.0
                )
        span //= 2
    return points


def operator_kernel(
    groups,
    coeffs_hbm,
    material_hbm,
    diag_hbm,
    off_hbm,
    table_hbm,
    theta_ref,
    gram_ref,
    coeffs_ref,
    material_ref,
    table_ref,
    diag_ref,
    off_ref,
    slab_ref,
    tensor_ref,
    high_ref,
    low_ref,
    back_ref,
    pair_ref,
    other_ref,
    swap_ref,
    result_ref,
    return_ref,
    out1_ref,
    in1_ref,
    field_ref,
    scaled_ref,
    out2_ref,
    in2_ref,
    out3_ref,
    in3_ref,
    acc_ref,
    sums_ref,
    load_sem,
    slab_send,
    slab_recv,
    half_sem,
    send1,
    recv1,
    send2,
    recv2,
    far_sem,
    swap_send,
    swap_recv,
    return_send,
    return_recv,
    other_send,
    other_recv,
    sums_sem,
):
    _, comps, bands, depth, height, breadth = coeffs_ref.shape
    total = depth * groups
    members = groups // 2
    columns = height // members
    levels = groups.bit_length() - 1
    me = lax.axis_index("gz")
    mine = lax.axis_index("ba")
    side = me // members
    seat = me % members
    partner = (me + members) % groups
    pack = members // 2
    inner = seat // pack == 1 - side
    outer = jnp.logical_not(inner)
    odd = seat % 2 == 1
    direct = jnp.logical_and(inner, jnp.logical_not(odd))
    second_guest = jnp.logical_or(inner, odd)
    mate = {"ba": 1 - mine}
    step_rows = 16
    steps = height // step_rows

    def each_peer(body):
        def step(k, carry):
            body((me + k) % groups)
            return carry

        lax.fori_loop(1, groups, step, 0)

    def each_member(body):
        def step(k, carry):
            body(k, (seat + k) % members)
            return carry

        lax.fori_loop(1, members, step, 0)

    def row_load(b, row, n):
        return pltpu.make_async_copy(
            coeffs_hbm.at[:, :, b, row], coeffs_ref.at[:, :, b, row], load_sem.at[n, row]
        )

    loads = [
        pltpu.make_async_copy(table_hbm, table_ref, load_sem.at[2, 0]),
        pltpu.make_async_copy(material_hbm, material_ref, load_sem.at[2, 1]),
        pltpu.make_async_copy(diag_hbm, diag_ref, load_sem.at[3, 0]),
        pltpu.make_async_copy(off_hbm, off_ref, load_sem.at[3, 1]),
    ]
    row_load(1 - side, 0, 0).start()
    barrier = pltpu.get_barrier_semaphore()
    each_peer(
        lambda peer: pl.semaphore_signal(
            barrier, inc=1, device_id={"gz": peer}, device_id_type=MESH
        )
    )
    pl.semaphore_signal(barrier, inc=1, device_id=mate, device_id_type=MESH)

    row_load(1 - side, 1, 0).start()
    for row in range(depth):
        row_load(side, row, 1).start()
    for load in loads:
        load.start()

    def signed(number, length):
        return number - length * (number // (length // 2))

    def row_number(owner, row):
        reversed_owner = 0
        for position in range(levels):
            bit = (owner // (1 << position)) % 2
            reversed_owner = reversed_owner + bit * (1 << (levels - 1 - position))
        return signed(reversed_owner + groups * row, total)

    def inverse_of(values):
        zero = values == 0
        return jnp.where(zero, 0.0, 1.0 / jnp.where(zero, 1, values).astype(single))

    class Waves:
        def __init__(self, owner, row, i):
            shape = (step_rows, breadth)
            nx = lax.broadcasted_iota(jnp.int32, shape, 1)
            ny = lax.broadcasted_iota(jnp.int32, shape, 0) + i * step_rows
            nx = jnp.where(nx < breadth // 2, nx, nx - breadth)
            ny = jnp.where(ny < height // 2, ny, ny - height)
            nz = jnp.full(shape, row_number(owner, row), jnp.int32)
            self.x = nx.astype(single) / (breadth / 2.0)
            self.y = ny.astype(single) / (height / 2.0)
            self.z = nz.astype(single) / (total / 2.0)
            ax, ay, az = jnp.abs(nx) * total, jnp.abs(ny) * total, jnp.abs(nz) * breadth
            self.is_x = (ax >= ay) & (ax >= az)
            self.is_y = ay >= az
            self.numbers = (nx, ny, nz)

        def cross(self, v):
            q = (self.x, self.y, self.z)
            return [
                q[(c + 1) % 3] * v[(c + 2) % 3] - q[(c + 2) % 3] * v[(c + 1) % 3]
                for c in range(3)
            ]

        def pick(self, first, second, third):
            return jnp.where(self.is_x, first, jnp.where(self.is_y, second, third))

        def inverse(self):
            nx, ny, nz = self.numbers
            scaled = self.pick(nx * total, ny * total, nz * breadth)
            return inverse_of(scaled) * (total * breadth / 2.0)

        def ratios(self):
            inverse = self.inverse()
            return (
                self.pick(self.y, self.z, self.x) * inverse,
                self.pick(self.z, self.x, self.y) * inverse,
            )

        def reduce(self, v):
            return self.pick(v[1], v[2], v[0]), self.pick(v[2], v[0], v[1])

        def rebuild(self, ratios, first, second):
            last = -(ratios[0] * first + ratios[1] * second)
            return [
                self.pick(last, second, first),
                self.pick(first, last, second),
                self.pick(second, first, last),
            ]

    def rows_of(i):
        return pl.ds(pl.multiple_of(i * step_rows, step_rows), step_rows)

    def each_step(row, body):
        def step(i, carry):
            body(row, i)
            return carry

        lax.fori_loop(0, steps, step, 0)

    def each_row(body):
        def step(row, carry):
            body(row)
            return carry

        lax.fori_loop(0, depth, step, 0)

    def put_halves(curls, p, row, i):
        at = pl.ds(pl.multiple_of(p * height + i * step_rows, step_rows), step_rows)
        for c in range(3):
            high, low = halves(curls[c])
            lanes = pl.ds(c * breadth, breadth)
            high_ref[row, at, lanes] = high
            low_ref[row, at, lanes] = low

    def put_pair(b, p, row, i, pair):
        for n in range(2):
            pair_ref[b, row, n, p, rows_of(i), :] = pair[n]

    def away_step(row, i):
        waves = Waves(me, row, i)
        for p in range(2):
            values = [coeffs_ref[p, c, 1 - side, row, rows_of(i), :] for c in range(3)]
            put_pair(1 - side, p, row, i, waves.reduce(waves.cross(values)))

    def home_step(row, i):
        waves = Waves(me, row, i)
        for p in range(2):
            values = [coeffs_ref[p, c, side, row, rows_of(i), :] for c in range(3)]
            curls = waves.cross(values)
            put_halves(curls, p, row, i)
            put_pair(side, p, row, i, waves.reduce(curls))

    def direct_step(row, i):
        waves = Waves(me, row, i)
        for p in range(2):
            values = [coeffs_ref[p, c, 1 - side, row, rows_of(i), :] for c in range(3)]
            put_halves(waves.cross(values), p, row, i)

    def guest_step(row, i):
        waves = Waves(partner, row, i)
        ratios = waves.ratios()
        for p in range(2):
            pair = [swap_ref[row, n, p, rows_of(i), :] for n in range(2)]
            put_halves(waves.rebuild(ratios, *pair), p, row, i)

    def plain_table():
        return table_ref[0], table_ref[1]

    def turned_table():
        return table_ref[2], table_ref[3]

    def gather_blocks(values):
        top, bottom = values[:height], values[height:]
        return jnp.concatenate(
            [
                jnp.concatenate(
                    [
                        top[:, z * breadth : (z + 1) * breadth],
                        bottom[:, z * breadth : (z + 1) * breadth],
                    ],
                    axis=1,
                )
                for z in range(3)
            ],
            axis=0,
        )

    def spread_blocks(values):
        return jnp.concatenate(
            [
                jnp.concatenate(
                    [
                        values[z * height : (z + 1) * height, p * breadth : (p + 1) * breadth]
                        for z in range(3)
                    ],
                    axis=1,
                )
                for p in range(2)
            ],
            axis=0,
        )

    def to_peer(out, into, send, recv, s, row, peer, from_at, to_at):
        return pltpu.make_async_remote_copy(
            src_ref=out.at[from_at, row, peer],
            dst_ref=into.at[to_at, row, seat],
            send_sem=send.at[s, row],
            recv_sem=recv.at[s, row],
            device_id={"gz": side * members + peer},
            device_id_type=MESH,
        )

    def blocks(count, out, into, send, recv, s, row, from_at, to_at):
        return pltpu.make_async_remote_copy(
            src_ref=out.at[from_at, row, pl.ds(0, count)],
            dst_ref=into.at[to_at, row, pl.ds(0, count)],
            send_sem=send.at[s, row],
            recv_sem=recv.at[s, row],
            device_id={"gz": side * members + (seat + 1) % members},
            device_id_type=MESH,
        )

    def ends1(s):
        return s, (side + s) % 2

    def ends2(s):
        return (side + s) % 2, s

    def start_all(out, into, send, recv, s, row, ends):
        each_member(lambda k, peer: to_peer(out, into, send, recv, s, row, peer, *ends).start())
        into[ends[1], row, seat] = out[ends[0], row, seat]

    def finish_all(out, into, send, recv, s, row, ends):
        blocks(members - 1, out, into, send, recv, s, row, *ends).wait_recv()

    def drain_all(out, into, send, recv, s, row, ends):
        blocks(members - 1, out, into, send, recv, s, row, *ends).wait_send()

    def is_inner(peer):
        return peer // pack == 1 - side

    def each_inner(body):
        def one(k, peer):
            pl.when(is_inner(peer))(lambda: body(k, peer))

        each_member(one)

    def across(peer):
        return {"gz": (1 - side) * members + peer}

    def direct_copy(peer):
        return pltpu.make_async_remote_copy(
            src_ref=out3_ref.at[peer],
            dst_ref=in1_ref.at[side, 1, seat],
            send_sem=far_sem.at[0],
            recv_sem=far_sem.at[1],
            device_id=across(peer),
            device_id_type=MESH,
        )

    def direct_blocks(count):
        return pltpu.make_async_remote_copy(
            src_ref=out3_ref.at[pl.ds(0, count)],
            dst_ref=in1_ref.at[1 - side, 1, pl.ds(0, count)],
            send_sem=far_sem.at[0],
            recv_sem=far_sem.at[1],
            device_id=across(seat),
            device_id_type=MESH,
        )

    def direct_result(n):
        peer = side * pack + n
        return pltpu.make_async_remote_copy(
            src_ref=out2_ref.at[1 - side, 1, peer],
            dst_ref=in3_ref.at[seat],
            send_sem=far_sem.at[2],
            recv_sem=far_sem.at[3],
            device_id=across(peer),
            device_id_type=MESH,
        )

    def result_blocks(count):
        return pltpu.make_async_remote_copy(
            src_ref=out2_ref.at[1 - side, 1, pl.ds(0, count)],
            dst_ref=in3_ref.at[pl.ds(0, count)],
            send_sem=far_sem.at[2],
            recv_sem=far_sem.at[3],
            device_id=across(seat),
            device_id_type=MESH,
        )

    def each_of(count, body):
        def step(n, carry):
            body(n)
            return carry

        lax.fori_loop(0, count, step, 0)

    first = (out1_ref, in1_ref, send1, recv1)
    second = (out2_ref, in2_ref, send2, recv2)

    def planes_into(put, row):
        tall = product(turned_table(), (high_ref[row], low_ref[row]))
        wide = product(halves(gather_blocks(tall)), plain_table())
        for p in range(2):
            for c in range(3):
                plane = wide[c * height : (c + 1) * height, p * breadth : (p + 1) * breadth]
                put(c, p, plane.reshape(members, columns, breadth))

    def make_planes(s, row):
        def put(c, p, block):
            out1_ref[s, row, :, c, p] = block

        planes_into(put, row)

    def swap_copy(row):
        return pltpu.make_async_remote_copy(
            src_ref=pair_ref.at[1 - side, row],
            dst_ref=swap_ref.at[row],
            send_sem=swap_send.at[row],
            recv_sem=swap_recv.at[row],
            device_id={"gz": partner},
            device_id_type=MESH,
        )

    def return_copy(row):
        return pltpu.make_async_remote_copy(
            src_ref=result_ref.at[row],
            dst_ref=return_ref.at[row],
            send_sem=return_send.at[row],
            recv_sem=return_recv.at[row],
            device_id={"gz": partner},
            device_id_type=MESH,
        )

    def other_copy(b, n):
        return pltpu.make_async_remote_copy(
            src_ref=pair_ref.at[b],
            dst_ref=other_ref.at[b],
            send_sem=other_send.at[n],
            recv_sem=other_recv.at[n],
            device_id=mate,
            device_id_type=MESH,
        )

    def columns_of(peer):
        return pl.ds(pl.multiple_of((peer % members) * columns, columns), columns)

    def slab_copy(peer, n):
        return pltpu.make_async_remote_copy(
            src_ref=material_ref.at[mine, columns_of(peer), :],
            dst_ref=slab_ref.at[mine, me],
            send_sem=slab_send.at[n],
            recv_sem=slab_recv.at[n],
            device_id={"gz": peer},
            device_id_type=MESH,
        )

    def slab_blocks(n):
        slots = slab_ref.at[mine, pl.ds(0, members - 1 + n)]
        return pltpu.make_async_remote_copy(
            src_ref=slots,
            dst_ref=slots,
            send_sem=slab_send.at[n],
            recv_sem=slab_recv.at[n],
            device_id={"gz": partner},
            device_id_type=MESH,
        )

    def half_copy(row, part):
        at = pl.ds(pl.multiple_of(part * members, members), members)
        return pltpu.make_async_remote_copy(
            src_ref=slab_ref.at[row, at],
            dst_ref=slab_ref.at[row, at],
            send_sem=half_sem.at[0, part],
            recv_sem=half_sem.at[1, part],
            device_id=mate,
            device_id_type=MESH,
        )

    def away_row(row):
        row_load(1 - side, row, 0).wait()
        each_step(row, away_step)

    def home_row(row):
        row_load(side, row, 1).wait()
        each_step(row, home_step)
        make_planes(0, row)
        start_all(*first, 0, row, ends1(0))

    def start_slab(base, n):
        def step(k, carry):
            slab_copy(base * members + (seat + k) % members, n).start()
            return carry

        lax.fori_loop(1 - n, members, step, 0)

    away_row(0)
    pl.semaphore_wait(barrier, groups)
    swap_copy(0).start()
    for load in loads:
        load.wait()
    pl.when(inner)(lambda: start_slab(side, 0))
    pl.when(inner)(lambda: start_slab(1 - side, 1))
    away_row(1)
    pl.when(jnp.logical_not(direct))(lambda: swap_copy(1).start())
    pl.when(outer)(lambda: start_slab(side, 0))
    pl.when(outer)(lambda: start_slab(1 - side, 1))
    slab_ref[mine, me] = material_ref[mine, columns_of(me), :]
    home_row(0)
    home_row(1)

    def make_direct():
        each_step(1, direct_step)

        def put(c, p, block):
            out3_ref[:, c, p] = block

        planes_into(put, 1)

    def send_direct():
        each_of(members, lambda n: direct_copy((seat + n) % members).start())

    pl.when(direct)(make_direct)
    other_copy(side, 1).start()
    acc_ref[...] = jnp.zeros(acc_ref.shape, single)

    def guest_row(row):
        swap_copy(row).wait_recv()
        each_step(row, guest_step)
        make_planes(1, row)
        start_all(*first, 1, row, ends1(1))

    guest_row(0)
    slab_blocks(0).wait_recv()
    half_copy(mine, side).start()
    pl.when(inner)(lambda: guest_row(1))
    slab_blocks(1).wait_recv()
    half_copy(mine, 1 - side).start()
    pl.when(direct)(send_direct)
    pl.when(jnp.logical_and(outer, odd))(lambda: guest_row(1))
    half_copy(1 - mine, side).wait_recv()
    half_copy(1 - mine, 1 - side).wait_recv()
    kinds = diag_ref.shape[0]

    def tensor_step(owner, carry):
        for row in range(depth):
            codes = slab_ref[row, owner]
            for entry in range(6):
                table = diag_ref if entry < 3 else off_ref
                values = jnp.full(codes.shape, table[0, entry % 3], single)
                for kind in range(1, kinds):
                    values = jnp.where(codes == kind, table[kind, entry % 3], values)
                tensor_ref[entry, owner, row] = values
        return carry

    lax.fori_loop(0, groups, tensor_step, 0)

    def part_of(n):
        return pl.ds(pl.multiple_of(n * 8, 8), 8)

    each_row(lambda row: finish_all(*first, 0, row, ends1(0)))
    finish_all(*first, 1, 0, ends1(1))

    def finish_second(count):
        blocks(count, *first, 1, 1, *ends1(1)).wait_recv()

    guests = pack + pack // 2
    pl.when(second_guest)(lambda: finish_second(guests - 1))
    pl.when(jnp.logical_not(second_guest))(lambda: finish_second(guests))
    direct_blocks(pack // 2).wait_recv()

    def inverse(at, c):
        points = []
        for r in range(total):
            owner, row = r // depth, r % depth
            where = (owner // members, row, owner % members, c)
            points.append((in1_ref[(*where, 0, at)], in1_ref[(*where, 1, at)]))
        for z, (real, imag) in enumerate(to_voxels(points)):
            field_ref[c, 0, z, at] = real
            field_ref[c, 1, z, at] = imag

    def scale(at, z):
        entries = [tensor_ref[entry, z // depth, z % depth, at] for entry in range(6)]
        xx, yy, zz, xy, yz, zx = entries
        for p in range(2):
            fx, fy, fz = [field_ref[c, p, z, at] for c in range(3)]
            scaled_ref[0, p, z, at] = xx * fx + xy * fy + zx * fz
            scaled_ref[1, p, z, at] = xy * fx + yy * fy + yz * fz
            scaled_ref[2, p, z, at] = zx * fx + yz * fy + zz * fz

    def forward(at, c):
        points = [(scaled_ref[c, 0, z, at], scaled_ref[c, 1, z, at]) for z in range(total)]
        for r, (real, imag) in enumerate(to_waves(points)):
            owner, row = r // depth, r % depth
            where = (owner // members, row, owner % members, c)
            out2_ref[(*where, 0, at)] = real
            out2_ref[(*where, 1, at)] = imag

    parts = columns // 8

    def part_copy(n, peer):
        at = part_of(n)
        return pltpu.make_async_remote_copy(
            src_ref=out2_ref.at[1 - side, 0, peer, :, :, at],
            dst_ref=in2_ref.at[1, 0, seat, :, :, at],
            send_sem=send2.at[1, 0],
            recv_sem=recv2.at[1, 0],
            device_id={"gz": side * members + peer},
            device_id_type=MESH,
        )

    def voxel_part(n):
        at = part_of(n)
        each_of(3, functools.partial(inverse, at))

        def scale_step(z, carry):
            scale(at, z)
            return carry

        lax.fori_loop(0, total, scale_step, 0, unroll=4)
        each_of(3, functools.partial(forward, at))
        each_member(lambda k, peer: part_copy(n, peer).start())

    each_of(parts, voxel_part)
    in2_ref[1, 0, seat] = out2_ref[1 - side, 0, seat]
    each_of(pack, lambda n: direct_result((seat + n) % pack).start())
    each_inner(lambda k, peer: to_peer(*second, 1, 1, peer, *ends2(1)).start())

    def keep_guest():
        in2_ref[1, 1, seat] = out2_ref[1 - side, 1, seat]

    pl.when(inner)(keep_guest)

    def start_home(row):
        start_all(*second, 0, row, ends2(0))

    pl.when(inner)(lambda: start_home(0))
    pl.when(inner)(lambda: start_home(1))
    other_copy(1 - side, 0).start()

    def planes_back(get, row):
        planes = jnp.concatenate(
            [
                jnp.concatenate(
                    [get(c, p).reshape(height, breadth) for p in range(2)], axis=1
                )
                for c in range(3)
            ],
            axis=0,
        )
        wide = product(halves(planes), turned_table())
        back_ref[row] = product(plain_table(), halves(spread_blocks(wide)))

    def take_planes(s, row):
        planes_back(lambda c, p: in2_ref[s, row, :, c, p], row)

    def theta_at(waves, p, row, i):
        at = pl.ds(pl.multiple_of(p * height + i * step_rows, step_rows), step_rows)
        lanes = [pl.ds(c * breadth, breadth) for c in range(3)]
        return [-v for v in waves.cross([back_ref[row, at, lanes[c]] for c in range(3)])]

    def guest_result(row, i):
        waves = Waves(partner, row, i)
        for p in range(2):
            pair = waves.reduce(theta_at(waves, p, row, i))
            for n in range(2):
                result_ref[row, n, p, rows_of(i), :] = pair[n]

    def add_sums(waves, pairs, row, i, sums):
        inverse = waves.inverse()
        (real1, real2), (imag1, imag2) = [[inverse * v for v in pair] for pair in pairs]
        sums = list(sums)
        n = 0
        for source in (pair_ref, other_ref):
            for a in range(bands):
                one_real, one_imag = [source[a, row, 0, p, rows_of(i), :] for p in range(2)]
                two_real, two_imag = [source[a, row, 1, p, rows_of(i), :] for p in range(2)]
                real = (two_real * real1 + two_imag * imag1) - (one_real * real2 + one_imag * imag2)
                imag = (two_real * imag1 - two_imag * real1) - (one_real * imag2 - one_imag * real2)
                sums[n] = sums[n] + real
                sums[n + 1] = sums[n + 1] + imag
                n += 2
        return tuple(sums)

    def each_sum(row, b, body):
        def step(i, sums):
            return body(row, i, sums)

        sums = lax.fori_loop(0, steps, step, tuple(acc_ref[b, n] for n in range(4 * bands)))
        for n in range(4 * bands):
            acc_ref[b, n] = sums[n]

    def keep_sums(b):
        sums = [acc_ref[b, n] for n in range(4 * bands)]
        lane = lax.broadcasted_iota(jnp.int32, (1, breadth), 1)
        rows = [jnp.zeros((1, breadth), single)] * 2
        n = 0
        for source in (mine, 1 - mine):
            for a in range(bands):
                for p in range(2):
                    value = jnp.sum(jnp.sum(sums[n], axis=0, keepdims=True), axis=1, keepdims=True)
                    rows[p] = rows[p] + jnp.where(lane == source * bands + a, value, 0.0)
                    n += 1
        sums_ref[me, b] = jnp.concatenate(rows, axis=0) * (1.0 / (breadth * height * total))

    def result_of(b):
        def result(row, i, sums):
            waves = Waves(me, row, i)
            pairs = []
            for p in range(2):
                theta = theta_at(waves, p, row, i)
                for c in range(3):
                    theta_ref[p, c, b, row, rows_of(i), :] = theta[c]
                pairs.append(waves.reduce(theta))
            return add_sums(waves, pairs, row, i, sums)

        return result

    def away_result(row, i, sums):
        waves = Waves(me, row, i)
        ratios = waves.ratios()
        pairs = []
        for p in range(2):
            pair = [return_ref[row, n, p, rows_of(i), :] for n in range(2)]
            theta = waves.rebuild(ratios, *pair)
            for c in range(3):
                theta_ref[p, c, 1 - side, row, rows_of(i), :] = theta[c]
            pairs.append(pair)
        return add_sums(waves, pairs, row, i, sums)

    def sums_copy(peer):
        return pltpu.make_async_remote_copy(
            src_ref=sums_ref.at[me],
            dst_ref=sums_ref.at[me],
            send_sem=sums_sem.at[0],
            recv_sem=sums_sem.at[1],
            device_id={"gz": peer},
            device_id_type=MESH,
        )

    def sums_blocks():
        slots = sums_ref.at[pl.ds(0, groups - 1)]
        return pltpu.make_async_remote_copy(
            src_ref=slots,
            dst_ref=slots,
            send_sem=sums_sem.at[0],
            recv_sem=sums_sem.at[1],
            device_id={"gz": partner},
            device_id_type=MESH,
        )

    def guest_back(row):
        take_planes(1, row)
        each_step(row, guest_result)
        return_copy(row).start()

    def second_back():
        finish_all(*second, 1, 1, ends2(1))
        guest_back(1)

    finish_all(*second, 1, 0, ends2(1))
    guest_back(0)
    pl.when(outer)(lambda: start_home(0))
    pl.when(outer)(lambda: start_home(1))
    pl.when(inner)(second_back)
    other_copy(side, 1).wait_recv()
    other_copy(1 - side, 0).wait_recv()

    def take_direct():
        result_blocks(members).wait_recv()
        planes_back(lambda c, p: in3_ref[:, c, p], 1)
        each_sum(1, 1 - side, result_of(1 - side))

    pl.when(inner)(take_direct)

    def home_back(row):
        finish_all(*second, 0, row, ends2(0))
        take_planes(0, row)
        each_sum(row, side, result_of(side))

    def away_back(row):
        return_copy(row).wait_recv()
        each_sum(row, 1 - side, away_result)

    def finish_inner():
        away_back(0)
        keep_sums(1 - side)
        home_back(1)
        keep_sums(side)

    def finish_outer():
        home_back(1)
        keep_sums(side)
        away_back(0)
        away_back(1)
        keep_sums(1 - side)

    home_back(0)
    pl.when(inner)(finish_inner)
    pl.when(outer)(finish_outer)

    def start_sums(n, carry):
        peer = (2 * groups - 1 - me + n) % groups
        pl.when(peer != me)(lambda: sums_copy(peer).start())
        return carry

    lax.fori_loop(0, groups, start_sums, 0)
    half_copy(mine, side).wait_send()
    half_copy(mine, 1 - side).wait_send()
    slab_blocks(0).wait_send()
    slab_blocks(1).wait_send()
    other_copy(1 - side, 0).wait_send()
    other_copy(side, 1).wait_send()
    swap_copy(0).wait_send()
    return_copy(0).wait_send()
    pl.when(jnp.logical_not(direct))(lambda: swap_copy(1).wait_send())

    pl.when(direct)(lambda: direct_blocks(members).wait_send())
    pl.when(second_guest)(lambda: drain_all(*first, 1, 1, ends1(1)))
    pl.when(inner)(lambda: return_copy(1).wait_send())
    pl.when(inner)(lambda: blocks(pack - 1, *second, 1, 1, *ends2(1)).wait_send())
    pl.when(outer)(lambda: blocks(pack, *second, 1, 1, *ends2(1)).wait_send())
    result_blocks(pack).wait_send()
    drain_all(*first, 1, 0, ends1(1))
    drain_all(*second, 1, 0, ends2(1))
    each_row(lambda row: drain_all(*first, 0, row, ends1(0)))
    each_row(lambda row: drain_all(*second, 0, row, ends2(0)))
    sums_blocks().wait_recv()
    grams = jnp.sum(sums_ref[...], axis=0)
    for p in range(2):
        for b in range(bands):
            gram_ref[p, b : b + 1, :] = grams[b, p : p + 1, : 2 * bands]
    sums_blocks().wait_send()


def deliver_kernel(theta_ref, gram_ref, theta_out, gram_out, theta_sem, gram_sem):
    copies = [pltpu.make_async_copy(gram_ref, gram_out, gram_sem)]
    for p in range(2):
        for c in range(3):
            copies.append(
                pltpu.make_async_copy(theta_ref.at[p, c], theta_out.at[p, c], theta_sem.at[p, c])
            )
    for copy in copies:
        copy.start()
    for copy in copies:
        copy.wait()


def on_device_kernel(coeffs, material, inv_diag, inv_off):
    groups = lax.axis_size("gz")
    _, comps, bands, depth, height, breadth = coeffs.shape
    total = depth * groups
    members = groups // 2
    columns = height // members
    table = jnp.asarray(split_table(breadth, total**-0.25))
    voxels = (3, 2, total, columns, breadth)
    block = (2, depth, members, 3, 2, columns, breadth)
    pairs = (depth, 2, 2, height, breadth)
    vmem = pl.BlockSpec(memory_space=pltpu.VMEM)
    hbm = pl.BlockSpec(memory_space=pltpu.HBM)
    dma = pltpu.SemaphoreType.DMA
    operands = [
        pltpu.with_memory_space_constraint(v, pltpu.HBM)
        for v in (coeffs, material, inv_diag, inv_off, table)
    ]
    theta, gram = pl.pallas_call(
        functools.partial(operator_kernel, groups),
        out_shape=(
            jax.ShapeDtypeStruct(coeffs.shape, single),
            jax.ShapeDtypeStruct((2, bands, 2 * bands), single),
        ),
        in_specs=[hbm, hbm, hbm, hbm, hbm],
        out_specs=(vmem, vmem),
        scratch_shapes=[
            pltpu.VMEM(coeffs.shape, single),
            pltpu.VMEM(material.shape, jnp.int32),
            pltpu.VMEM(table.shape, half),
            pltpu.SMEM(inv_diag.shape, single),
            pltpu.SMEM(inv_off.shape, single),
            pltpu.VMEM((depth, groups, columns, breadth), jnp.int32),
            pltpu.VMEM((6, groups, depth, columns, breadth), single),
            pltpu.VMEM((depth, 2 * height, 3 * breadth), half),
            pltpu.VMEM((depth, 2 * height, 3 * breadth), half),
            pltpu.VMEM((depth, 2 * height, 3 * breadth), single),
            pltpu.VMEM((bands, *pairs), single),
            pltpu.VMEM((bands, *pairs), single),
            pltpu.VMEM(pairs, single),
            pltpu.VMEM(pairs, single),
            pltpu.VMEM(pairs, single),
            pltpu.VMEM(block, single),
            pltpu.VMEM(block, single),
            pltpu.VMEM(voxels, single),
            pltpu.VMEM(voxels, single),
            pltpu.VMEM(block, single),
            pltpu.VMEM(block, single),
            pltpu.VMEM(block[2:], single),
            pltpu.VMEM(block[2:], single),
            pltpu.VMEM((bands, 4 * bands, 16, breadth), single),
            pltpu.VMEM((groups, bands, 2, breadth), single),
            dma((4, depth)),
            dma((2,)),
            dma((2,)),
            dma((2, 2)),
            dma((2, depth)),
            dma((2, depth)),
            dma((2, depth)),
            dma((2, depth)),
            dma((4,)),
            dma((depth,)),
            dma((depth,)),
            dma((depth,)),
            dma((depth,)),
            dma((2,)),
            dma((2,)),
            dma((2,)),
        ],
        compiler_params=pltpu.CompilerParams(
            collective_id=0, has_side_effects=True, vmem_limit_bytes=48 * 1024 * 1024
        ),
        name="maxwell",
    )(*operands)
    theta, gram = pl.pallas_call(
        deliver_kernel,
        out_shape=(
            jax.ShapeDtypeStruct(theta.shape, single),
            jax.ShapeDtypeStruct(gram.shape, single),
        ),
        in_specs=[vmem, vmem],
        out_specs=(hbm, hbm),
        scratch_shapes=[dma((2, 3)), dma(())],
        compiler_params=pltpu.CompilerParams(vmem_limit_bytes=8 * 1024 * 1024),
        name="deliver",
    )(theta, gram)
    return (theta, gram.transpose(0, 2, 1))


def fits(coeffs):
    groups = lax.axis_size("gz")
    _, _, bands, depth, height, breadth = coeffs.shape
    return (
        lax.axis_size("ba") == 2
        and bands == 2
        and depth == 2
        and groups >= 8
        and height % (4 * groups) == 0
        and height % 16 == 0
        and height == breadth
        and breadth % 128 == 0
    )


def on_either(coeffs, material, inv_diag, inv_off):
    chosen = on_device_kernel if fits(coeffs) else on_device
    return chosen(coeffs, material, inv_diag, inv_off)


def solution(mesh):
    in_specs = (P(None, None, "ba", "gz", None, None), P("gz", None, None), P(), P())
    out_specs = (P(None, None, "ba", "gz", None, None), P(None, None, "ba"))
    return jax.shard_map(
        on_either, mesh=mesh, in_specs=in_specs, out_specs=out_specs, check_vma=False
    )
```

```python
import functools
import math

import jax
import jax.numpy as jnp
import numpy as np
from jax import lax
from jax.experimental import pallas as pl
from jax.experimental.pallas import tpu as pltpu
from jax.sharding import PartitionSpec as P

highest = lax.Precision.HIGHEST
half_turn = 3.141592653589793


def reverse_bits(values, levels):
    flipped = jnp.zeros_like(values)
    for position in range(levels):
        flipped = flipped + (values >> position & 1) * (1 << levels - 1 - position)
    return flipped


def signed_wave(numbers, length):
    shifted = jnp.where(numbers < length // 2, numbers, numbers - length)
    return shifted.astype(jnp.float32) / (length / 2.0)


def phase_tables(first, second, length, sign):
    product = first[:, None] * second[None, :] % length
    angle = 2.0 * half_turn / length * product.astype(jnp.float32)
    factor = 1.0 / math.sqrt(length)
    return (jnp.cos(angle) * factor, sign * jnp.sin(angle) * factor)


def cross_waves(waves, field):
    first, second, third = waves
    return jnp.stack(
        [
            second * field[:, 2] - third * field[:, 1],
            third * field[:, 0] - first * field[:, 2],
            first * field[:, 1] - second * field[:, 0],
        ],
        axis=1,
    )


def along_width(field, cosine, sine):
    breadth = field.shape[-1]
    rows = field.reshape(2, -1, breadth)
    joined = jnp.concatenate([cosine, sine], axis=1)
    real_prod = jnp.dot(rows[0], joined, precision=highest)
    imag_prod = jnp.dot(rows[1], joined, precision=highest)
    real_out = real_prod[:, :breadth] - imag_prod[:, breadth:]
    imag_out = real_prod[:, breadth:] + imag_prod[:, :breadth]
    return jnp.stack([real_out, imag_out]).reshape(field.shape)


def along_height(field, cosine, sine):
    tables = jnp.stack([cosine, sine])
    product = jnp.einsum("pcbzyx,tyk->tpcbzkx", field, tables, precision=highest)
    return jnp.stack([product[0, 0] - product[1, 1], product[1, 0] + product[0, 1]])


def along_depth(field, cosine, sine):
    tables = jnp.stack([cosine, sine])
    product = jnp.einsum("pcbzyx,tzk->tpcbkyx", field, tables, precision=highest)
    return jnp.stack([product[0, 0] - product[1, 1], product[1, 0] + product[0, 1]])


def apply_material(field, material, inv_diag, inv_off):
    materials = inv_diag.shape[0]
    onehot = (material[None] == jnp.arange(materials, dtype=jnp.int32)[:, None, None, None]).astype(
        jnp.float32
    )
    table = jnp.concatenate([inv_diag, inv_off], axis=1)
    tensor = jnp.einsum("mk,mzyx->kzyx", table, onehot, precision=highest)
    first = field[:, 0]
    second = field[:, 1]
    third = field[:, 2]
    return jnp.stack(
        [
            tensor[0] * first + tensor[3] * second + tensor[5] * third,
            tensor[3] * first + tensor[1] * second + tensor[4] * third,
            tensor[5] * first + tensor[4] * second + tensor[2] * third,
        ],
        axis=1,
    )


def on_device(coeffs, material, inv_diag, inv_off):
    groups = lax.axis_size("gz")
    levels = groups.bit_length() - 1
    depth = coeffs.shape[3]
    height = coeffs.shape[4]
    breadth = coeffs.shape[5]
    total_depth = depth * groups
    device = lax.axis_index("gz")
    local_rows = jnp.arange(depth, dtype=jnp.int32)
    waves_here = reverse_bits(device, levels) + groups * local_rows
    across = jnp.arange(breadth, dtype=jnp.int32)
    upward = jnp.arange(height, dtype=jnp.int32)
    waves = (
        signed_wave(across, breadth)[None, None, :],
        signed_wave(upward, height)[None, :, None],
        signed_wave(waves_here, total_depth)[:, None, None],
    )
    curl = cross_waves(waves, coeffs)
    all_rows = jnp.arange(total_depth, dtype=jnp.int32)
    wave_rows = reverse_bits(all_rows // depth, levels) + groups * (all_rows % depth)
    height_cos, height_sin = phase_tables(upward, upward, height, 1.0)
    width_cos, width_sin = phase_tables(across, across, breadth, 1.0)
    planar = along_height(curl, height_cos, height_sin)
    planar = along_width(planar, width_cos, width_sin)
    material_slab = lax.all_to_all(material, "gz", split_axis=1, concat_axis=0, tiled=True)
    inverse_cos, inverse_sin = phase_tables(wave_rows, all_rows, total_depth, 1.0)
    forward_cos, forward_sin = phase_tables(all_rows, wave_rows, total_depth, -1.0)
    spatial_piece = along_depth(
        lax.all_to_all(planar, "gz", split_axis=4, concat_axis=3, tiled=True),
        inverse_cos,
        inverse_sin,
    )
    scaled_piece = apply_material(spatial_piece, material_slab, inv_diag, inv_off)
    returned = along_depth(scaled_piece, forward_cos, forward_sin)
    spectral = lax.all_to_all(returned, "gz", split_axis=3, concat_axis=4, tiled=True)
    spectral = along_width(spectral, width_cos, -width_sin)
    spectral = along_height(spectral, height_cos, -height_sin)
    theta = -cross_waves(waves, spectral)
    factor = 1.0 / (breadth * height * total_depth)
    piece = lax.all_gather(coeffs, "ba", axis=2, tiled=True)
    real_part = jnp.einsum("cbzyx,cezyx->be", piece[0], theta[0], precision=highest) + jnp.einsum(
        "cbzyx,cezyx->be", piece[1], theta[1], precision=highest
    )
    imag_part = jnp.einsum("cbzyx,cezyx->be", piece[0], theta[1], precision=highest) - jnp.einsum(
        "cbzyx,cezyx->be", piece[1], theta[0], precision=highest
    )
    block = jnp.stack([real_part, imag_part]) * factor
    gram = lax.psum(block, "gz")
    return (theta, gram)


MESH = pl.DeviceIdType.MESH
single = jnp.float32
half = jnp.bfloat16


def split_table(length, extra):
    numbers = np.arange(length)
    angle = 2.0 * np.pi / length * (numbers[:, None] * numbers[None, :] % length)
    cosine = np.cos(angle) * extra / math.sqrt(length)
    sine = np.sin(angle) * extra / math.sqrt(length)
    inverse = np.block([[cosine, sine], [-sine, cosine]])
    parts = []
    for table in (inverse, inverse.T):
        high = table.astype(np.float32).astype(half)
        low = (table - high.astype(np.float64)).astype(half)
        parts += [high, low]
    return np.stack(parts)


def halves(values):
    high = values.astype(half)
    return high, (values - high.astype(single)).astype(half)


def product(first, second):
    dot = functools.partial(jnp.dot, preferred_element_type=single)
    return dot(first[0], second[0]) + (dot(first[0], second[1]) + dot(first[1], second[0]))


def twiddled(pair, step, span, sign):
    real, imag = pair
    if step == 0:
        return real, imag
    if 2 * step == span:
        return (-imag, real) if sign > 0 else (imag, -real)
    angle = math.pi * step / span
    cosine, sine = math.cos(angle), sign * math.sin(angle)
    return real * cosine - imag * sine, real * sine + imag * cosine


def to_voxels(points):
    points = list(points)
    span = 1
    while span < len(points):
        for base in range(0, len(points), 2 * span):
            for step in range(span):
                a = points[base + step]
                t = twiddled(points[base + step + span], step, span, 1.0)
                points[base + step] = (a[0] + t[0], a[1] + t[1])
                points[base + step + span] = (a[0] - t[0], a[1] - t[1])
        span *= 2
    return points


def to_waves(points):
    points = list(points)
    span = len(points) // 2
    while span >= 1:
        for base in range(0, len(points), 2 * span):
            for step in range(span):
                a, t = points[base + step], points[base + step + span]
                points[base + step] = (a[0] + t[0], a[1] + t[1])
                points[base + step + span] = twiddled(
                    (a[0] - t[0], a[1] - t[1]), step, span, -1.0
                )
        span //= 2
    return points


def operator_kernel(
    groups,
    coeffs_hbm,
    material_hbm,
    diag_hbm,
    off_hbm,
    table_hbm,
    theta_ref,
    gram_ref,
    coeffs_ref,
    material_ref,
    table_ref,
    diag_ref,
    off_ref,
    slab_ref,
    tensor_ref,
    high_ref,
    low_ref,
    back_ref,
    pair_ref,
    other_ref,
    swap_ref,
    result_ref,
    return_ref,
    out1_ref,
    in1_ref,
    field_ref,
    scaled_ref,
    out2_ref,
    in2_ref,
    out3_ref,
    in3_ref,
    acc_ref,
    sums_ref,
    load_sem,
    slab_send,
    slab_recv,
    half_sem,
    send1,
    recv1,
    send2,
    recv2,
    far_sem,
    swap_send,
    swap_recv,
    return_send,
    return_recv,
    other_send,
    other_recv,
    sums_sem,
):
    _, comps, bands, depth, height, breadth = coeffs_ref.shape
    total = depth * groups
    members = groups // 2
    columns = height // members
    levels = groups.bit_length() - 1
    me = lax.axis_index("gz")
    mine = lax.axis_index("ba")
    side = me // members
    seat = me % members
    partner = (me + members) % groups
    pack = members // 2
    inner = seat // pack == 1 - side
    outer = jnp.logical_not(inner)
    odd = seat % 2 == 1
    direct = jnp.logical_and(inner, jnp.logical_not(odd))
    second_guest = jnp.logical_or(inner, odd)
    mate = {"ba": 1 - mine}
    step_rows = 16
    steps = height // step_rows

    def each_peer(body):
        def step(k, carry):
            body((me + k) % groups)
            return carry

        lax.fori_loop(1, groups, step, 0)

    def each_member(body):
        def step(k, carry):
            body(k, (seat + k) % members)
            return carry

        lax.fori_loop(1, members, step, 0)

    def row_load(b, row, n):
        return pltpu.make_async_copy(
            coeffs_hbm.at[:, :, b, row], coeffs_ref.at[:, :, b, row], load_sem.at[n, row]
        )

    loads = [
        pltpu.make_async_copy(table_hbm, table_ref, load_sem.at[2, 0]),
        pltpu.make_async_copy(material_hbm, material_ref, load_sem.at[2, 1]),
        pltpu.make_async_copy(diag_hbm, diag_ref, load_sem.at[3, 0]),
        pltpu.make_async_copy(off_hbm, off_ref, load_sem.at[3, 1]),
    ]
    row_load(1 - side, 0, 0).start()
    barrier = pltpu.get_barrier_semaphore()
    each_peer(
        lambda peer: pl.semaphore_signal(
            barrier, inc=1, device_id={"gz": peer}, device_id_type=MESH
        )
    )
    pl.semaphore_signal(barrier, inc=1, device_id=mate, device_id_type=MESH)

    row_load(1 - side, 1, 0).start()
    for row in range(depth):
        row_load(side, row, 1).start()
    for load in loads:
        load.start()

    def signed(number, length):
        return number - length * (number // (length // 2))

    def row_number(owner, row):
        reversed_owner = 0
        for position in range(levels):
            bit = (owner // (1 << position)) % 2
            reversed_owner = reversed_owner + bit * (1 << (levels - 1 - position))
        return signed(reversed_owner + groups * row, total)

    def inverse_of(values):
        zero = values == 0
        return jnp.where(zero, 0.0, 1.0 / jnp.where(zero, 1, values).astype(single))

    class Waves:
        def __init__(self, owner, row, i):
            shape = (step_rows, breadth)
            nx = lax.broadcasted_iota(jnp.int32, shape, 1)
            ny = lax.broadcasted_iota(jnp.int32, shape, 0) + i * step_rows
            nx = jnp.where(nx < breadth // 2, nx, nx - breadth)
            ny = jnp.where(ny < height // 2, ny, ny - height)
            nz = jnp.full(shape, row_number(owner, row), jnp.int32)
            self.x = nx.astype(single) / (breadth / 2.0)
            self.y = ny.astype(single) / (height / 2.0)
            self.z = nz.astype(single) / (total / 2.0)
            ax, ay, az = jnp.abs(nx) * total, jnp.abs(ny) * total, jnp.abs(nz) * breadth
            self.is_x = (ax >= ay) & (ax >= az)
            self.is_y = ay >= az
            self.numbers = (nx, ny, nz)

        def cross(self, v):
            q = (self.x, self.y, self.z)
            return [
                q[(c + 1) % 3] * v[(c + 2) % 3] - q[(c + 2) % 3] * v[(c + 1) % 3]
                for c in range(3)
            ]

        def pick(self, first, second, third):
            return jnp.where(self.is_x, first, jnp.where(self.is_y, second, third))

        def inverse(self):
            nx, ny, nz = self.numbers
            scaled = self.pick(nx * total, ny * total, nz * breadth)
            return inverse_of(scaled) * (total * breadth / 2.0)

        def ratios(self):
            inverse = self.inverse()
            return (
                self.pick(self.y, self.z, self.x) * inverse,
                self.pick(self.z, self.x, self.y) * inverse,
            )

        def reduce(self, v):
            return self.pick(v[1], v[2], v[0]), self.pick(v[2], v[0], v[1])

        def rebuild(self, ratios, first, second):
            last = -(ratios[0] * first + ratios[1] * second)
            return [
                self.pick(last, second, first),
                self.pick(first, last, second),
                self.pick(second, first, last),
            ]

    def rows_of(i):
        return pl.ds(pl.multiple_of(i * step_rows, step_rows), step_rows)

    def each_step(row, body):
        def step(i, carry):
            body(row, i)
            return carry

        lax.fori_loop(0, steps, step, 0, unroll=2)

    def each_row(body):
        def step(row, carry):
            body(row)
            return carry

        lax.fori_loop(0, depth, step, 0)

    def put_halves(curls, p, row, i):
        at = pl.ds(pl.multiple_of(p * height + i * step_rows, step_rows), step_rows)
        for c in range(3):
            high, low = halves(curls[c])
            lanes = pl.ds(c * breadth, breadth)
            high_ref[row, at, lanes] = high
            low_ref[row, at, lanes] = low

    def put_pair(b, p, row, i, pair):
        for n in range(2):
            pair_ref[b, row, n, p, rows_of(i), :] = pair[n]

    def away_step(row, i):
        waves = Waves(me, row, i)
        for p in range(2):
            values = [coeffs_ref[p, c, 1 - side, row, rows_of(i), :] for c in range(3)]
            put_pair(1 - side, p, row, i, waves.reduce(waves.cross(values)))

    def home_step(row, i):
        waves = Waves(me, row, i)
        for p in range(2):
            values = [coeffs_ref[p, c, side, row, rows_of(i), :] for c in range(3)]
            curls = waves.cross(values)
            put_halves(curls, p, row, i)
            put_pair(side, p, row, i, waves.reduce(curls))

    def direct_step(row, i):
        waves = Waves(me, row, i)
        for p in range(2):
            values = [coeffs_ref[p, c, 1 - side, row, rows_of(i), :] for c in range(3)]
            put_halves(waves.cross(values), p, row, i)

    def guest_step(row, i):
        waves = Waves(partner, row, i)
        ratios = waves.ratios()
        for p in range(2):
            pair = [swap_ref[row, n, p, rows_of(i), :] for n in range(2)]
            put_halves(waves.rebuild(ratios, *pair), p, row, i)

    def plain_table():
        return table_ref[0], table_ref[1]

    def turned_table():
        return table_ref[2], table_ref[3]

    def gather_blocks(values):
        top, bottom = values[:height], values[height:]
        return jnp.concatenate(
            [
                jnp.concatenate(
                    [
                        top[:, z * breadth : (z + 1) * breadth],
                        bottom[:, z * breadth : (z + 1) * breadth],
                    ],
                    axis=1,
                )
                for z in range(3)
            ],
            axis=0,
        )

    def spread_blocks(values):
        return jnp.concatenate(
            [
                jnp.concatenate(
                    [
                        values[z * height : (z + 1) * height, p * breadth : (p + 1) * breadth]
                        for z in range(3)
                    ],
                    axis=1,
                )
                for p in range(2)
            ],
            axis=0,
        )

    def to_peer(out, into, send, recv, s, row, peer, from_at, to_at):
        return pltpu.make_async_remote_copy(
            src_ref=out.at[from_at, row, peer],
            dst_ref=into.at[to_at, row, seat],
            send_sem=send.at[s, row],
            recv_sem=recv.at[s, row],
            device_id={"gz": side * members + peer},
            device_id_type=MESH,
        )

    def blocks(count, out, into, send, recv, s, row, from_at, to_at):
        return pltpu.make_async_remote_copy(
            src_ref=out.at[from_at, row, pl.ds(0, count)],
            dst_ref=into.at[to_at, row, pl.ds(0, count)],
            send_sem=send.at[s, row],
            recv_sem=recv.at[s, row],
            device_id={"gz": side * members + (seat + 1) % members},
            device_id_type=MESH,
        )

    def ends1(s):
        return s, (side + s) % 2

    def ends2(s):
        return (side + s) % 2, s

    def start_all(out, into, send, recv, s, row, ends):
        each_member(lambda k, peer: to_peer(out, into, send, recv, s, row, peer, *ends).start())
        into[ends[1], row, seat] = out[ends[0], row, seat]

    def finish_all(out, into, send, recv, s, row, ends):
        blocks(members - 1, out, into, send, recv, s, row, *ends).wait_recv()

    def drain_all(out, into, send, recv, s, row, ends):
        blocks(members - 1, out, into, send, recv, s, row, *ends).wait_send()

    def is_inner(peer):
        return peer // pack == 1 - side

    def each_inner(body):
        def one(k, peer):
            pl.when(is_inner(peer))(lambda: body(k, peer))

        each_member(one)

    def across(peer):
        return {"gz": (1 - side) * members + peer}

    def direct_copy(peer):
        return pltpu.make_async_remote_copy(
            src_ref=out3_ref.at[peer],
            dst_ref=in1_ref.at[side, 1, seat],
            send_sem=far_sem.at[0],
            recv_sem=far_sem.at[1],
            device_id=across(peer),
            device_id_type=MESH,
        )

    def direct_blocks(count):
        return pltpu.make_async_remote_copy(
            src_ref=out3_ref.at[pl.ds(0, count)],
            dst_ref=in1_ref.at[1 - side, 1, pl.ds(0, count)],
            send_sem=far_sem.at[0],
            recv_sem=far_sem.at[1],
            device_id=across(seat),
            device_id_type=MESH,
        )

    def direct_result(n):
        peer = side * pack + n
        return pltpu.make_async_remote_copy(
            src_ref=out2_ref.at[1 - side, 1, peer],
            dst_ref=in3_ref.at[seat],
            send_sem=far_sem.at[2],
            recv_sem=far_sem.at[3],
            device_id=across(peer),
            device_id_type=MESH,
        )

    def result_blocks(count):
        return pltpu.make_async_remote_copy(
            src_ref=out2_ref.at[1 - side, 1, pl.ds(0, count)],
            dst_ref=in3_ref.at[pl.ds(0, count)],
            send_sem=far_sem.at[2],
            recv_sem=far_sem.at[3],
            device_id=across(seat),
            device_id_type=MESH,
        )

    def each_of(count, body):
        def step(n, carry):
            body(n)
            return carry

        lax.fori_loop(0, count, step, 0)

    first = (out1_ref, in1_ref, send1, recv1)
    second = (out2_ref, in2_ref, send2, recv2)

    def planes_into(put, row):
        tall = product(turned_table(), (high_ref[row], low_ref[row]))
        wide = product(halves(gather_blocks(tall)), plain_table())
        for p in range(2):
            for c in range(3):
                plane = wide[c * height : (c + 1) * height, p * breadth : (p + 1) * breadth]
                put(c, p, plane.reshape(members, columns, breadth))

    def make_planes(s, row):
        def put(c, p, block):
            out1_ref[s, row, :, c, p] = block

        planes_into(put, row)

    def swap_copy(row):
        return pltpu.make_async_remote_copy(
            src_ref=pair_ref.at[1 - side, row],
            dst_ref=swap_ref.at[row],
            send_sem=swap_send.at[row],
            recv_sem=swap_recv.at[row],
            device_id={"gz": partner},
            device_id_type=MESH,
        )

    def return_copy(row):
        return pltpu.make_async_remote_copy(
            src_ref=result_ref.at[row],
            dst_ref=return_ref.at[row],
            send_sem=return_send.at[row],
            recv_sem=return_recv.at[row],
            device_id={"gz": partner},
            device_id_type=MESH,
        )

    def other_copy(b, n):
        return pltpu.make_async_remote_copy(
            src_ref=pair_ref.at[b],
            dst_ref=other_ref.at[b],
            send_sem=other_send.at[n],
            recv_sem=other_recv.at[n],
            device_id=mate,
            device_id_type=MESH,
        )

    def columns_of(peer):
        return pl.ds(pl.multiple_of((peer % members) * columns, columns), columns)

    def slab_copy(peer, n):
        return pltpu.make_async_remote_copy(
            src_ref=material_ref.at[mine, columns_of(peer), :],
            dst_ref=slab_ref.at[mine, me],
            send_sem=slab_send.at[n],
            recv_sem=slab_recv.at[n],
            device_id={"gz": peer},
            device_id_type=MESH,
        )

    def slab_blocks(n):
        slots = slab_ref.at[mine, pl.ds(0, members - 1 + n)]
        return pltpu.make_async_remote_copy(
            src_ref=slots,
            dst_ref=slots,
            send_sem=slab_send.at[n],
            recv_sem=slab_recv.at[n],
            device_id={"gz": partner},
            device_id_type=MESH,
        )

    def half_copy(row, part):
        at = pl.ds(pl.multiple_of(part * members, members), members)
        return pltpu.make_async_remote_copy(
            src_ref=slab_ref.at[row, at],
            dst_ref=slab_ref.at[row, at],
            send_sem=half_sem.at[0, part],
            recv_sem=half_sem.at[1, part],
            device_id=mate,
            device_id_type=MESH,
        )

    def away_row(row):
        row_load(1 - side, row, 0).wait()
        each_step(row, away_step)

    def home_row(row):
        row_load(side, row, 1).wait()
        each_step(row, home_step)
        make_planes(0, row)
        start_all(*first, 0, row, ends1(0))

    def start_slab(base, n):
        def step(k, carry):
            slab_copy(base * members + (seat + k) % members, n).start()
            return carry

        lax.fori_loop(1 - n, members, step, 0)

    away_row(0)
    pl.semaphore_wait(barrier, groups)
    swap_copy(0).start()
    for load in loads:
        load.wait()
    pl.when(inner)(lambda: start_slab(side, 0))
    pl.when(inner)(lambda: start_slab(1 - side, 1))
    away_row(1)
    pl.when(jnp.logical_not(direct))(lambda: swap_copy(1).start())
    pl.when(outer)(lambda: start_slab(side, 0))
    pl.when(outer)(lambda: start_slab(1 - side, 1))
    slab_ref[mine, me] = material_ref[mine, columns_of(me), :]
    home_row(0)
    home_row(1)

    def make_direct():
        each_step(1, direct_step)

        def put(c, p, block):
            out3_ref[:, c, p] = block

        planes_into(put, 1)

    def send_direct():
        each_of(members, lambda n: direct_copy((seat + n) % members).start())

    pl.when(direct)(make_direct)
    other_copy(side, 1).start()
    acc_ref[...] = jnp.zeros(acc_ref.shape, single)

    def guest_row(row):
        swap_copy(row).wait_recv()
        each_step(row, guest_step)
        make_planes(1, row)
        start_all(*first, 1, row, ends1(1))

    guest_row(0)
    slab_blocks(0).wait_recv()
    half_copy(mine, side).start()
    pl.when(inner)(lambda: guest_row(1))
    slab_blocks(1).wait_recv()
    half_copy(mine, 1 - side).start()
    pl.when(direct)(send_direct)
    pl.when(jnp.logical_and(outer, odd))(lambda: guest_row(1))
    half_copy(1 - mine, side).wait_recv()
    half_copy(1 - mine, 1 - side).wait_recv()
    kinds = diag_ref.shape[0]

    def tensor_step(owner, carry):
        for row in range(depth):
            codes = slab_ref[row, owner]
            for entry in range(6):
                table = diag_ref if entry < 3 else off_ref
                values = jnp.full(codes.shape, table[0, entry % 3], single)
                for kind in range(1, kinds):
                    values = jnp.where(codes == kind, table[kind, entry % 3], values)
                tensor_ref[entry, owner, row] = values
        return carry

    lax.fori_loop(0, groups, tensor_step, 0)

    def part_of(n):
        return pl.ds(pl.multiple_of(n * 8, 8), 8)

    each_row(lambda row: finish_all(*first, 0, row, ends1(0)))
    finish_all(*first, 1, 0, ends1(1))

    def finish_second(count):
        blocks(count, *first, 1, 1, *ends1(1)).wait_recv()

    guests = pack + pack // 2
    pl.when(second_guest)(lambda: finish_second(guests - 1))
    pl.when(jnp.logical_not(second_guest))(lambda: finish_second(guests))
    direct_blocks(pack // 2).wait_recv()

    def inverse(at, c):
        points = []
        for r in range(total):
            owner, row = r // depth, r % depth
            where = (owner // members, row, owner % members, c)
            points.append((in1_ref[(*where, 0, at)], in1_ref[(*where, 1, at)]))
        for z, (real, imag) in enumerate(to_voxels(points)):
            field_ref[c, 0, z, at] = real
            field_ref[c, 1, z, at] = imag

    def scale(at, z):
        entries = [tensor_ref[entry, z // depth, z % depth, at] for entry in range(6)]
        xx, yy, zz, xy, yz, zx = entries
        for p in range(2):
            fx, fy, fz = [field_ref[c, p, z, at] for c in range(3)]
            scaled_ref[0, p, z, at] = xx * fx + xy * fy + zx * fz
            scaled_ref[1, p, z, at] = xy * fx + yy * fy + yz * fz
            scaled_ref[2, p, z, at] = zx * fx + yz * fy + zz * fz

    def forward(at, c):
        points = [(scaled_ref[c, 0, z, at], scaled_ref[c, 1, z, at]) for z in range(total)]
        for r, (real, imag) in enumerate(to_waves(points)):
            owner, row = r // depth, r % depth
            where = (owner // members, row, owner % members, c)
            out2_ref[(*where, 0, at)] = real
            out2_ref[(*where, 1, at)] = imag

    parts = columns // 8

    def part_copy(n, peer):
        at = part_of(n)
        return pltpu.make_async_remote_copy(
            src_ref=out2_ref.at[1 - side, 0, peer, :, :, at],
            dst_ref=in2_ref.at[1, 0, seat, :, :, at],
            send_sem=send2.at[1, 0],
            recv_sem=recv2.at[1, 0],
            device_id={"gz": side * members + peer},
            device_id_type=MESH,
        )

    def voxel_part(n):
        at = part_of(n)
        each_of(3, functools.partial(inverse, at))

        def scale_step(z, carry):
            scale(at, z)
            return carry

        lax.fori_loop(0, total, scale_step, 0, unroll=4)
        each_of(3, functools.partial(forward, at))
        each_member(lambda k, peer: part_copy(n, peer).start())

    each_of(parts, voxel_part)
    in2_ref[1, 0, seat] = out2_ref[1 - side, 0, seat]
    each_of(pack, lambda n: direct_result((seat + n) % pack).start())
    each_inner(lambda k, peer: to_peer(*second, 1, 1, peer, *ends2(1)).start())

    def keep_guest():
        in2_ref[1, 1, seat] = out2_ref[1 - side, 1, seat]

    pl.when(inner)(keep_guest)

    def start_home(row):
        start_all(*second, 0, row, ends2(0))

    pl.when(inner)(lambda: start_home(0))
    pl.when(inner)(lambda: start_home(1))
    other_copy(1 - side, 0).start()

    def planes_back(get, row):
        planes = jnp.concatenate(
            [
                jnp.concatenate(
                    [get(c, p).reshape(height, breadth) for p in range(2)], axis=1
                )
                for c in range(3)
            ],
            axis=0,
        )
        wide = product(halves(planes), turned_table())
        back_ref[row] = product(plain_table(), halves(spread_blocks(wide)))

    def take_planes(s, row):
        planes_back(lambda c, p: in2_ref[s, row, :, c, p], row)

    def theta_at(waves, p, row, i):
        at = pl.ds(pl.multiple_of(p * height + i * step_rows, step_rows), step_rows)
        lanes = [pl.ds(c * breadth, breadth) for c in range(3)]
        return [-v for v in waves.cross([back_ref[row, at, lanes[c]] for c in range(3)])]

    def guest_result(row, i):
        waves = Waves(partner, row, i)
        for p in range(2):
            pair = waves.reduce(theta_at(waves, p, row, i))
            for n in range(2):
                result_ref[row, n, p, rows_of(i), :] = pair[n]

    def add_sums(waves, pairs, row, i, sums):
        inverse = waves.inverse()
        (real1, real2), (imag1, imag2) = [[inverse * v for v in pair] for pair in pairs]
        sums = list(sums)
        n = 0
        for source in (pair_ref, other_ref):
            for a in range(bands):
                one_real, one_imag = [source[a, row, 0, p, rows_of(i), :] for p in range(2)]
                two_real, two_imag = [source[a, row, 1, p, rows_of(i), :] for p in range(2)]
                real = (two_real * real1 + two_imag * imag1) - (one_real * real2 + one_imag * imag2)
                imag = (two_real * imag1 - two_imag * real1) - (one_real * imag2 - one_imag * real2)
                sums[n] = sums[n] + real
                sums[n + 1] = sums[n + 1] + imag
                n += 2
        return tuple(sums)

    def each_sum(row, b, body):
        def step(i, sums):
            return body(row, i, sums)

        sums = lax.fori_loop(0, steps, step, tuple(acc_ref[b, n] for n in range(4 * bands)), unroll=2)
        for n in range(4 * bands):
            acc_ref[b, n] = sums[n]

    def keep_sums(b):
        sums = [acc_ref[b, n] for n in range(4 * bands)]
        lane = lax.broadcasted_iota(jnp.int32, (1, breadth), 1)
        rows = [jnp.zeros((1, breadth), single)] * 2
        n = 0
        for source in (mine, 1 - mine):
            for a in range(bands):
                for p in range(2):
                    value = jnp.sum(jnp.sum(sums[n], axis=0, keepdims=True), axis=1, keepdims=True)
                    rows[p] = rows[p] + jnp.where(lane == source * bands + a, value, 0.0)
                    n += 1
        sums_ref[me, b] = jnp.concatenate(rows, axis=0) * (1.0 / (breadth * height * total))

    def result_of(b):
        def result(row, i, sums):
            waves = Waves(me, row, i)
            pairs = []
            for p in range(2):
                theta = theta_at(waves, p, row, i)
                for c in range(3):
                    theta_ref[p, c, b, row, rows_of(i), :] = theta[c]
                pairs.append(waves.reduce(theta))
            return add_sums(waves, pairs, row, i, sums)

        return result

    def away_result(row, i, sums):
        waves = Waves(me, row, i)
        ratios = waves.ratios()
        pairs = []
        for p in range(2):
            pair = [return_ref[row, n, p, rows_of(i), :] for n in range(2)]
            theta = waves.rebuild(ratios, *pair)
            for c in range(3):
                theta_ref[p, c, 1 - side, row, rows_of(i), :] = theta[c]
            pairs.append(pair)
        return add_sums(waves, pairs, row, i, sums)

    def sums_copy(peer):
        return pltpu.make_async_remote_copy(
            src_ref=sums_ref.at[me],
            dst_ref=sums_ref.at[me],
            send_sem=sums_sem.at[0],
            recv_sem=sums_sem.at[1],
            device_id={"gz": peer},
            device_id_type=MESH,
        )

    def sums_blocks():
        slots = sums_ref.at[pl.ds(0, groups - 1)]
        return pltpu.make_async_remote_copy(
            src_ref=slots,
            dst_ref=slots,
            send_sem=sums_sem.at[0],
            recv_sem=sums_sem.at[1],
            device_id={"gz": partner},
            device_id_type=MESH,
        )

    def guest_back(row):
        take_planes(1, row)
        each_step(row, guest_result)
        return_copy(row).start()

    def second_back():
        finish_all(*second, 1, 1, ends2(1))
        guest_back(1)

    finish_all(*second, 1, 0, ends2(1))
    guest_back(0)
    pl.when(outer)(lambda: start_home(0))
    pl.when(outer)(lambda: start_home(1))
    pl.when(inner)(second_back)
    other_copy(side, 1).wait_recv()
    other_copy(1 - side, 0).wait_recv()

    def take_direct():
        result_blocks(members).wait_recv()
        planes_back(lambda c, p: in3_ref[:, c, p], 1)
        each_sum(1, 1 - side, result_of(1 - side))

    pl.when(inner)(take_direct)

    def home_back(row):
        finish_all(*second, 0, row, ends2(0))
        take_planes(0, row)
        each_sum(row, side, result_of(side))

    def away_back(row):
        return_copy(row).wait_recv()
        each_sum(row, 1 - side, away_result)

    def finish_inner():
        away_back(0)
        keep_sums(1 - side)
        home_back(1)
        keep_sums(side)

    def finish_outer():
        home_back(1)
        keep_sums(side)
        away_back(0)
        away_back(1)
        keep_sums(1 - side)

    home_back(0)
    pl.when(inner)(finish_inner)
    pl.when(outer)(finish_outer)

    def start_sums(n, carry):
        peer = (2 * groups - 1 - me + n) % groups
        pl.when(peer != me)(lambda: sums_copy(peer).start())
        return carry

    lax.fori_loop(0, groups, start_sums, 0, unroll=True)
    half_copy(mine, side).wait_send()
    half_copy(mine, 1 - side).wait_send()
    slab_blocks(0).wait_send()
    slab_blocks(1).wait_send()
    other_copy(1 - side, 0).wait_send()
    other_copy(side, 1).wait_send()
    swap_copy(0).wait_send()
    return_copy(0).wait_send()
    pl.when(jnp.logical_not(direct))(lambda: swap_copy(1).wait_send())

    pl.when(direct)(lambda: direct_blocks(members).wait_send())
    pl.when(second_guest)(lambda: drain_all(*first, 1, 1, ends1(1)))
    pl.when(inner)(lambda: return_copy(1).wait_send())
    pl.when(inner)(lambda: blocks(pack - 1, *second, 1, 1, *ends2(1)).wait_send())
    pl.when(outer)(lambda: blocks(pack, *second, 1, 1, *ends2(1)).wait_send())
    result_blocks(pack).wait_send()
    drain_all(*first, 1, 0, ends1(1))
    drain_all(*second, 1, 0, ends2(1))
    each_row(lambda row: drain_all(*first, 0, row, ends1(0)))
    each_row(lambda row: drain_all(*second, 0, row, ends2(0)))
    sums_blocks().wait_recv()
    grams = jnp.sum(sums_ref[...], axis=0)
    for p in range(2):
        for b in range(bands):
            gram_ref[p, b : b + 1, :] = grams[b, p : p + 1, : 2 * bands]
    sums_blocks().wait_send()


def deliver_kernel(theta_ref, gram_ref, theta_out, gram_out, theta_sem, gram_sem):
    copies = [pltpu.make_async_copy(gram_ref, gram_out, gram_sem)]
    for p in range(2):
        copies.append(pltpu.make_async_copy(theta_ref.at[p], theta_out.at[p], theta_sem.at[p]))
    for copy in copies:
        copy.start()
    for copy in copies:
        copy.wait()


def on_device_kernel(coeffs, material, inv_diag, inv_off):
    groups = lax.axis_size("gz")
    _, comps, bands, depth, height, breadth = coeffs.shape
    total = depth * groups
    members = groups // 2
    columns = height // members
    table = jnp.asarray(split_table(breadth, total**-0.25))
    voxels = (3, 2, total, columns, breadth)
    block = (2, depth, members, 3, 2, columns, breadth)
    pairs = (depth, 2, 2, height, breadth)
    vmem = pl.BlockSpec(memory_space=pltpu.VMEM)
    hbm = pl.BlockSpec(memory_space=pltpu.HBM)
    dma = pltpu.SemaphoreType.DMA
    operands = [
        pltpu.with_memory_space_constraint(v, pltpu.HBM)
        for v in (coeffs, material, inv_diag, inv_off, table)
    ]
    theta, gram = pl.pallas_call(
        functools.partial(operator_kernel, groups),
        out_shape=(
            jax.ShapeDtypeStruct(coeffs.shape, single),
            jax.ShapeDtypeStruct((2, bands, 2 * bands), single),
        ),
        in_specs=[hbm, hbm, hbm, hbm, hbm],
        out_specs=(vmem, vmem),
        scratch_shapes=[
            pltpu.VMEM(coeffs.shape, single),
            pltpu.VMEM(material.shape, jnp.int32),
            pltpu.VMEM(table.shape, half),
            pltpu.SMEM(inv_diag.shape, single),
            pltpu.SMEM(inv_off.shape, single),
            pltpu.VMEM((depth, groups, columns, breadth), jnp.int32),
            pltpu.VMEM((6, groups, depth, columns, breadth), single),
            pltpu.VMEM((depth, 2 * height, 3 * breadth), half),
            pltpu.VMEM((depth, 2 * height, 3 * breadth), half),
            pltpu.VMEM((depth, 2 * height, 3 * breadth), single),
            pltpu.VMEM((bands, *pairs), single),
            pltpu.VMEM((bands, *pairs), single),
            pltpu.VMEM(pairs, single),
            pltpu.VMEM(pairs, single),
            pltpu.VMEM(pairs, single),
            pltpu.VMEM(block, single),
            pltpu.VMEM(block, single),
            pltpu.VMEM(voxels, single),
            pltpu.VMEM(voxels, single),
            pltpu.VMEM(block, single),
            pltpu.VMEM(block, single),
            pltpu.VMEM(block[2:], single),
            pltpu.VMEM(block[2:], single),
            pltpu.VMEM((bands, 4 * bands, 16, breadth), single),
            pltpu.VMEM((groups, bands, 2, breadth), single),
            dma((4, depth)),
            dma((2,)),
            dma((2,)),
            dma((2, 2)),
            dma((2, depth)),
            dma((2, depth)),
            dma((2, depth)),
            dma((2, depth)),
            dma((4,)),
            dma((depth,)),
            dma((depth,)),
            dma((depth,)),
            dma((depth,)),
            dma((2,)),
            dma((2,)),
            dma((2,)),
        ],
        compiler_params=pltpu.CompilerParams(
            collective_id=0, has_side_effects=True, vmem_limit_bytes=48 * 1024 * 1024
        ),
        name="maxwell",
    )(*operands)
    theta, gram = pl.pallas_call(
        deliver_kernel,
        out_shape=(
            jax.ShapeDtypeStruct(theta.shape, single),
            jax.ShapeDtypeStruct(gram.shape, single),
        ),
        in_specs=[vmem, vmem],
        out_specs=(hbm, hbm),
        scratch_shapes=[dma((2,)), dma(())],
        compiler_params=pltpu.CompilerParams(vmem_limit_bytes=8 * 1024 * 1024),
        name="deliver",
    )(theta, gram)
    return (theta, gram.transpose(0, 2, 1))


def fits(coeffs):
    groups = lax.axis_size("gz")
    _, _, bands, depth, height, breadth = coeffs.shape
    return (
        lax.axis_size("ba") == 2
        and bands == 2
        and depth == 2
        and groups >= 8
        and height % (4 * groups) == 0
        and height % 16 == 0
        and height == breadth
        and breadth % 128 == 0
    )


def on_either(coeffs, material, inv_diag, inv_off):
    chosen = on_device_kernel if fits(coeffs) else on_device
    return chosen(coeffs, material, inv_diag, inv_off)


def solution(mesh):
    in_specs = (P(None, None, "ba", "gz", None, None), P("gz", None, None), P(), P())
    out_specs = (P(None, None, "ba", "gz", None, None), P(None, None, "ba"))
    return jax.shard_map(
        on_either, mesh=mesh, in_specs=in_specs, out_specs=out_specs, check_vma=False
    )
```
